32 devices in a mesh: atom: 4 (over y, x), tm: 8 (over z, core).
Axes of the slice: x: 2, y: 2, z: 4, core: 2. Of those that a mesh axis runs over, the one named last changes fastest.
Arguments:
- signal: bfloat16 [306, 8192], P(None, 'tm'), may hold values from -6 to 6
- spatial: bfloat16 [256, 306], P('atom'), may hold values from -0.3125 to 0.3125
- temporal: bfloat16 [256, 256], P('atom'), may hold values from -0.375 to 0.375
- code_values: bfloat16 [256, 8192], P('atom', 'tm'), may hold values from 0 to 2
- block_mask: int32 [256, 32], P('atom', 'tm'), may hold values 0 or 1
Outputs:
- grad_spatial: float32 [256, 306], P('atom')
- grad_temporal: float32 [256, 256], P('atom')
The draws below stay inside these ranges and needn't reach their ends.
All inputs are finite; a program needn't handle non-finite values. No bound on the sum of `block_mask` on one device may be relied on, other than what follows from the above.
Results may differ from the reference program's by a relative error of at most 0.0025.
Values may be sent and summed in bfloat16 or wider, within the bound.
A program may use at most 64 MiB of HBM per device.

```python
import math
import jax
import jax.numpy as jnp
from jax import lax

K = 256
P_SIZE = 306
L = 256
TIME = 8192
NBLK = 32
N_ATOM = 4


def place_ends(drawn, own_key, smallest, largest):
    index_at = [jax.random.randint(jax.random.fold_in(own_key, axis), (), 0, length) for axis, length in enumerate(drawn.shape)]
    main_axis = drawn.shape.index(max(drawn.shape))
    beside = index_at[:main_axis] + [(index_at[main_axis] + 1) % drawn.shape[main_axis]] + index_at[main_axis + 1:]
    return drawn.at[tuple(index_at)].set(smallest).at[tuple(beside)].set(largest)


def level_of(stream_key, dims, shards, low, largest):
    level, own = 1.0, jax.random.fold_in(stream_key, 6)
    for axis_at, blocks in shards:
        draws = jnp.exp(jax.random.uniform(jax.random.fold_in(own, axis_at), (blocks,), jnp.float32, low / len(shards), largest / len(shards)))
        level = level * jnp.repeat(draws, dims[axis_at] // blocks).reshape([-1 if axis == axis_at else 1 for axis in range(len(dims))])
    return level


def gaussian(key, extent, spread, bound, cuts=(), kind=jnp.bfloat16):
    result = spread * jax.random.normal(key, extent, jnp.float32)
    if cuts:
        result = result * level_of(key, extent, cuts, -0.22, 0.18)
    return jnp.clip(result, -bound, bound).astype(kind)


def setup_inputs(seed: int = 0) -> dict:
    streams_of = jax.random.split(jax.random.key(seed), 6)
    return {
        "signal": gaussian(streams_of[0], (P_SIZE, TIME), 1.0, 6.0, ((1, 8),)),
        "spatial": gaussian(streams_of[1], (K, P_SIZE), P_SIZE ** -0.5, 0.3125, ((0, 4),)),
        "temporal": gaussian(streams_of[2], (K, L), L ** -0.5, 0.375, ((0, 4),)),
        "code_values": jnp.clip(2.0 * jax.random.uniform(streams_of[3], (K, TIME), jnp.float32) ** level_of(streams_of[3], (K, TIME), ((0, 4), (1, 8)), -0.2, 0.2), 0.0, 2.0).astype(jnp.bfloat16),
        "block_mask": place_ends((jax.random.randint(streams_of[4], (K, NBLK), 0, 3) < 1).astype(jnp.int32), jax.random.fold_in(streams_of[4], 1), 0, 1),
    }


def toeplitz(kernels):
    count, length = kernels.shape
    heads = jnp.concatenate([jnp.zeros((count, 2 * length), kernels.dtype), kernels], axis=1)
    tiled = jnp.tile(heads, (1, 2 * length))[:, :2 * length * (3 * length - 1)]
    return tiled.reshape(count, 2 * length, 3 * length - 1)[:, :, :length]

def diagonals(products):
    count, rows_all, length = products.shape
    padded = jnp.concatenate([jnp.zeros((count, rows_all, 2 * length), products.dtype), products], axis=2)
    padded = padded.reshape(count, rows_all * 3 * length)
    padded = jnp.concatenate([padded, jnp.zeros((count, rows_all), products.dtype)], axis=1)
    skewed = padded.reshape(count, rows_all, 3 * length + 1)
    return lax.optimization_barrier(jnp.sum(skewed, axis=1))[:, length:2 * length]

def windows_of(extended, length):
    count, total = extended.shape
    blocks = extended.reshape(count, total // length, length)
    return jnp.concatenate([blocks[:, :-1], blocks[:, 1:]], axis=2)

def reference(signal, spatial, temporal, code_values, block_mask):
    atoms, channels = spatial.shape
    length = temporal.shape[1]
    samples = signal.shape[1]
    nblocks = samples // length
    groups = atoms // 4
    codes = (code_values.reshape(atoms, nblocks, length) * block_mask[:, :, None].astype(code_values.dtype)).reshape(atoms, samples)
    extended = jnp.concatenate([jnp.zeros((atoms, length), codes.dtype), codes], axis=1)

    def forward_group(operands):
        ext_group, kernels = operands
        windows = windows_of(ext_group, length).astype(jnp.float32)
        matrix = toeplitz(kernels).astype(jnp.float32)
        course_group = jnp.einsum('gbm,gms->gbs', windows, matrix)
        return course_group.reshape(4, samples).astype(jnp.bfloat16)
    course = lax.map(forward_group, (extended.reshape(groups, 4, length + samples), temporal.reshape(groups, 4, length)))
    course = course.reshape(atoms, samples)
    per_device = atoms // N_ATOM

    def add_group(total, operands):
        spatial_group, course_group = operands
        part = jnp.dot(spatial_group.T, course_group, preferred_element_type=jnp.float32).astype(jnp.bfloat16)
        part = lax.optimization_barrier(part)
        return (total + part.astype(jnp.float32), None)
    model, _ = lax.scan(add_group, jnp.zeros((channels, samples), jnp.float32), (spatial.reshape(N_ATOM, per_device, channels), course.reshape(N_ATOM, per_device, samples)))
    residual = (model - signal.astype(jnp.float32)).astype(jnp.bfloat16)
    projected = jnp.dot(spatial, residual, preferred_element_type=jnp.float32).astype(jnp.bfloat16)
    factor = 1.0 / math.sqrt(samples)
    grad_spatial = lax.dot_general(course, residual, (((1,), (1,)), ((), ())), preferred_element_type=jnp.float32) * factor

    def adjoint_group(operands):
        ext_group, proj_group = operands
        windows = windows_of(ext_group, length).astype(jnp.float32)
        proj_blocks = proj_group.reshape(4, nblocks, length).astype(jnp.float32)
        products = jnp.einsum('gbm,gbs->gms', windows, proj_blocks)
        return diagonals(products)
    grad_temporal = lax.map(adjoint_group, (extended.reshape(groups, 4, length + samples), projected.reshape(groups, 4, samples)))
    grad_temporal = grad_temporal.reshape(atoms, length) * factor
    return (grad_spatial, grad_temporal)
```

```python
import functools
import math

import jax
import jax.numpy as jnp
from jax import lax
from jax.experimental import pallas as pl
from jax.experimental.pallas import tpu as pltpu
from jax.sharding import PartitionSpec as P

W = 128
B = 32
GROUP = 16
MESH = pl.DeviceIdType.MESH
F32 = jnp.float32
BF16 = jnp.bfloat16


def kernel(
    n_atom, n_tm, factor,
    signal_ref, spatial_ref, temporal_ref, values_ref, mask_ref,
    out_sp_ref, out_tm_ref,
    tail, halo, cx, xt, wt, tbuf, cf, cbuf, sbuf, sp32, st, own_w, resb, pj, lt, gt,
    part, recv1, half, total,
    halo_sems, s_send, s_recv, c_send, c_recv,
    p_send, p_recv, z_send, z_recv, f_send, f_recv,
):
    atoms, channels = spatial_ref.shape
    length = temporal_ref.shape[1]
    samples = signal_ref.shape[1]
    blocks = mask_ref.shape[0]
    block = samples // blocks
    nb = samples // W
    hb = length // W
    chunk = length
    chunks = samples // chunk
    per = chunk // W
    rows_p = st.shape[0]
    wide = sp32.shape[1]
    chips = n_tm // 2
    me_a = lax.axis_index("atom")
    me_t = lax.axis_index("tm")
    me_z = me_t // 2
    core = lax.rem(me_t, 2)
    partner = me_z * 2 + 1 - core
    a_peers = [lax.rem(me_a + d, n_atom) for d in range(1, n_atom)]
    t_peers = [lax.rem(me_t + d, n_tm) for d in range(1, n_tm)]
    z_peers = [lax.rem(me_z + d, chips) for d in range(1, chips)]
    mine = pl.ds(pl.multiple_of(me_a * atoms, atoms), atoms)

    barrier = pltpu.get_barrier_semaphore()
    for peer in a_peers:
        pl.semaphore_signal(barrier, inc=1, device_id={"atom": peer}, device_id_type=MESH)
    for peer in t_peers:
        pl.semaphore_signal(barrier, inc=1, device_id={"tm": peer}, device_id_type=MESH)

    mask = mask_ref[...].astype(F32).T
    codes = [
        values_ref[:, j * block : (j + 1) * block].astype(F32) * mask[:, j : j + 1]
        for j in range(blocks)
    ]
    codes = jnp.concatenate(codes, axis=1)
    tail[...] = codes[:, samples - length :].astype(BF16)
    cx[: hb * atoms, :] = jnp.zeros((hb * atoms, W), F32)
    for b in range(nb):
        cx[(hb + b) * atoms : (hb + b + 1) * atoms, :] = codes[:, b * W : (b + 1) * W]
    for d in range(hb):
        wt[d * atoms : (d + 1) * atoms, :] = temporal_ref[:, d * W : (d + 1) * W].astype(F32)

    row = lax.broadcasted_iota(jnp.int32, (W, W), 0)
    col = lax.broadcasted_iota(jnp.int32, (W, W), 1)
    ahead = col >= row

    def toeplitz(k):
        circ = [
            pltpu.roll(
                jnp.broadcast_to(wt[pl.ds(d * atoms + k, 1), :], (W, W)),
                0, 1, stride=1, stride_axis=0,
            )
            for d in range(hb)
        ]
        zero = jnp.zeros((W, W), F32)
        parts = []
        for d in range(hb, -1, -1):
            near = circ[d] if d < hb else zero
            far = circ[d - 1] if d > 0 else zero
            parts.append(jnp.where(ahead, near, far))
        return jnp.concatenate(parts, axis=0)

    def windows(k):
        return jnp.concatenate(
            [cx[pl.ds(j * atoms + k, nb, stride=atoms), :] for j in range(hb + 1)], axis=1
        )

    def apply(p, taps):
        k = 2 * p
        lhs = jnp.concatenate([windows(k), windows(k + 1)], axis=0).astype(BF16)
        out = jnp.dot(lhs, taps, preferred_element_type=F32)
        cf[pl.ds(k, nb, stride=atoms), :] = out[:nb, :W]
        cf[pl.ds(k + 1, nb, stride=atoms), :] = out[nb:, W:]

    def first(p, carry):
        k = 2 * p
        taps = jnp.concatenate([toeplitz(k), toeplitz(k + 1)], axis=1).astype(BF16)
        tbuf[p] = taps
        apply(p, taps)
        return carry

    def again(p, carry):
        apply(p, tbuf[p])
        return carry

    lax.fori_loop(0, atoms // 2, first, 0)

    pl.semaphore_wait(barrier, n_atom - 1 + n_tm - 1)

    right = lax.rem(me_t + 1, n_tm)
    halo_copy = pltpu.make_async_remote_copy(
        src_ref=tail, dst_ref=halo, send_sem=halo_sems.at[0], recv_sem=halo_sems.at[1],
        device_id={"tm": right}, device_id_type=MESH,
    )

    @pl.when(me_t < n_tm - 1)
    def _():
        halo_copy.start()

    c_copies = [[None] * (n_atom - 1) for _ in range(chunks)]

    def send(c):
        for b in range(per):
            at = c * per + b
            cbuf[c, mine, b * W : (b + 1) * W] = cf[at * atoms : (at + 1) * atoms, :].astype(BF16)
        for d, peer in enumerate(a_peers):
            copy = pltpu.make_async_remote_copy(
                src_ref=cbuf.at[c, mine], dst_ref=cbuf.at[c, mine],
                send_sem=c_send.at[d, c], recv_sem=c_recv.at[d, c],
                device_id={"atom": peer}, device_id_type=MESH,
            )
            copy.start()
            c_copies[c][d] = copy

    s_copies = []
    for d, peer in enumerate(a_peers):
        copy = pltpu.make_async_remote_copy(
            src_ref=spatial_ref, dst_ref=sbuf.at[mine], send_sem=s_send.at[d],
            recv_sem=s_recv.at[d], device_id={"atom": peer}, device_id_type=MESH,
        )
        copy.start()
        s_copies.append(copy)
    for c in range(1, chunks):
        send(c)

    xt[length : length + samples, :atoms] = codes.T
    xt[length + samples :, :] = jnp.zeros((xt.shape[0] - length - samples, W), F32)
    pj[...] = jnp.zeros(pj.shape, F32)
    resb[:, channels // 16 * 16 :, :] = jnp.zeros(
        (chunks, rows_p - channels // 16 * 16, chunk), BF16
    )
    sp32[...] = jnp.zeros(sp32.shape, F32)

    @pl.when(me_t == 0)
    def _():
        halo[...] = jnp.zeros(halo.shape, halo.dtype)

    @pl.when(me_t > 0)
    def _():
        halo_copy.wait_recv()

    before = halo[...].astype(F32)
    for b in range(hb):
        cx[b * atoms : (b + 1) * atoms, :] = before[:, b * W : (b + 1) * W]
    lax.fori_loop(0, atoms // 2, again, 0)
    send(0)
    xt[:length, :atoms] = before.T

    per_block = W // B

    def lay(i, carry):
        s = B - 1 - i
        picked = jnp.concatenate(
            [xt[pl.ds(B * r + s, GROUP, stride=W), :] for r in range(per_block)], axis=0
        )
        lt[pl.ds(pl.multiple_of(i * atoms, atoms), atoms), : per_block * GROUP] = picked.T[:atoms]
        return carry

    lax.fori_loop(0, B, lay, 0)

    sbuf[mine, :] = spatial_ref[...]
    for copy in s_copies:
        copy.wait_recv()
    sp32[:, :channels] = sbuf[...].astype(F32)
    st[...] = sp32[...].T[:rows_p].astype(BF16)
    own_w[...] = sp32[mine, :rows_p].astype(BF16)

    def process(c, gsp):
        for copy in c_copies[c]:
            copy.wait_recv()
        model = jnp.dot(st[...], cbuf[c], preferred_element_type=F32)
        resb[c, :channels, :] = (
            model[:channels] - signal_ref[:, c * chunk : (c + 1) * chunk].astype(F32)
        ).astype(BF16)
        residual = resb[c]
        projected = jnp.dot(own_w[...], residual, preferred_element_type=F32)
        projected = projected.astype(BF16).astype(F32)
        for b in range(per):
            at = hb + c * per + b
            pj[0, at * atoms : (at + 1) * atoms, :] = projected[:, b * W : (b + 1) * W]
        grad = lax.dot_general(
            cbuf[c, mine, :], residual, (((1,), (1,)), ((), ())), preferred_element_type=F32
        )
        return grad if gsp is None else gsp + grad

    gsp = None
    for c in list(range(1, chunks)) + [0]:
        gsp = process(c, gsp)

    low = pl.ds(pl.multiple_of(core * (atoms // 2), atoms // 2), atoms // 2)
    other = pl.ds(pl.multiple_of((1 - core) * (atoms // 2), atoms // 2), atoms // 2)

    def swap(i, lanes):
        copy = pltpu.make_async_remote_copy(
            src_ref=part.at[i, other, lanes], dst_ref=recv1.at[i, :, lanes],
            send_sem=p_send.at[i], recv_sem=p_recv.at[i],
            device_id={"tm": partner}, device_id_type=MESH,
        )
        copy.start()
        return copy

    def spread(i, lanes, copy):
        copy.wait_recv()
        half[i, me_z, :, lanes] = part[i, low, lanes] + recv1[i, :, lanes]
        copies = []
        for d, peer in enumerate(z_peers):
            out = pltpu.make_async_remote_copy(
                src_ref=half.at[i, me_z, :, lanes], dst_ref=half.at[i, me_z, :, lanes],
                send_sem=z_send.at[i, d], recv_sem=z_recv.at[i, d],
                device_id={"tm": peer * 2 + core}, device_id_type=MESH,
            )
            out.start()
            copies.append(out)
        return copies

    def finish(i, lanes, copies):
        for copy in copies:
            copy.wait_recv()
        acc = half[i, 0, :, lanes]
        for z in range(1, chips):
            acc = acc + half[i, z, :, lanes]
        total[i, low, lanes] = acc * factor
        copy = pltpu.make_async_remote_copy(
            src_ref=total.at[i, low, lanes], dst_ref=total.at[i, low, lanes],
            send_sem=f_send.at[i], recv_sem=f_recv.at[i],
            device_id={"tm": partner}, device_id_type=MESH,
        )
        copy.start()
        return copy

    sp_lanes = slice(0, wide)
    tm_lanes = slice(0, length)
    part[0, :, :rows_p] = gsp
    if rows_p < wide:
        part[0, :, rows_p:] = jnp.zeros((atoms, wide - rows_p), F32)
    swap_sp = swap(0, sp_lanes)

    lane = lax.broadcasted_iota(jnp.int32, (atoms, W), 1)
    for r in range(1, per_block):
        turned = [
            pltpu.roll(pj[0, i * atoms : (i + 1) * atoms, :], W - B * r, 1)
            for i in range(hb, hb + nb)
        ]
        turned = [jnp.zeros((atoms, W), F32)] + turned + [jnp.zeros((atoms, W), F32)]
        for n in range(nb + 1):
            i = hb - 1 + n
            pj[r, i * atoms : (i + 1) * atoms, :] = jnp.where(
                lane < W - B * r, turned[n], turned[n + 1]
            )

    spread_sp = spread(0, sp_lanes, swap_sp)

    depth = (length + B - 1) // W + 1

    def correlate(k, carry):
        lhs = lt[pl.ds(k, B, stride=atoms), :][:, : per_block * GROUP].astype(BF16)
        rhs = jnp.concatenate(
            [
                jnp.concatenate(
                    [pj[r, pl.ds(j * atoms + k, GROUP, stride=atoms), :] for r in range(per_block)],
                    axis=0,
                )
                for j in range(depth)
            ],
            axis=1,
        ).astype(BF16)
        prod = jnp.dot(lhs, rhs, preferred_element_type=F32)
        prod = pltpu.roll(prod, depth * W - (B - 1), 1, stride=1, stride_axis=0)[:, :length]
        acc = prod[:8]
        for i in range(1, B // 8):
            acc = acc + prod[8 * i : 8 * i + 8]
        for d in range(hb):
            gt[pl.ds(pl.multiple_of(8 * (d * atoms + k), 8), 8), :] = acc[:, d * W : (d + 1) * W]
        return carry

    lax.fori_loop(0, atoms, correlate, 0)
    for d in range(hb):
        gtm = gt[pl.ds(8 * d * atoms, atoms, stride=8), :]
        for i in range(1, 8):
            gtm = gtm + gt[pl.ds(8 * d * atoms + i, atoms, stride=8), :]
        part[1, :, d * W : (d + 1) * W] = gtm
    swap_tm = swap(1, tm_lanes)
    spread_tm = spread(1, tm_lanes, swap_tm)
    last_sp = finish(0, sp_lanes, spread_sp)
    last_tm = finish(1, tm_lanes, spread_tm)
    last_sp.wait_recv()
    out_sp_ref[...] = total[0, :, :channels]
    last_tm.wait_recv()
    out_tm_ref[...] = total[1, :, :length]

    @pl.when(me_t < n_tm - 1)
    def _():
        halo_copy.wait_send()

    for copy in s_copies + [copy for line in c_copies for copy in line]:
        copy.wait_send()
    for copy in [swap_sp, swap_tm, last_sp, last_tm] + spread_sp + spread_tm:
        copy.wait_send()


def local(n_atom, n_tm, signal, spatial, temporal, values, mask):
    atoms, channels = spatial.shape
    length = temporal.shape[1]
    samples = signal.shape[1]
    chunks = samples // length
    nb, hb = samples // W, length // W
    wide = -(-channels // W) * W
    rows_p = -(-channels // 32) * 32
    per_block = W // B
    every = n_atom * atoms
    depth = (length + B - 1) // W + 1
    span = (GROUP + depth - 1) * atoms
    width = max(wide, length)
    chips = n_tm // 2
    factor = 1.0 / math.sqrt(samples * n_tm)
    dma = pltpu.SemaphoreType.DMA
    vmem = pl.BlockSpec(memory_space=pltpu.VMEM)
    return pl.pallas_call(
        functools.partial(kernel, n_atom, n_tm, factor),
        out_shape=(
            pltpu.VMEM((atoms, channels), F32),
            pltpu.VMEM((atoms, length), F32),
        ),
        in_specs=[vmem] * 5,
        out_specs=(vmem, vmem),
        scratch_shapes=[
            pltpu.VMEM((atoms, length), BF16),
            pltpu.VMEM((atoms, length), BF16),
            pltpu.VMEM(((hb + nb) * atoms, W), F32),
            pltpu.VMEM((GROUP * W, W), F32),
            pltpu.VMEM((hb * atoms, W), F32),
            pltpu.VMEM((atoms // 2, (hb + 1) * W, 2 * W), BF16),
            pltpu.VMEM((nb * atoms, W), F32),
            pltpu.VMEM((chunks, every, length), BF16),
            pltpu.VMEM((every, channels), BF16),
            pltpu.VMEM((every, wide), F32),
            pltpu.VMEM((rows_p, every), BF16),
            pltpu.VMEM((atoms, rows_p), BF16),
            pltpu.VMEM((chunks, rows_p, length), BF16),
            pltpu.VMEM((per_block, span, W), F32),
            pltpu.VMEM((B * atoms, W), F32),
            pltpu.VMEM((8 * hb * atoms, W), F32),
            pltpu.VMEM((2, atoms, width), F32),
            pltpu.VMEM((2, atoms // 2, width), F32),
            pltpu.VMEM((2, chips, atoms // 2, width), F32),
            pltpu.VMEM((2, atoms, width), F32),
            dma((2,)),
            dma((n_atom - 1,)),
            dma((n_atom - 1,)),
            dma((n_atom - 1, chunks)),
            dma((n_atom - 1, chunks)),
            dma((2,)),
            dma((2,)),
            dma((2, chips - 1)),
            dma((2, chips - 1)),
            dma((2,)),
            dma((2,)),
        ],
        compiler_params=pltpu.CompilerParams(collective_id=0, has_side_effects=True),
    )(signal, spatial, temporal, values, mask.T)


def solution(mesh):
    in_specs = (P(None, "tm"), P("atom", None), P("atom", None), P("atom", "tm"), P("atom", "tm"))
    out_specs = (P("atom", None), P("atom", None))
    body = functools.partial(local, mesh.shape["atom"], mesh.shape["tm"])
    return jax.shard_map(body, mesh=mesh, in_specs=in_specs, out_specs=out_specs, check_vma=False)
```

```python
import functools
import math

import jax
import jax.numpy as jnp
from jax import lax
from jax.experimental import pallas as pl
from jax.experimental.pallas import tpu as pltpu
from jax.sharding import PartitionSpec as P

W = 128
B = 32
GROUP = 16
MESH = pl.DeviceIdType.MESH
F32 = jnp.float32
BF16 = jnp.bfloat16


def kernel(
    n_atom, n_tm, factor,
    signal_ref, spatial_ref, temporal_ref, values_ref, mask_ref,
    out_sp_ref, out_tm_ref,
    tail, halo, cx, xt, wt, tbuf, cf, cbuf, sbuf, sp32, st, own_w, resb, pj, lt, gt,
    part, recv1, half, total,
    halo_sems, s_send, s_recv, c_send, c_recv,
    p_send, p_recv, z_send, z_recv, f_send, f_recv,
):
    atoms, channels = spatial_ref.shape
    length = temporal_ref.shape[1]
    samples = signal_ref.shape[1]
    blocks = mask_ref.shape[0]
    block = samples // blocks
    nb = samples // W
    hb = length // W
    chunk = length
    chunks = samples // chunk
    per = chunk // W
    rows_p = st.shape[0]
    wide = sp32.shape[1]
    span = pj.shape[1] // atoms
    chips = n_tm // 2
    me_a = lax.axis_index("atom")
    me_t = lax.axis_index("tm")
    me_z = me_t // 2
    core = lax.rem(me_t, 2)
    partner = me_z * 2 + 1 - core
    a_peers = [lax.rem(me_a + d, n_atom) for d in range(1, n_atom)]
    t_peers = [lax.rem(me_t + d, n_tm) for d in range(1, n_tm)]
    z_peers = [lax.rem(me_z + d, chips) for d in range(1, chips)]
    mine = pl.ds(pl.multiple_of(me_a * atoms, atoms), atoms)

    barrier = pltpu.get_barrier_semaphore()
    for peer in a_peers:
        pl.semaphore_signal(barrier, inc=1, device_id={"atom": peer}, device_id_type=MESH)
    for peer in t_peers:
        pl.semaphore_signal(barrier, inc=1, device_id={"tm": peer}, device_id_type=MESH)

    groups = atoms // 8

    def put(ref, count, b, value):
        for g in range(groups):
            ref[(g * count + b) * 8 : (g * count + b + 1) * 8, :] = value[8 * g : 8 * g + 8]

    def natural(ref, count, b):
        return jnp.concatenate(
            [ref[(g * count + b) * 8 : (g * count + b + 1) * 8, :] for g in range(groups)], axis=0
        )

    def series(ref, count, g, i, first, size):
        return ref[pl.ds((g * count + first) * 8 + i, size, stride=8), :]

    mask = mask_ref[...].astype(F32).T
    codes = [
        values_ref[:, j * block : (j + 1) * block].astype(F32) * mask[:, j : j + 1]
        for j in range(blocks)
    ]
    codes = jnp.concatenate(codes, axis=1)
    tail[...] = codes[:, samples - length :].astype(BF16)
    for b in range(hb):
        put(cx, hb + nb, b, jnp.zeros((atoms, W), F32))
    for b in range(nb):
        put(cx, hb + nb, hb + b, codes[:, b * W : (b + 1) * W])
    for d in range(hb):
        wt[d * atoms : (d + 1) * atoms, :] = temporal_ref[:, d * W : (d + 1) * W].astype(F32)

    row = lax.broadcasted_iota(jnp.int32, (W, W), 0)
    col = lax.broadcasted_iota(jnp.int32, (W, W), 1)
    ahead = col >= row

    def toeplitz(rows, i):
        circ = [
            pltpu.roll(
                jnp.broadcast_to(rows[d][i : i + 1], (W, W)), 0, 1, stride=1, stride_axis=0
            )
            for d in range(hb)
        ]
        zero = jnp.zeros((W, W), F32)
        parts = []
        for d in range(hb, -1, -1):
            near = circ[d] if d < hb else zero
            far = circ[d - 1] if d > 0 else zero
            parts.append(jnp.where(ahead, near, far))
        return jnp.concatenate(parts, axis=0)

    def windows(g, i):
        return jnp.concatenate(
            [series(cx, hb + nb, g, i, j, nb) for j in range(hb + 1)], axis=1
        )

    def apply(g, i, taps):
        lhs = jnp.concatenate([windows(g, i), windows(g, i + 1)], axis=0).astype(BF16)
        out = jnp.dot(lhs, taps, preferred_element_type=F32)
        cf[pl.ds(g * nb * 8 + i, nb, stride=8), :] = out[:nb, :W]
        cf[pl.ds(g * nb * 8 + i + 1, nb, stride=8), :] = out[nb:, W:]

    def first(g, carry):
        rows = [
            wt[pl.ds(pl.multiple_of(d * atoms + 8 * g, 8), 8), :] for d in range(hb)
        ]
        for i in range(0, 8, 2):
            taps = jnp.concatenate([toeplitz(rows, i), toeplitz(rows, i + 1)], axis=1).astype(BF16)
            tbuf[g * 4 + i // 2] = taps
            apply(g, i, taps)
        return carry

    def again(g, carry):
        for i in range(0, 8, 2):
            apply(g, i, tbuf[g * 4 + i // 2])
        return carry

    lax.fori_loop(0, groups, first, 0)

    pl.semaphore_wait(barrier, n_atom - 1 + n_tm - 1)

    right = lax.rem(me_t + 1, n_tm)
    halo_copy = pltpu.make_async_remote_copy(
        src_ref=tail, dst_ref=halo, send_sem=halo_sems.at[0], recv_sem=halo_sems.at[1],
        device_id={"tm": right}, device_id_type=MESH,
    )

    @pl.when(me_t < n_tm - 1)
    def _():
        halo_copy.start()

    c_copies = [[None] * (n_atom - 1) for _ in range(chunks)]

    def send(c):
        for b in range(per):
            at = c * per + b
            cbuf[c, mine, b * W : (b + 1) * W] = natural(cf, nb, at).astype(BF16)
        for d, peer in enumerate(a_peers):
            copy = pltpu.make_async_remote_copy(
                src_ref=cbuf.at[c, mine], dst_ref=cbuf.at[c, mine],
                send_sem=c_send.at[d, c], recv_sem=c_recv.at[d, c],
                device_id={"atom": peer}, device_id_type=MESH,
            )
            copy.start()
            c_copies[c][d] = copy

    s_copies = []
    for d, peer in enumerate(a_peers):
        copy = pltpu.make_async_remote_copy(
            src_ref=spatial_ref, dst_ref=sbuf.at[mine], send_sem=s_send.at[d],
            recv_sem=s_recv.at[d], device_id={"atom": peer}, device_id_type=MESH,
        )
        copy.start()
        s_copies.append(copy)
    for c in range(1, chunks):
        send(c)

    def lay_time(b, value):
        turned = value.T
        for u in range(W // 8):
            at = (u * GROUP + b) * 8
            xt[at : at + 8, :atoms] = turned[8 * u : 8 * u + 8]

    for b in range(nb):
        lay_time(hb + b, codes[:, b * W : (b + 1) * W])
    for u in range(W // 8):
        xt[(u * GROUP + hb + nb) * 8 : (u + 1) * GROUP * 8, :] = jnp.zeros(
            ((GROUP - hb - nb) * 8, W), F32
        )
    pj[...] = jnp.zeros(pj.shape, F32)
    resb[:, channels // 16 * 16 :, :] = jnp.zeros(
        (chunks, rows_p - channels // 16 * 16, chunk), BF16
    )
    sp32[...] = jnp.zeros(sp32.shape, F32)

    @pl.when(me_t == 0)
    def _():
        halo[...] = jnp.zeros(halo.shape, halo.dtype)

    @pl.when(me_t > 0)
    def _():
        halo_copy.wait_recv()

    before = halo[...].astype(F32)
    for b in range(hb):
        put(cx, hb + nb, b, before[:, b * W : (b + 1) * W])
    lax.fori_loop(0, groups, again, 0)
    send(0)
    for b in range(hb):
        lay_time(b, before[:, b * W : (b + 1) * W])

    per_block = W // B

    def lay(n, carry):
        for i in range(8):
            picked = jnp.concatenate(
                [
                    xt[pl.ds((B // 8 * r + B // 8 - 1 - n) * GROUP * 8 + 7 - i, GROUP, stride=8), :]
                    for r in range(per_block)
                ],
                axis=0,
            ).T
            for g in range(groups):
                at = pl.multiple_of((g * B + 8 * n + i) * 8, 8)
                lt[pl.ds(at, 8), : per_block * GROUP] = picked[8 * g : 8 * g + 8]
        return carry

    lax.fori_loop(0, B // 8, lay, 0)

    sbuf[mine, :] = spatial_ref[...]
    for copy in s_copies:
        copy.wait_recv()
    sp32[:, :channels] = sbuf[...].astype(F32)
    st[...] = sp32[...].T[:rows_p].astype(BF16)
    own_w[...] = sp32[mine, :rows_p].astype(BF16)

    def process(c, gsp):
        for copy in c_copies[c]:
            copy.wait_recv()
        model = jnp.dot(st[...], cbuf[c], preferred_element_type=F32)
        resb[c, :channels, :] = (
            model[:channels] - signal_ref[:, c * chunk : (c + 1) * chunk].astype(F32)
        ).astype(BF16)
        residual = resb[c]
        projected = jnp.dot(own_w[...], residual, preferred_element_type=F32)
        projected = projected.astype(BF16).astype(F32)
        for b in range(per):
            at = hb + c * per + b
            put(pj.at[0], span, at, projected[:, b * W : (b + 1) * W])
        grad = lax.dot_general(
            cbuf[c, mine, :], residual, (((1,), (1,)), ((), ())), preferred_element_type=F32
        )
        return grad if gsp is None else gsp + grad

    gsp = None
    for c in list(range(1, chunks)) + [0]:
        gsp = process(c, gsp)

    low = pl.ds(pl.multiple_of(core * (atoms // 2), atoms // 2), atoms // 2)
    other = pl.ds(pl.multiple_of((1 - core) * (atoms // 2), atoms // 2), atoms // 2)

    def swap(i, lanes):
        copy = pltpu.make_async_remote_copy(
            src_ref=part.at[i, other, lanes], dst_ref=recv1.at[i, :, lanes],
            send_sem=p_send.at[i], recv_sem=p_recv.at[i],
            device_id={"tm": partner}, device_id_type=MESH,
        )
        copy.start()
        return copy

    def spread(i, lanes, copy):
        copy.wait_recv()
        half[i, me_z, :, lanes] = part[i, low, lanes] + recv1[i, :, lanes]
        copies = []
        for d, peer in enumerate(z_peers):
            out = pltpu.make_async_remote_copy(
                src_ref=half.at[i, me_z, :, lanes], dst_ref=half.at[i, me_z, :, lanes],
                send_sem=z_send.at[i, d], recv_sem=z_recv.at[i, d],
                device_id={"tm": peer * 2 + core}, device_id_type=MESH,
            )
            out.start()
            copies.append(out)
        return copies

    def finish(i, lanes, copies):
        for copy in copies:
            copy.wait_recv()
        acc = half[i, 0, :, lanes]
        for z in range(1, chips):
            acc = acc + half[i, z, :, lanes]
        total[i, low, lanes] = acc * factor
        copy = pltpu.make_async_remote_copy(
            src_ref=total.at[i, low, lanes], dst_ref=total.at[i, low, lanes],
            send_sem=f_send.at[i], recv_sem=f_recv.at[i],
            device_id={"tm": partner}, device_id_type=MESH,
        )
        copy.start()
        return copy

    sp_lanes = slice(0, wide)
    tm_lanes = slice(0, length)
    part[0, :, :rows_p] = gsp
    if rows_p < wide:
        part[0, :, rows_p:] = jnp.zeros((atoms, wide - rows_p), F32)
    swap_sp = swap(0, sp_lanes)

    lane = lax.broadcasted_iota(jnp.int32, (atoms, W), 1)
    for r in range(1, per_block):
        turned = [
            pltpu.roll(natural(pj.at[0], span, i), W - B * r, 1)
            for i in range(hb, hb + nb)
        ]
        turned = [jnp.zeros((atoms, W), F32)] + turned + [jnp.zeros((atoms, W), F32)]
        for n in range(nb + 1):
            put(
                pj.at[r], span, hb - 1 + n,
                jnp.where(lane < W - B * r, turned[n], turned[n + 1]),
            )

    spread_sp = spread(0, sp_lanes, swap_sp)

    depth = (length + B - 1) // W + 1

    def correlate(g, carry):
        for i in range(8):
            lhs = series(lt, B, g, i, 0, B)[:, : per_block * GROUP].astype(BF16)
            rhs = jnp.concatenate(
                [
                    jnp.concatenate(
                        [series(pj.at[r], span, g, i, j, GROUP) for r in range(per_block)], axis=0
                    )
                    for j in range(depth)
                ],
                axis=1,
            ).astype(BF16)
            prod = jnp.dot(lhs, rhs, preferred_element_type=F32)
            prod = pltpu.roll(prod, depth * W - (B - 1), 1, stride=1, stride_axis=0)[:, :length]
            acc = prod[:8]
            for q in range(1, B // 8):
                acc = acc + prod[8 * q : 8 * q + 8]
            for d in range(hb):
                at = pl.multiple_of((d * groups + g) * 64 + 8 * i, 8)
                gt[pl.ds(at, 8), :] = acc[:, d * W : (d + 1) * W]
        return carry

    lax.fori_loop(0, groups, correlate, 0)
    for d in range(hb):
        gtm = gt[pl.ds(8 * d * atoms, atoms, stride=8), :]
        for i in range(1, 8):
            gtm = gtm + gt[pl.ds(8 * d * atoms + i, atoms, stride=8), :]
        part[1, :, d * W : (d + 1) * W] = gtm
    swap_tm = swap(1, tm_lanes)
    spread_tm = spread(1, tm_lanes, swap_tm)
    last_sp = finish(0, sp_lanes, spread_sp)
    last_tm = finish(1, tm_lanes, spread_tm)
    last_sp.wait_recv()
    out_sp_ref[...] = total[0, :, :channels]
    last_tm.wait_recv()
    out_tm_ref[...] = total[1, :, :length]

    @pl.when(me_t < n_tm - 1)
    def _():
        halo_copy.wait_send()

    for copy in s_copies + [copy for line in c_copies for copy in line]:
        copy.wait_send()
    for copy in [swap_sp, swap_tm, last_sp, last_tm] + spread_sp + spread_tm:
        copy.wait_send()


def local(n_atom, n_tm, signal, spatial, temporal, values, mask):
    atoms, channels = spatial.shape
    length = temporal.shape[1]
    samples = signal.shape[1]
    chunks = samples // length
    nb, hb = samples // W, length // W
    wide = -(-channels // W) * W
    rows_p = -(-channels // 32) * 32
    per_block = W // B
    every = n_atom * atoms
    depth = (length + B - 1) // W + 1
    span = (GROUP + depth - 1) * atoms
    width = max(wide, length)
    chips = n_tm // 2
    factor = 1.0 / math.sqrt(samples * n_tm)
    dma = pltpu.SemaphoreType.DMA
    vmem = pl.BlockSpec(memory_space=pltpu.VMEM)
    return pl.pallas_call(
        functools.partial(kernel, n_atom, n_tm, factor),
        out_shape=(
            pltpu.VMEM((atoms, channels), F32),
            pltpu.VMEM((atoms, length), F32),
        ),
        in_specs=[vmem] * 5,
        out_specs=(vmem, vmem),
        scratch_shapes=[
            pltpu.VMEM((atoms, length), BF16),
            pltpu.VMEM((atoms, length), BF16),
            pltpu.VMEM(((hb + nb) * atoms, W), F32),
            pltpu.VMEM((GROUP * W, W), F32),
            pltpu.VMEM((hb * atoms, W), F32),
            pltpu.VMEM((atoms // 2, (hb + 1) * W, 2 * W), BF16),
            pltpu.VMEM((nb * atoms, W), F32),
            pltpu.VMEM((chunks, every, length), BF16),
            pltpu.VMEM((every, channels), BF16),
            pltpu.VMEM((every, wide), F32),
            pltpu.VMEM((rows_p, every), BF16),
            pltpu.VMEM((atoms, rows_p), BF16),
            pltpu.VMEM((chunks, rows_p, length), BF16),
            pltpu.VMEM((per_block, span, W), F32),
            pltpu.VMEM((B * atoms, W), F32),
            pltpu.VMEM((8 * hb * atoms, W), F32),
            pltpu.VMEM((2, atoms, width), F32),
            pltpu.VMEM((2, atoms // 2, width), F32),
            pltpu.VMEM((2, chips, atoms // 2, width), F32),
            pltpu.VMEM((2, atoms, width), F32),
            dma((2,)),
            dma((n_atom - 1,)),
            dma((n_atom - 1,)),
            dma((n_atom - 1, chunks)),
            dma((n_atom - 1, chunks)),
            dma((2,)),
            dma((2,)),
            dma((2, chips - 1)),
            dma((2, chips - 1)),
            dma((2,)),
            dma((2,)),
        ],
        compiler_params=pltpu.CompilerParams(collective_id=0, has_side_effects=True),
    )(signal, spatial, temporal, values, mask.T)


def solution(mesh):
    in_specs = (P(None, "tm"), P("atom", None), P("atom", None), P("atom", "tm"), P("atom", "tm"))
    out_specs = (P("atom", None), P("atom", None))
    body = functools.partial(local, mesh.shape["atom"], mesh.shape["tm"])
    return jax.shard_map(body, mesh=mesh, in_specs=in_specs, out_specs=out_specs, check_vma=False)
```

```python
import functools
import math

import jax
import jax.numpy as jnp
from jax import lax
from jax.experimental import pallas as pl
from jax.experimental.pallas import tpu as pltpu
from jax.sharding import PartitionSpec as P

W = 128
B = 32
GROUP = 16
MESH = pl.DeviceIdType.MESH
F32 = jnp.float32
BF16 = jnp.bfloat16
STEPS = 32767.0
TINY = 2.0**-112


def kernel(
    n_atom, n_tm, factor,
    signal_ref, spatial_ref, temporal_ref, values_ref, mask_ref,
    out_sp_ref, out_tm_ref,
    tail, halo, cx, xt, wt, tbuf, cf, cbuf, sbuf, sp32, st, own_w, resb, pj, lt, gt,
    part, recv1, half, scale, total,
    halo_sems, s_send, s_recv, c_send, c_recv,
    p_send, p_recv, z_send, z_recv, f_send, f_recv,
):
    atoms, channels = spatial_ref.shape
    length = temporal_ref.shape[1]
    samples = signal_ref.shape[1]
    blocks = mask_ref.shape[0]
    block = samples // blocks
    nb = samples // W
    hb = length // W
    chunk = length
    chunks = samples // chunk
    per = chunk // W
    rows_p = st.shape[0]
    wide = sp32.shape[1]
    span = pj.shape[1] // atoms
    chips = n_tm // 2
    me_a = lax.axis_index("atom")
    me_t = lax.axis_index("tm")
    me_z = me_t // 2
    core = lax.rem(me_t, 2)
    partner = me_z * 2 + 1 - core
    a_peers = [lax.rem(me_a + d, n_atom) for d in range(1, n_atom)]
    t_peers = [lax.rem(me_t + d, n_tm) for d in range(1, n_tm)]
    z_peers = [lax.rem(me_z + d, chips) for d in range(1, chips)]
    mine = pl.ds(pl.multiple_of(me_a * atoms, atoms), atoms)

    barrier = pltpu.get_barrier_semaphore()
    for peer in a_peers:
        pl.semaphore_signal(barrier, inc=1, device_id={"atom": peer}, device_id_type=MESH)
    for peer in t_peers:
        pl.semaphore_signal(barrier, inc=1, device_id={"tm": peer}, device_id_type=MESH)

    groups = atoms // 8

    def put(ref, count, b, value):
        for g in range(groups):
            ref[(g * count + b) * 8 : (g * count + b + 1) * 8, :] = value[8 * g : 8 * g + 8]

    def natural(ref, count, b):
        return jnp.concatenate(
            [ref[(g * count + b) * 8 : (g * count + b + 1) * 8, :] for g in range(groups)], axis=0
        )

    def series(ref, count, g, i, first, size):
        return ref[pl.ds((g * count + first) * 8 + i, size, stride=8), :]

    mask = mask_ref[...].astype(F32).T
    codes = [
        values_ref[:, j * block : (j + 1) * block].astype(F32) * mask[:, j : j + 1]
        for j in range(blocks)
    ]
    codes = jnp.concatenate(codes, axis=1)
    tail[...] = codes[:, samples - length :].astype(BF16)
    for b in range(hb):
        put(cx, hb + nb, b, jnp.zeros((atoms, W), F32))
    for b in range(nb):
        put(cx, hb + nb, hb + b, codes[:, b * W : (b + 1) * W])
    for d in range(hb):
        wt[d * atoms : (d + 1) * atoms, :] = temporal_ref[:, d * W : (d + 1) * W].astype(F32)

    row = lax.broadcasted_iota(jnp.int32, (W, W), 0)
    col = lax.broadcasted_iota(jnp.int32, (W, W), 1)
    ahead = col >= row

    def toeplitz(rows, i):
        circ = [
            pltpu.roll(
                jnp.broadcast_to(rows[d][i : i + 1], (W, W)), 0, 1, stride=1, stride_axis=0
            )
            for d in range(hb)
        ]
        zero = jnp.zeros((W, W), F32)
        parts = []
        for d in range(hb, -1, -1):
            near = circ[d] if d < hb else zero
            far = circ[d - 1] if d > 0 else zero
            parts.append(jnp.where(ahead, near, far))
        return jnp.concatenate(parts, axis=0)

    def windows(g, i):
        return jnp.concatenate(
            [series(cx, hb + nb, g, i, j, nb) for j in range(hb + 1)], axis=1
        )

    def apply(g, i, taps):
        lhs = jnp.concatenate([windows(g, i), windows(g, i + 1)], axis=0).astype(BF16)
        out = jnp.dot(lhs, taps, preferred_element_type=F32)
        cf[pl.ds(g * nb * 8 + i, nb, stride=8), :] = out[:nb, :W]
        cf[pl.ds(g * nb * 8 + i + 1, nb, stride=8), :] = out[nb:, W:]

    def first(g, carry):
        rows = [
            wt[pl.ds(pl.multiple_of(d * atoms + 8 * g, 8), 8), :] for d in range(hb)
        ]
        for i in range(0, 8, 2):
            taps = jnp.concatenate([toeplitz(rows, i), toeplitz(rows, i + 1)], axis=1).astype(BF16)
            tbuf[g * 4 + i // 2] = taps
            apply(g, i, taps)
        return carry

    def again(g, carry):
        for i in range(0, 8, 2):
            apply(g, i, tbuf[g * 4 + i // 2])
        return carry

    lax.fori_loop(0, groups, first, 0)

    pl.semaphore_wait(barrier, n_atom - 1 + n_tm - 1)

    right = lax.rem(me_t + 1, n_tm)
    halo_copy = pltpu.make_async_remote_copy(
        src_ref=tail, dst_ref=halo, send_sem=halo_sems.at[0], recv_sem=halo_sems.at[1],
        device_id={"tm": right}, device_id_type=MESH,
    )

    @pl.when(me_t < n_tm - 1)
    def _():
        halo_copy.start()

    c_copies = [[None] * (n_atom - 1) for _ in range(chunks)]

    def send(c):
        for b in range(per):
            at = c * per + b
            cbuf[c, mine, b * W : (b + 1) * W] = natural(cf, nb, at).astype(BF16)
        for d, peer in enumerate(a_peers):
            copy = pltpu.make_async_remote_copy(
                src_ref=cbuf.at[c, mine], dst_ref=cbuf.at[c, mine],
                send_sem=c_send.at[d, c], recv_sem=c_recv.at[d, c],
                device_id={"atom": peer}, device_id_type=MESH,
            )
            copy.start()
            c_copies[c][d] = copy

    s_copies = []
    for d, peer in enumerate(a_peers):
        copy = pltpu.make_async_remote_copy(
            src_ref=spatial_ref, dst_ref=sbuf.at[mine], send_sem=s_send.at[d],
            recv_sem=s_recv.at[d], device_id={"atom": peer}, device_id_type=MESH,
        )
        copy.start()
        s_copies.append(copy)
    for c in range(1, chunks):
        send(c)

    def lay_time(b, value):
        turned = value.T
        for u in range(W // 8):
            at = (u * GROUP + b) * 8
            xt[at : at + 8, :atoms] = turned[8 * u : 8 * u + 8]

    for b in range(nb):
        lay_time(hb + b, codes[:, b * W : (b + 1) * W])
    for u in range(W // 8):
        xt[(u * GROUP + hb + nb) * 8 : (u + 1) * GROUP * 8, :] = jnp.zeros(
            ((GROUP - hb - nb) * 8, W), F32
        )
    pj[...] = jnp.zeros(pj.shape, F32)
    resb[:, channels // 16 * 16 :, :] = jnp.zeros(
        (chunks, rows_p - channels // 16 * 16, chunk), BF16
    )
    sp32[...] = jnp.zeros(sp32.shape, F32)

    @pl.when(me_t == 0)
    def _():
        halo[...] = jnp.zeros(halo.shape, halo.dtype)

    @pl.when(me_t > 0)
    def _():
        halo_copy.wait_recv()

    before = halo[...].astype(F32)
    for b in range(hb):
        put(cx, hb + nb, b, before[:, b * W : (b + 1) * W])
    lax.fori_loop(0, groups, again, 0)
    send(0)
    for b in range(hb):
        lay_time(b, before[:, b * W : (b + 1) * W])

    per_block = W // B

    def lay(n, carry):
        for i in range(8):
            picked = jnp.concatenate(
                [
                    xt[pl.ds((B // 8 * r + B // 8 - 1 - n) * GROUP * 8 + 7 - i, GROUP, stride=8), :]
                    for r in range(per_block)
                ],
                axis=0,
            ).T
            for g in range(groups):
                at = pl.multiple_of((g * B + 8 * n + i) * 8, 8)
                lt[pl.ds(at, 8), : per_block * GROUP] = picked[8 * g : 8 * g + 8]
        return carry

    lax.fori_loop(0, B // 8, lay, 0)

    sbuf[mine, :] = spatial_ref[...]
    for copy in s_copies:
        copy.wait_recv()
    sp32[:, :channels] = sbuf[...].astype(F32)
    st[...] = sp32[...].T[:rows_p].astype(BF16)
    own_w[...] = sp32[mine, :rows_p].astype(BF16)

    def process(c, gsp):
        for copy in c_copies[c]:
            copy.wait_recv()
        model = jnp.dot(st[...], cbuf[c], preferred_element_type=F32)
        resb[c, :channels, :] = (
            model[:channels] - signal_ref[:, c * chunk : (c + 1) * chunk].astype(F32)
        ).astype(BF16)
        residual = resb[c]
        projected = jnp.dot(own_w[...], residual, preferred_element_type=F32)
        projected = projected.astype(BF16).astype(F32)
        for b in range(per):
            at = hb + c * per + b
            put(pj.at[0], span, at, projected[:, b * W : (b + 1) * W])
        grad = lax.dot_general(
            cbuf[c, mine, :], residual, (((1,), (1,)), ((), ())), preferred_element_type=F32
        )
        return grad if gsp is None else gsp + grad

    gsp = None
    for c in list(range(1, chunks)) + [0]:
        gsp = process(c, gsp)

    low = pl.ds(pl.multiple_of(core * (atoms // 2), atoms // 2), atoms // 2)
    other = pl.ds(pl.multiple_of((1 - core) * (atoms // 2), atoms // 2), atoms // 2)

    def swap(i, lanes):
        copy = pltpu.make_async_remote_copy(
            src_ref=part.at[i, other, lanes], dst_ref=recv1.at[i, :, lanes],
            send_sem=p_send.at[i], recv_sem=p_recv.at[i],
            device_id={"tm": partner}, device_id_type=MESH,
        )
        copy.start()
        return copy

    def spread(i, lanes, copy):
        copy.wait_recv()
        value = part[i, low, lanes] + recv1[i, :, lanes]
        top = jnp.max(jnp.abs(value), axis=0, keepdims=True)
        up = jnp.where(top > TINY, STEPS / jnp.maximum(top, TINY), 0.0)
        shift = jnp.where(value < 0, -0.5, 0.5)
        half[i, me_z, :, lanes] = (value * up + shift).astype(jnp.int32).astype(jnp.int16)
        scale[i, me_z, :, lanes] = top * (1.0 / STEPS)
        copies = []
        for d, peer in enumerate(z_peers):
            for n, ref in enumerate((half, scale)):
                out = pltpu.make_async_remote_copy(
                    src_ref=ref.at[i, me_z, :, lanes], dst_ref=ref.at[i, me_z, :, lanes],
                    send_sem=z_send.at[i, n, d], recv_sem=z_recv.at[i, n, d],
                    device_id={"tm": peer * 2 + core}, device_id_type=MESH,
                )
                out.start()
                copies.append(out)
        return copies

    def finish(i, lanes, copies):
        for copy in copies:
            copy.wait_recv()
        acc = None
        for z in range(chips):
            value = half[i, z, :, lanes].astype(jnp.int32).astype(F32) * scale[i, z, :, lanes]
            acc = value if acc is None else acc + value
        total[i, low, lanes] = acc * factor
        copy = pltpu.make_async_remote_copy(
            src_ref=total.at[i, low, lanes], dst_ref=total.at[i, low, lanes],
            send_sem=f_send.at[i], recv_sem=f_recv.at[i],
            device_id={"tm": partner}, device_id_type=MESH,
        )
        copy.start()
        return copy

    sp_lanes = slice(0, wide)
    tm_lanes = slice(0, length)
    part[0, :, :rows_p] = gsp
    if rows_p < wide:
        part[0, :, rows_p:] = jnp.zeros((atoms, wide - rows_p), F32)
    swap_sp = swap(0, sp_lanes)

    lane = lax.broadcasted_iota(jnp.int32, (atoms, W), 1)
    for r in range(1, per_block):
        turned = [
            pltpu.roll(natural(pj.at[0], span, i), W - B * r, 1)
            for i in range(hb, hb + nb)
        ]
        turned = [jnp.zeros((atoms, W), F32)] + turned + [jnp.zeros((atoms, W), F32)]
        for n in range(nb + 1):
            put(
                pj.at[r], span, hb - 1 + n,
                jnp.where(lane < W - B * r, turned[n], turned[n + 1]),
            )

    spread_sp = spread(0, sp_lanes, swap_sp)

    depth = (length + B - 1) // W + 1

    def correlate(g, carry):
        for i in range(8):
            lhs = series(lt, B, g, i, 0, B)[:, : per_block * GROUP].astype(BF16)
            rhs = jnp.concatenate(
                [
                    jnp.concatenate(
                        [series(pj.at[r], span, g, i, j, GROUP) for r in range(per_block)], axis=0
                    )
                    for j in range(depth)
                ],
                axis=1,
            ).astype(BF16)
            prod = jnp.dot(lhs, rhs, preferred_element_type=F32)
            prod = pltpu.roll(prod, depth * W - (B - 1), 1, stride=1, stride_axis=0)[:, :length]
            acc = prod[:8]
            for q in range(1, B // 8):
                acc = acc + prod[8 * q : 8 * q + 8]
            for d in range(hb):
                at = pl.multiple_of((d * groups + g) * 64 + 8 * i, 8)
                gt[pl.ds(at, 8), :] = acc[:, d * W : (d + 1) * W]
        return carry

    lax.fori_loop(0, groups, correlate, 0)
    for d in range(hb):
        gtm = gt[pl.ds(8 * d * atoms, atoms, stride=8), :]
        for i in range(1, 8):
            gtm = gtm + gt[pl.ds(8 * d * atoms + i, atoms, stride=8), :]
        part[1, :, d * W : (d + 1) * W] = gtm
    swap_tm = swap(1, tm_lanes)
    spread_tm = spread(1, tm_lanes, swap_tm)
    last_sp = finish(0, sp_lanes, spread_sp)
    last_tm = finish(1, tm_lanes, spread_tm)
    last_sp.wait_recv()
    out_sp_ref[...] = total[0, :, :channels]
    last_tm.wait_recv()
    out_tm_ref[...] = total[1, :, :length]

    @pl.when(me_t < n_tm - 1)
    def _():
        halo_copy.wait_send()

    for copy in s_copies + [copy for line in c_copies for copy in line]:
        copy.wait_send()
    for copy in [swap_sp, swap_tm, last_sp, last_tm] + spread_sp + spread_tm:
        copy.wait_send()


def local(n_atom, n_tm, signal, spatial, temporal, values, mask):
    atoms, channels = spatial.shape
    length = temporal.shape[1]
    samples = signal.shape[1]
    chunks = samples // length
    nb, hb = samples // W, length // W
    wide = -(-channels // W) * W
    rows_p = -(-channels // 32) * 32
    per_block = W // B
    every = n_atom * atoms
    depth = (length + B - 1) // W + 1
    span = (GROUP + depth - 1) * atoms
    width = max(wide, length)
    chips = n_tm // 2
    factor = 1.0 / math.sqrt(samples * n_tm)
    dma = pltpu.SemaphoreType.DMA
    vmem = pl.BlockSpec(memory_space=pltpu.VMEM)
    return pl.pallas_call(
        functools.partial(kernel, n_atom, n_tm, factor),
        out_shape=(
            pltpu.VMEM((atoms, channels), F32),
            pltpu.VMEM((atoms, length), F32),
        ),
        in_specs=[vmem] * 5,
        out_specs=(vmem, vmem),
        scratch_shapes=[
            pltpu.VMEM((atoms, length), BF16),
            pltpu.VMEM((atoms, length), BF16),
            pltpu.VMEM(((hb + nb) * atoms, W), F32),
            pltpu.VMEM((GROUP * W, W), F32),
            pltpu.VMEM((hb * atoms, W), F32),
            pltpu.VMEM((atoms // 2, (hb + 1) * W, 2 * W), BF16),
            pltpu.VMEM((nb * atoms, W), F32),
            pltpu.VMEM((chunks, every, length), BF16),
            pltpu.VMEM((every, channels), BF16),
            pltpu.VMEM((every, wide), F32),
            pltpu.VMEM((rows_p, every), BF16),
            pltpu.VMEM((atoms, rows_p), BF16),
            pltpu.VMEM((chunks, rows_p, length), BF16),
            pltpu.VMEM((per_block, span, W), F32),
            pltpu.VMEM((B * atoms, W), F32),
            pltpu.VMEM((8 * hb * atoms, W), F32),
            pltpu.VMEM((2, atoms, width), F32),
            pltpu.VMEM((2, atoms // 2, width), F32),
            pltpu.VMEM((2, chips, atoms // 2, width), jnp.int16),
            pltpu.VMEM((2, chips, 1, width), F32),
            pltpu.VMEM((2, atoms, width), F32),
            dma((2,)),
            dma((n_atom - 1,)),
            dma((n_atom - 1,)),
            dma((n_atom - 1, chunks)),
            dma((n_atom - 1, chunks)),
            dma((2,)),
            dma((2,)),
            dma((2, 2, chips - 1)),
            dma((2, 2, chips - 1)),
            dma((2,)),
            dma((2,)),
        ],
        compiler_params=pltpu.CompilerParams(collective_id=0, has_side_effects=True),
    )(signal, spatial, temporal, values, mask.T)


def solution(mesh):
    in_specs = (P(None, "tm"), P("atom", None), P("atom", None), P("atom", "tm"), P("atom", "tm"))
    out_specs = (P("atom", None), P("atom", None))
    body = functools.partial(local, mesh.shape["atom"], mesh.shape["tm"])
    return jax.shard_map(body, mesh=mesh, in_specs=in_specs, out_specs=out_specs, check_vma=False)
```

```python
import functools
import math

import jax
import jax.numpy as jnp
from jax import lax
from jax.experimental import pallas as pl
from jax.experimental.pallas import tpu as pltpu
from jax.sharding import PartitionSpec as P

W = 128
B = 32
GROUP = 16
MESH = pl.DeviceIdType.MESH
F32 = jnp.float32
BF16 = jnp.bfloat16
STEPS = 32767.0
TINY = 2.0**-112


def kernel(
    n_atom, n_tm, factor,
    signal_ref, spatial_ref, temporal_ref, values_ref, mask_ref,
    out_sp_ref, out_tm_ref,
    tail, halo, spill, spilled, cx, xt, wt, cf, cbuf, sbuf, sp32, st, own_w, resb, pj, lt, gt,
    part, recv1, half, scale, total,
    halo_sems, s_send, s_recv, h_send, h_recv, c_send, c_recv,
    p_send, p_recv, z_send, z_recv, f_send, f_recv,
):
    atoms, channels = spatial_ref.shape
    length = temporal_ref.shape[1]
    samples = signal_ref.shape[1]
    blocks = mask_ref.shape[0]
    block = samples // blocks
    nb = samples // W
    hb = length // W
    chunk = length
    chunks = samples // chunk
    per = chunk // W
    rows_p = st.shape[0]
    wide = sp32.shape[1]
    span = pj.shape[1] // atoms
    chips = n_tm // 2
    me_a = lax.axis_index("atom")
    me_t = lax.axis_index("tm")
    me_z = me_t // 2
    core = lax.rem(me_t, 2)
    partner = me_z * 2 + 1 - core

    def across(at, count):
        def flip(d):
            out = at
            for bit in range(d.bit_length()):
                if d >> bit & 1:
                    step = 1 << bit
                    out = out + step - 2 * step * lax.rem(at // step, 2)
            return out

        if count & (count - 1) == 0:
            return [flip(d) for d in range(count - 1, 0, -1)]
        return [lax.rem(at + d, count) for d in range(1, count)]

    def sources(at, count):
        if count & (count - 1) == 0:
            return across(at, count)
        return [lax.rem(at + count - d, count) for d in range(1, count)]

    a_peers = across(me_a, n_atom)
    t_peers = [lax.rem(me_t + d, n_tm) for d in range(1, n_tm)]
    z_peers = across(me_z, chips)
    mine = pl.ds(pl.multiple_of(me_a * atoms, atoms), atoms)

    barrier = pltpu.get_barrier_semaphore()
    for peer in a_peers:
        pl.semaphore_signal(barrier, inc=1, device_id={"atom": peer}, device_id_type=MESH)
    for peer in t_peers:
        pl.semaphore_signal(barrier, inc=1, device_id={"tm": peer}, device_id_type=MESH)

    groups = atoms // 8

    def put(ref, count, b, value):
        for g in range(groups):
            ref[(g * count + b) * 8 : (g * count + b + 1) * 8, :] = value[8 * g : 8 * g + 8]

    def filtered(b, lo, hi):
        return jnp.concatenate(
            [
                cf[pl.ds((g * (GROUP // 8) + b // 8) * 64 + b % 8, 8, stride=8), :]
                for g in range(lo, hi)
            ],
            axis=0,
        )

    def natural(ref, count, b):
        return jnp.concatenate(
            [ref[(g * count + b) * 8 : (g * count + b + 1) * 8, :] for g in range(groups)], axis=0
        )

    def series(ref, count, g, i, first, size):
        return ref[pl.ds((g * count + first) * 8 + i, size, stride=8), :]

    mask = mask_ref[...].astype(F32).T
    codes = [
        values_ref[:, j * block : (j + 1) * block].astype(F32) * mask[:, j : j + 1]
        for j in range(blocks)
    ]
    codes = jnp.concatenate(codes, axis=1)
    tail[...] = codes[:, samples - length :].astype(BF16)
    gap = jnp.zeros((atoms, W), F32)
    for b in list(range(hb)) + list(range(hb + nb, GROUP + hb)):
        put(cx, GROUP + hb, b, gap)
    for b in range(nb):
        put(cx, GROUP + hb, hb + b, codes[:, b * W : (b + 1) * W])
    for d in range(hb):
        wt[d * atoms : (d + 1) * atoms, :] = temporal_ref[:, d * W : (d + 1) * W].astype(F32)

    row = lax.broadcasted_iota(jnp.int32, (W, W), 0)
    col = lax.broadcasted_iota(jnp.int32, (W, W), 1)
    ahead = col >= row

    def toeplitz(rows, i):
        circ = []
        for d in range(hb):
            base = jnp.broadcast_to(rows[d][i : i + 1], (GROUP, W))
            base = pltpu.roll(base, 0, 1, stride=1, stride_axis=0).astype(BF16)
            tiles = [base] + [pltpu.roll(base, GROUP * n, 1) for n in range(1, W // GROUP)]
            circ.append(jnp.concatenate(tiles, axis=0))
        zero = jnp.zeros((W, W), BF16)
        parts = []
        for d in range(hb, -1, -1):
            near = circ[d] if d < hb else zero
            far = circ[d - 1] if d > 0 else zero
            parts.append(jnp.where(ahead, near, far))
        return jnp.concatenate(parts, axis=0)

    def windows(g, i):
        return jnp.concatenate(
            [series(cx, GROUP + hb, g, i, j, GROUP) for j in range(hb + 1)], axis=1
        )

    def first(g, carry):
        rows = [
            wt[pl.ds(pl.multiple_of(d * atoms + 8 * g, 8), 8), :] for d in range(hb)
        ]
        for i in range(0, 8, 2):
            taps = jnp.concatenate([toeplitz(rows, i), toeplitz(rows, i + 1)], axis=1)
            lhs = jnp.concatenate([windows(g, i), windows(g, i + 1)], axis=0).astype(BF16)
            out = jnp.dot(lhs, taps, preferred_element_type=F32)
            for n in range(2):
                for h in range(GROUP // 8):
                    at = pl.multiple_of(((g * (GROUP // 8) + h) * 8 + i + n) * 8, 8)
                    row = n * GROUP + 8 * h
                    cf[pl.ds(at, 8), :] = out[row : row + 8, n * W : (n + 1) * W]
        return carry

    lax.fori_loop(0, groups // 2, first, 0, unroll=4)

    pl.semaphore_wait(barrier, n_atom - 1 + n_tm - 1)

    right = lax.rem(me_t + 1, n_tm)
    halo_copy = pltpu.make_async_remote_copy(
        src_ref=tail, dst_ref=halo, send_sem=halo_sems.at[0], recv_sem=halo_sems.at[1],
        device_id={"tm": right}, device_id_type=MESH,
    )

    spill_copy = pltpu.make_async_remote_copy(
        src_ref=spill, dst_ref=spilled, send_sem=halo_sems.at[2], recv_sem=halo_sems.at[3],
        device_id={"tm": right}, device_id_type=MESH,
    )
    @pl.when(me_t < n_tm - 1)
    def _():
        halo_copy.start()

    c_copies = [[] for _ in range(chunks)]

    def send(c, lo, hi):
        rows = pl.ds(pl.multiple_of(me_a * atoms + 8 * lo, 8 * (hi - lo)), 8 * (hi - lo))
        for b in range(per):
            value = filtered(c * per + b, lo, hi)
            if c == 0:
                value = value + spilled[8 * lo : 8 * hi, b * W : (b + 1) * W]
            cbuf[c, rows, b * W : (b + 1) * W] = value.astype(BF16)
        for d, peer in enumerate(a_peers):
            copy = pltpu.make_async_remote_copy(
                src_ref=cbuf.at[c, rows], dst_ref=cbuf.at[c, rows],
                send_sem=c_send.at[d, c, 2 * lo // groups], recv_sem=c_recv.at[d, c, 2 * lo // groups],
                device_id={"atom": peer}, device_id_type=MESH,
            )
            copy.start()
            c_copies[c].append(copy)

    s_copies = []
    own_half = pl.ds(pl.multiple_of(core * (atoms // 2), atoms // 2), atoms // 2)

    def half_of(peer):
        at = peer * atoms + core * (atoms // 2)
        return pl.ds(pl.multiple_of(at, atoms // 2), atoms // 2)

    for d, peer in enumerate(a_peers):
        copy = pltpu.make_async_remote_copy(
            src_ref=spatial_ref.at[own_half], dst_ref=sbuf.at[half_of(me_a)],
            send_sem=s_send.at[d], recv_sem=s_recv.at[d],
            device_id={"atom": peer}, device_id_type=MESH,
        )
        copy.start()
        s_copies.append(copy)
    for c in range(1, chunks):
        send(c, 0, groups // 2)
    lax.fori_loop(groups // 2, groups, first, 0, unroll=4)
    for b in range(hb):
        spill[:, b * W : (b + 1) * W] = filtered(nb + b, 0, groups)

    @pl.when(me_t < n_tm - 1)
    def _():
        spill_copy.start()

    for c in range(1, chunks):
        send(c, groups // 2, groups)

    def lay_time(b, value):
        turned = value.T
        for u in range(W // 8):
            at = (u * GROUP + b) * 8
            xt[at : at + 8, :atoms] = turned[8 * u : 8 * u + 8]

    for b in range(nb):
        lay_time(hb + b, codes[:, b * W : (b + 1) * W])
    for u in range(W // 8):
        xt[(u * GROUP + hb + nb) * 8 : (u + 1) * GROUP * 8, :] = jnp.zeros(
            ((GROUP - hb - nb) * 8, W), F32
        )
    pj[...] = jnp.zeros(pj.shape, F32)
    resb[:, channels // 16 * 16 :, :] = jnp.zeros(
        (chunks, rows_p - channels // 16 * 16, chunk), BF16
    )
    sp32[...] = jnp.zeros(sp32.shape, F32)

    @pl.when(me_t == 0)
    def _():
        halo[...] = jnp.zeros(halo.shape, halo.dtype)
        spilled[...] = jnp.zeros(spilled.shape, F32)

    @pl.when(me_t > 0)
    def _():
        spill_copy.wait_recv()

    send(0, 0, groups)

    sbuf[mine, :] = spatial_ref[...]
    passed = []
    for d, source in enumerate(sources(me_a, n_atom)):
        s_copies[d].wait_recv()
        rows = half_of(source)
        out = pltpu.make_async_remote_copy(
            src_ref=sbuf.at[rows], dst_ref=sbuf.at[rows],
            send_sem=h_send.at[d], recv_sem=h_recv.at[d],
            device_id={"tm": partner}, device_id_type=MESH,
        )
        out.start()
        passed.append(out)

    @pl.when(me_t > 0)
    def _():
        halo_copy.wait_recv()

    before = halo[...].astype(F32)
    for b in range(hb):
        lay_time(b, before[:, b * W : (b + 1) * W])

    per_block = W // B
    deep = per_block * GROUP
    slots = W // deep
    place = lax.rem(lax.broadcasted_iota(jnp.int32, (8, W), 0), slots) == (
        lax.broadcasted_iota(jnp.int32, (8, W), 1) // deep
    )

    def lay(n, carry):
        for i in range(8):
            picked = [
                xt[pl.ds((B // 8 * r + B // 8 - 1 - n) * GROUP * 8 + 7 - i, GROUP, stride=8), :]
                for r in range(per_block)
            ]
            picked = jnp.concatenate(picked * (W // deep), axis=0).T
            for g in range(groups):
                at = pl.multiple_of((g * B + 8 * n + i) * 8, 8)
                lt[pl.ds(at, 8), :] = jnp.where(place, picked[8 * g : 8 * g + 8], 0.0)
        return carry

    lax.fori_loop(0, B // 8, lay, 0)

    for copy in passed:
        copy.wait_recv()
    sp32[:, :channels] = sbuf[...].astype(F32)
    st[...] = sp32[...].T[:rows_p].astype(BF16)
    own_w[...] = sp32[mine, :rows_p].astype(BF16)

    def process(c, gsp):
        for copy in c_copies[c]:
            copy.wait_recv()
        model = jnp.dot(st[...], cbuf[c], preferred_element_type=F32)
        resb[c, :channels, :] = (
            model[:channels] - signal_ref[:, c * chunk : (c + 1) * chunk].astype(F32)
        ).astype(BF16)
        residual = resb[c]
        projected = jnp.dot(own_w[...], residual, preferred_element_type=F32)
        projected = projected.astype(BF16).astype(F32)
        for b in range(per):
            at = hb + c * per + b
            put(pj.at[0], span, at, projected[:, b * W : (b + 1) * W])
        grad = lax.dot_general(
            cbuf[c, mine, :], residual, (((1,), (1,)), ((), ())), preferred_element_type=F32
        )
        return grad if gsp is None else gsp + grad

    gsp = None
    for c in list(range(1, chunks)) + [0]:
        gsp = process(c, gsp)

    low = pl.ds(pl.multiple_of(core * (atoms // 2), atoms // 2), atoms // 2)
    other = pl.ds(pl.multiple_of((1 - core) * (atoms // 2), atoms // 2), atoms // 2)

    def swap(i, lanes):
        copy = pltpu.make_async_remote_copy(
            src_ref=part.at[i, other, lanes], dst_ref=recv1.at[i, :, lanes],
            send_sem=p_send.at[i], recv_sem=p_recv.at[i],
            device_id={"tm": partner}, device_id_type=MESH,
        )
        copy.start()
        return copy

    def spread(i, lanes, copy):
        copy.wait_recv()
        value = part[i, low, lanes] + recv1[i, :, lanes]
        top = jnp.max(jnp.abs(value), axis=0, keepdims=True)
        up = jnp.where(top > TINY, STEPS / jnp.maximum(top, TINY), 0.0)
        shift = jnp.where(value < 0, -0.5, 0.5)
        half[i, me_z, :, lanes] = (value * up + shift).astype(jnp.int32).astype(jnp.int16)
        scale[i, me_z, :, lanes] = top * (1.0 / STEPS)
        copies = []
        for d, peer in enumerate(z_peers):
            for n, ref in enumerate((half, scale)):
                out = pltpu.make_async_remote_copy(
                    src_ref=ref.at[i, me_z, :, lanes], dst_ref=ref.at[i, me_z, :, lanes],
                    send_sem=z_send.at[i, n, d], recv_sem=z_recv.at[i, n, d],
                    device_id={"tm": peer * 2 + core}, device_id_type=MESH,
                )
                out.start()
                copies.append(out)
        return copies

    def finish(i, lanes, copies):
        for copy in copies:
            copy.wait_recv()
        acc = None
        for z in range(chips):
            value = half[i, z, :, lanes].astype(jnp.int32).astype(F32) * scale[i, z, :, lanes]
            acc = value if acc is None else acc + value
        total[i, low, lanes] = acc * factor
        copy = pltpu.make_async_remote_copy(
            src_ref=total.at[i, low, lanes], dst_ref=total.at[i, low, lanes],
            send_sem=f_send.at[i], recv_sem=f_recv.at[i],
            device_id={"tm": partner}, device_id_type=MESH,
        )
        copy.start()
        return copy

    sp_lanes = slice(0, wide)
    tm_lanes = slice(0, length)
    part[0, :, :rows_p] = gsp
    if rows_p < wide:
        part[0, :, rows_p:] = jnp.zeros((atoms, wide - rows_p), F32)
    swap_sp = swap(0, sp_lanes)

    lane = lax.broadcasted_iota(jnp.int32, (atoms, W), 1)
    for r in range(1, per_block):
        turned = [
            pltpu.roll(natural(pj.at[0], span, i), W - B * r, 1)
            for i in range(hb, hb + nb)
        ]
        turned = [jnp.zeros((atoms, W), F32)] + turned + [jnp.zeros((atoms, W), F32)]
        for n in range(nb + 1):
            put(
                pj.at[r], span, hb - 1 + n,
                jnp.where(lane < W - B * r, turned[n], turned[n + 1]),
            )

    depth = (length + B - 1) // W + 1

    def correlate(g, carry):
        for first_atom in range(0, 8, 2 * slots):
            some = range(first_atom, first_atom + 2 * slots)
            lhs = []
            rhs = []
            for i in some:
                left = series(lt, B, g, i, 0, B).astype(BF16)
                none = jnp.zeros((B, W), BF16)
                pair = [left, none] if i - first_atom < slots else [none, left]
                lhs.append(jnp.concatenate(pair, axis=1))
                for r in range(per_block):
                    rhs.append(
                        jnp.concatenate(
                            [series(pj.at[r], span, g, i, j, GROUP) for j in range(depth)], axis=1
                        )
                    )
            prods = jnp.dot(
                jnp.concatenate(lhs, axis=0),
                jnp.concatenate(rhs, axis=0).astype(BF16),
                preferred_element_type=F32,
            )
            for n, i in enumerate(some):
                prod = prods[n * B : (n + 1) * B]
                prod = pltpu.roll(prod, depth * W - (B - 1), 1, stride=1, stride_axis=0)
                acc = prod[:8, :length]
                for q in range(1, B // 8):
                    acc = acc + prod[8 * q : 8 * q + 8, :length]
                for d in range(hb):
                    at = pl.multiple_of((d * groups + g) * 64 + 8 * i, 8)
                    gt[pl.ds(at, 8), :] = acc[:, d * W : (d + 1) * W]
        return carry

    def lags(mine_first, rows):
        for d in range(hb):
            at = 8 * (d * atoms + mine_first)
            total_d = gt[pl.ds(at, atoms // 2, stride=8), :]
            for i in range(1, 8):
                total_d = total_d + gt[pl.ds(at + i, atoms // 2, stride=8), :]
            part[1, rows, d * W : (d + 1) * W] = total_d

    def correlate_from(start, count):
        lax.fori_loop(0, count, lambda n, carry: correlate(start + n, carry), 0, unroll=count)

    correlate_from((1 - core) * (groups // 2), groups // 2)
    lags((1 - core) * (atoms // 2), other)
    swap_tm = swap(1, tm_lanes)
    correlate_from(core * (groups // 2), groups // 4)
    spread_sp = spread(0, sp_lanes, swap_sp)
    correlate_from(core * (groups // 2) + groups // 4, groups // 4)
    lags(core * (atoms // 2), low)
    spread_tm = spread(1, tm_lanes, swap_tm)
    last_sp = finish(0, sp_lanes, spread_sp)
    last_tm = finish(1, tm_lanes, spread_tm)
    last_sp.wait_recv()
    out_sp_ref[...] = total[0, :, :channels]
    last_tm.wait_recv()
    out_tm_ref[...] = total[1, :, :length]

    @pl.when(me_t < n_tm - 1)
    def _():
        halo_copy.wait_send()
        spill_copy.wait_send()

    for copy in s_copies + passed + [copy for line in c_copies for copy in line]:
        copy.wait_send()
    for copy in [swap_sp, swap_tm, last_sp, last_tm] + spread_sp + spread_tm:
        copy.wait_send()


def local(n_atom, n_tm, signal, spatial, temporal, values, mask):
    atoms, channels = spatial.shape
    length = temporal.shape[1]
    samples = signal.shape[1]
    chunks = samples // length
    nb, hb = samples // W, length // W
    wide = -(-channels // W) * W
    rows_p = -(-channels // 32) * 32
    per_block = W // B
    deep = per_block * GROUP
    slots = W // deep
    place = lax.rem(lax.broadcasted_iota(jnp.int32, (8, W), 0), slots) == (
        lax.broadcasted_iota(jnp.int32, (8, W), 1) // deep
    )
    every = n_atom * atoms
    depth = (length + B - 1) // W + 1
    span = (GROUP + depth - 1) * atoms
    width = max(wide, length)
    chips = n_tm // 2
    factor = 1.0 / math.sqrt(samples * n_tm)
    dma = pltpu.SemaphoreType.DMA
    vmem = pl.BlockSpec(memory_space=pltpu.VMEM)
    return pl.pallas_call(
        functools.partial(kernel, n_atom, n_tm, factor),
        out_shape=(
            pltpu.VMEM((atoms, channels), F32),
            pltpu.VMEM((atoms, length), F32),
        ),
        in_specs=[vmem] * 5,
        out_specs=(vmem, vmem),
        scratch_shapes=[
            pltpu.VMEM((atoms, length), BF16),
            pltpu.VMEM((atoms, length), BF16),
            pltpu.VMEM((atoms, length), F32),
            pltpu.VMEM((atoms, length), F32),
            pltpu.VMEM(((GROUP + hb) * atoms, W), F32),
            pltpu.VMEM((GROUP * W, W), F32),
            pltpu.VMEM((hb * atoms, W), F32),
            pltpu.VMEM((GROUP * atoms, W), F32),
            pltpu.VMEM((chunks, every, length), BF16),
            pltpu.VMEM((every, channels), BF16),
            pltpu.VMEM((every, wide), F32),
            pltpu.VMEM((rows_p, every), BF16),
            pltpu.VMEM((atoms, rows_p), BF16),
            pltpu.VMEM((chunks, rows_p, length), BF16),
            pltpu.VMEM((per_block, span, W), F32),
            pltpu.VMEM((B * atoms, W), F32),
            pltpu.VMEM((8 * hb * atoms, W), F32),
            pltpu.VMEM((2, atoms, width), F32),
            pltpu.VMEM((2, atoms // 2, width), F32),
            pltpu.VMEM((2, chips, atoms // 2, width), jnp.int16),
            pltpu.VMEM((2, chips, 1, width), F32),
            pltpu.VMEM((2, atoms, width), F32),
            dma((4,)),
            dma((n_atom - 1,)),
            dma((n_atom - 1,)),
            dma((n_atom - 1,)),
            dma((n_atom - 1,)),
            dma((n_atom - 1, chunks, 2)),
            dma((n_atom - 1, chunks, 2)),
            dma((2,)),
            dma((2,)),
            dma((2, 2, chips - 1)),
            dma((2, 2, chips - 1)),
            dma((2,)),
            dma((2,)),
        ],
        compiler_params=pltpu.CompilerParams(collective_id=0, has_side_effects=True),
    )(signal, spatial, temporal, values, mask.T)


def solution(mesh):
    in_specs = (P(None, "tm"), P("atom", None), P("atom", None), P("atom", "tm"), P("atom", "tm"))
    out_specs = (P("atom", None), P("atom", None))
    body = functools.partial(local, mesh.shape["atom"], mesh.shape["tm"])
    return jax.shard_map(body, mesh=mesh, in_specs=in_specs, out_specs=out_specs, check_vma=False)
```

```python
import functools
import math

import jax
import jax.numpy as jnp
from jax import lax
from jax.experimental import pallas as pl
from jax.experimental.pallas import tpu as pltpu
from jax.sharding import PartitionSpec as P

W = 128
B = 32
GROUP = 16
SPLIT = 2
MESH = pl.DeviceIdType.MESH
F32 = jnp.float32
BF16 = jnp.bfloat16
STEPS = 32767.0
TINY = 2.0**-112


def kernel(
    n_atom, n_tm, factor,
    signal_ref, spatial_ref, temporal_ref, values_ref, mask_ref,
    out_sp_ref, out_tm_ref,
    tail, halo, spill, spilled, cx, xt, wt, cf, cbuf, sbuf, sp32, st, own_w, resb, pj, lt, gt,
    part, recv1, half, scale, total,
    heard, halo_sems, s_send, s_recv, h_send, h_recv, c_send, c_recv,
    p_send, p_recv, z_send, z_recv, f_send, f_recv,
):
    atoms, channels = spatial_ref.shape
    length = temporal_ref.shape[1]
    samples = signal_ref.shape[1]
    blocks = mask_ref.shape[0]
    block = samples // blocks
    nb = samples // W
    hb = length // W
    chunk = length
    chunks = samples // chunk
    per = chunk // W
    rows_p = st.shape[0]
    wide = sp32.shape[1]
    span = pj.shape[1] // atoms
    chips = n_tm // 2
    me_a = lax.axis_index("atom")
    me_t = lax.axis_index("tm")
    me_z = me_t // 2
    core = lax.rem(me_t, 2)
    partner = me_z * 2 + 1 - core

    def across(at, count):
        def flip(d):
            out = at
            for bit in range(d.bit_length()):
                if d >> bit & 1:
                    step = 1 << bit
                    out = out + step - 2 * step * lax.rem(at // step, 2)
            return out

        if count & (count - 1) == 0:
            return [flip(d) for d in range(count - 1, 0, -1)]
        return [lax.rem(at + d, count) for d in range(1, count)]

    def sources(at, count):
        if count & (count - 1) == 0:
            return across(at, count)
        return [lax.rem(at + count - d, count) for d in range(1, count)]

    a_peers = across(me_a, n_atom)
    z_peers = across(me_z, chips)
    mine = pl.ds(pl.multiple_of(me_a * atoms, atoms), atoms)

    barrier = pltpu.get_barrier_semaphore()
    for peer in a_peers:
        pl.semaphore_signal(barrier, inc=1, device_id={"atom": peer}, device_id_type=MESH)
    line = me_t - 1 + 2 * core
    beside = [
        (me_z > 0, me_t - 2),
        (me_z < chips - 1, me_t + 2),
        (jnp.logical_and(line >= 0, line < n_tm), line),
    ]

    def greet(peer):
        pl.semaphore_signal(barrier, inc=1, device_id={"tm": peer}, device_id_type=MESH)

    greet(partner)
    for there, peer in beside:
        pl.when(there)(functools.partial(greet, peer))

    def tell(turn):
        for n, (there, peer) in enumerate(beside[:2]):

            @pl.when(there)
            def _():
                pl.semaphore_signal(
                    heard.at[turn, 1 - n], inc=1, device_id={"tm": peer}, device_id_type=MESH
                )

    def listen(turn):
        for n, (there, peer) in enumerate(beside[:2]):

            @pl.when(there)
            def _():
                pl.semaphore_wait(heard.at[turn, n], 1)


    groups = atoms // 8

    def put(ref, count, b, value):
        for g in range(groups):
            ref[(g * count + b) * 8 : (g * count + b + 1) * 8, :] = value[8 * g : 8 * g + 8]

    def filtered(b, lo, hi):
        return jnp.concatenate(
            [
                cf[pl.ds((g * (GROUP // 8) + b // 8) * 64 + b % 8, 8, stride=8), :]
                for g in range(lo, hi)
            ],
            axis=0,
        )

    def natural(ref, count, b):
        return jnp.concatenate(
            [ref[(g * count + b) * 8 : (g * count + b + 1) * 8, :] for g in range(groups)], axis=0
        )

    def series(ref, count, g, i, first, size):
        return ref[pl.ds((g * count + first) * 8 + i, size, stride=8), :]

    mask = mask_ref[...].astype(F32).T
    codes = [
        values_ref[:, j * block : (j + 1) * block].astype(F32) * mask[:, j : j + 1]
        for j in range(blocks)
    ]
    codes = jnp.concatenate(codes, axis=1)
    tail[...] = codes[:, samples - length :].astype(BF16)
    gap = jnp.zeros((atoms, W), F32)
    for b in list(range(hb)) + list(range(hb + nb, GROUP + hb)):
        put(cx, GROUP + hb, b, gap)
    for b in range(nb):
        put(cx, GROUP + hb, hb + b, codes[:, b * W : (b + 1) * W])
    for d in range(hb):
        wt[d * atoms : (d + 1) * atoms, :] = temporal_ref[:, d * W : (d + 1) * W].astype(F32)

    row = lax.broadcasted_iota(jnp.int32, (W, W), 0)
    col = lax.broadcasted_iota(jnp.int32, (W, W), 1)
    ahead = col >= row

    def toeplitz(rows, i):
        circ = []
        for d in range(hb):
            base = jnp.broadcast_to(rows[d][i : i + 1], (GROUP, W))
            base = pltpu.roll(base, 0, 1, stride=1, stride_axis=0).astype(BF16)
            tiles = [base] + [pltpu.roll(base, GROUP * n, 1) for n in range(1, W // GROUP)]
            circ.append(jnp.concatenate(tiles, axis=0))
        zero = jnp.zeros((W, W), BF16)
        parts = []
        for d in range(hb, -1, -1):
            near = circ[d] if d < hb else zero
            far = circ[d - 1] if d > 0 else zero
            parts.append(jnp.where(ahead, near, far))
        return jnp.concatenate(parts, axis=0)

    def windows(g, i):
        return jnp.concatenate(
            [series(cx, GROUP + hb, g, i, j, GROUP) for j in range(hb + 1)], axis=1
        )

    def first(g, carry):
        rows = [
            wt[pl.ds(pl.multiple_of(d * atoms + 8 * g, 8), 8), :] for d in range(hb)
        ]
        for i in range(0, 8, 2):
            taps = jnp.concatenate([toeplitz(rows, i), toeplitz(rows, i + 1)], axis=1)
            lhs = jnp.concatenate([windows(g, i), windows(g, i + 1)], axis=0).astype(BF16)
            out = jnp.dot(lhs, taps, preferred_element_type=F32)
            for n in range(2):
                for h in range(GROUP // 8):
                    at = pl.multiple_of(((g * (GROUP // 8) + h) * 8 + i + n) * 8, 8)
                    row = n * GROUP + 8 * h
                    cf[pl.ds(at, 8), :] = out[row : row + 8, n * W : (n + 1) * W]
        return carry

    lax.fori_loop(0, SPLIT * groups // 4 // 2 * 2, first, 0, unroll=4)

    present = n_atom
    for there, _ in beside:
        present = present + jnp.where(there, 1, 0)
    pl.semaphore_wait(barrier, present)
    if chips > 2:
        tell(0)

    right = lax.rem(me_t + 1, n_tm)
    halo_copy = pltpu.make_async_remote_copy(
        src_ref=tail, dst_ref=halo, send_sem=halo_sems.at[0], recv_sem=halo_sems.at[1],
        device_id={"tm": right}, device_id_type=MESH,
    )

    spill_copies = []

    def send_spill(n, lo, hi):
        rows = slice(8 * lo, 8 * hi)
        for b in range(hb):
            spill[rows, b * W : (b + 1) * W] = filtered(nb + b, lo, hi)
        copy = pltpu.make_async_remote_copy(
            src_ref=spill.at[rows], dst_ref=spilled.at[rows],
            send_sem=halo_sems.at[2 + n], recv_sem=halo_sems.at[4 + n],
            device_id={"tm": right}, device_id_type=MESH,
        )
        spill_copies.append(copy)

        @pl.when(me_t < n_tm - 1)
        def _():
            copy.start()

    c_copies = [[] for _ in range(chunks)]
    c_waits = [[] for _ in range(chunks)]
    firsts = {}
    relays = {1: (2, 1), 2: (1, 2)} if n_atom == 4 and chunks > 2 else {}

    def send(c, lo, hi):
        rows = pl.ds(pl.multiple_of(me_a * atoms + 8 * lo, 8 * (hi - lo)), 8 * (hi - lo))
        for b in range(per):
            value = filtered(c * per + b, lo, hi)
            if c == 0:
                value = value + spilled[8 * lo : 8 * hi, b * W : (b + 1) * W]
            cbuf[c, rows, b * W : (b + 1) * W] = value.astype(BF16)
        for d, peer in enumerate(a_peers):
            if c in relays and lo == 0 and d == 0:
                continue
            copy = pltpu.make_async_remote_copy(
                src_ref=cbuf.at[c, rows], dst_ref=cbuf.at[c, rows],
                send_sem=c_send.at[d, c, min(lo, 1)], recv_sem=c_recv.at[d, c, min(lo, 1)],
                device_id={"atom": peer}, device_id_type=MESH,
            )
            copy.start()
            c_copies[c].append(copy)
            c_waits[c].append(copy)
            firsts[c, d, min(lo, 1)] = copy

    def relay(c):
        source, target = relays[c]
        copy = firsts[c, source, 0]
        copy.wait_recv()
        c_waits[c] = [other_copy for other_copy in c_waits[c] if other_copy is not copy]
        rows = pl.ds(pl.multiple_of(a_peers[source] * atoms, atoms), 8 * early)
        copy = pltpu.make_async_remote_copy(
            src_ref=cbuf.at[c, rows], dst_ref=cbuf.at[c, rows],
            send_sem=c_send.at[0, c, 0], recv_sem=c_recv.at[0, c, 0],
            device_id={"atom": a_peers[target]}, device_id_type=MESH,
        )
        copy.start()
        c_copies[c].append(copy)
        c_waits[c].append(copy)

    early = SPLIT * groups // 4 // 2 * 2
    send_spill(0, 0, early)

    @pl.when(me_t < n_tm - 1)
    def _():
        halo_copy.start()

    for c in relays:
        send(c, 0, early)

    s_copies = []
    own_half = pl.ds(pl.multiple_of(core * (atoms // 2), atoms // 2), atoms // 2)

    def half_of(peer):
        at = peer * atoms + core * (atoms // 2)
        return pl.ds(pl.multiple_of(at, atoms // 2), atoms // 2)

    for d, peer in enumerate(a_peers):
        copy = pltpu.make_async_remote_copy(
            src_ref=spatial_ref.at[own_half], dst_ref=sbuf.at[half_of(me_a)],
            send_sem=s_send.at[d], recv_sem=s_recv.at[d],
            device_id={"atom": peer}, device_id_type=MESH,
        )
        copy.start()
        s_copies.append(copy)
    for c in range(1, chunks):
        if c not in relays:
            send(c, 0, early)
    lax.fori_loop(early, groups, first, 0, unroll=4)
    send_spill(1, early, groups)
    for c in range(1, chunks):
        send(c, early, groups)

    def lay_time(b, value):
        turned = value.T
        for u in range(W // 8):
            at = (u * GROUP + b) * 8
            xt[at : at + 8, :atoms] = turned[8 * u : 8 * u + 8]

    for b in range(nb):
        lay_time(hb + b, codes[:, b * W : (b + 1) * W])
    for u in range(W // 8):
        xt[(u * GROUP + hb + nb) * 8 : (u + 1) * GROUP * 8, :] = jnp.zeros(
            ((GROUP - hb - nb) * 8, W), F32
        )
    pj[...] = jnp.zeros(pj.shape, F32)
    resb[:, channels // 16 * 16 :, :] = jnp.zeros(
        (chunks, rows_p - channels // 16 * 16, chunk), BF16
    )
    sp32[...] = jnp.zeros(sp32.shape, F32)

    for c in relays:
        relay(c)

    @pl.when(me_t == 0)
    def _():
        halo[...] = jnp.zeros(halo.shape, halo.dtype)
        spilled[...] = jnp.zeros(spilled.shape, F32)

    @pl.when(me_t > 0)
    def _():
        for copy in spill_copies:
            copy.wait_recv()

    send(0, 0, groups)
    if chips > 3:
        listen(0)
        tell(1)

    sbuf[mine, :] = spatial_ref[...]
    passed = []
    for d, source in enumerate(sources(me_a, n_atom)):
        s_copies[d].wait_recv()
        rows = half_of(source)
        out = pltpu.make_async_remote_copy(
            src_ref=sbuf.at[rows], dst_ref=sbuf.at[rows],
            send_sem=h_send.at[d], recv_sem=h_recv.at[d],
            device_id={"tm": partner}, device_id_type=MESH,
        )
        out.start()
        passed.append(out)

    @pl.when(me_t > 0)
    def _():
        halo_copy.wait_recv()

    before = halo[...].astype(F32)
    for b in range(hb):
        lay_time(b, before[:, b * W : (b + 1) * W])

    per_block = W // B
    deep = per_block * GROUP
    slots = W // deep
    place = lax.rem(lax.broadcasted_iota(jnp.int32, (8, W), 0), slots) == (
        lax.broadcasted_iota(jnp.int32, (8, W), 1) // deep
    )

    def lay(n, carry):
        for i in range(8):
            picked = [
                xt[pl.ds((B // 8 * r + B // 8 - 1 - n) * GROUP * 8 + 7 - i, GROUP, stride=8), :]
                for r in range(per_block)
            ]
            picked = jnp.concatenate(picked * (W // deep), axis=0).T
            for g in range(groups):
                at = pl.multiple_of((g * B + 8 * n + i) * 8, 8)
                lt[pl.ds(at, 8), :] = jnp.where(place, picked[8 * g : 8 * g + 8], 0.0)
        return carry

    lax.fori_loop(0, B // 8, lay, 0)

    for copy in passed:
        copy.wait_recv()
    sp32[:, :channels] = sbuf[...].astype(F32)
    st[...] = sp32[...].T[:rows_p].astype(BF16)
    own_w[...] = sp32[mine, :rows_p].astype(BF16)

    def process(c, gsp):
        for copy in c_waits[c]:
            copy.wait_recv()
        model = jnp.dot(st[...], cbuf[c], preferred_element_type=F32)
        resb[c, :channels, :] = (
            model[:channels] - signal_ref[:, c * chunk : (c + 1) * chunk].astype(F32)
        ).astype(BF16)
        residual = resb[c]
        projected = jnp.dot(own_w[...], residual, preferred_element_type=F32)
        projected = projected.astype(BF16).astype(F32)
        for b in range(per):
            at = hb + c * per + b
            put(pj.at[0], span, at, projected[:, b * W : (b + 1) * W])
        grad = lax.dot_general(
            cbuf[c, mine, :], residual, (((1,), (1,)), ((), ())), preferred_element_type=F32
        )
        return grad if gsp is None else gsp + grad

    gsp = None
    for c in list(range(1, chunks)) + [0]:
        gsp = process(c, gsp)

    low = pl.ds(pl.multiple_of(core * (atoms // 2), atoms // 2), atoms // 2)
    other = pl.ds(pl.multiple_of((1 - core) * (atoms // 2), atoms // 2), atoms // 2)

    def swap(i, lanes):
        copy = pltpu.make_async_remote_copy(
            src_ref=part.at[i, other, lanes], dst_ref=recv1.at[i, :, lanes],
            send_sem=p_send.at[i], recv_sem=p_recv.at[i],
            device_id={"tm": partner}, device_id_type=MESH,
        )
        copy.start()
        return copy

    def spread(i, lanes, copy):
        copy.wait_recv()
        value = part[i, low, lanes] + recv1[i, :, lanes]
        top = jnp.max(jnp.abs(value), axis=0, keepdims=True)
        up = jnp.where(top > TINY, STEPS / jnp.maximum(top, TINY), 0.0)
        shift = jnp.where(value < 0, -0.5, 0.5)
        half[i, me_z, :, lanes] = (value * up + shift).astype(jnp.int32).astype(jnp.int16)
        scale[i, me_z, :, lanes] = top * (1.0 / STEPS)
        copies = []
        for d, peer in enumerate(z_peers):
            for n, ref in enumerate((half, scale)):
                out = pltpu.make_async_remote_copy(
                    src_ref=ref.at[i, me_z, :, lanes], dst_ref=ref.at[i, me_z, :, lanes],
                    send_sem=z_send.at[i, n, d], recv_sem=z_recv.at[i, n, d],
                    device_id={"tm": peer * 2 + core}, device_id_type=MESH,
                )
                out.start()
                copies.append(out)
        return copies

    def finish(i, lanes, copies):
        for copy in copies:
            copy.wait_recv()
        acc = None
        for z in range(chips):
            value = half[i, z, :, lanes].astype(jnp.int32).astype(F32) * scale[i, z, :, lanes]
            acc = value if acc is None else acc + value
        total[i, low, lanes] = acc * factor
        copy = pltpu.make_async_remote_copy(
            src_ref=total.at[i, low, lanes], dst_ref=total.at[i, low, lanes],
            send_sem=f_send.at[i], recv_sem=f_recv.at[i],
            device_id={"tm": partner}, device_id_type=MESH,
        )
        copy.start()
        return copy

    sp_lanes = slice(0, wide)
    tm_lanes = slice(0, length)
    part[0, :, :rows_p] = gsp
    if rows_p < wide:
        part[0, :, rows_p:] = jnp.zeros((atoms, wide - rows_p), F32)
    swap_sp = swap(0, sp_lanes)

    lane = lax.broadcasted_iota(jnp.int32, (atoms, W), 1)
    for r in range(1, per_block):
        turned = [
            pltpu.roll(natural(pj.at[0], span, i), W - B * r, 1)
            for i in range(hb, hb + nb)
        ]
        turned = [jnp.zeros((atoms, W), F32)] + turned + [jnp.zeros((atoms, W), F32)]
        for n in range(nb + 1):
            put(
                pj.at[r], span, hb - 1 + n,
                jnp.where(lane < W - B * r, turned[n], turned[n + 1]),
            )

    depth = (length + B - 1) // W + 1

    def correlate(g, carry):
        for first_atom in range(0, 8, 2 * slots):
            some = range(first_atom, first_atom + 2 * slots)
            lhs = []
            rhs = []
            for i in some:
                left = series(lt, B, g, i, 0, B).astype(BF16)
                none = jnp.zeros((B, W), BF16)
                pair = [left, none] if i - first_atom < slots else [none, left]
                lhs.append(jnp.concatenate(pair, axis=1))
                for r in range(per_block):
                    rhs.append(
                        jnp.concatenate(
                            [series(pj.at[r], span, g, i, j, GROUP) for j in range(depth)], axis=1
                        )
                    )
            prods = jnp.dot(
                jnp.concatenate(lhs, axis=0),
                jnp.concatenate(rhs, axis=0).astype(BF16),
                preferred_element_type=F32,
            )
            for n, i in enumerate(some):
                prod = prods[n * B : (n + 1) * B]
                prod = pltpu.roll(prod, depth * W - (B - 1), 1, stride=1, stride_axis=0)
                acc = prod[:8, :length]
                for q in range(1, B // 8):
                    acc = acc + prod[8 * q : 8 * q + 8, :length]
                for d in range(hb):
                    at = pl.multiple_of((d * groups + g) * 64 + 8 * i, 8)
                    gt[pl.ds(at, 8), :] = acc[:, d * W : (d + 1) * W]
        return carry

    def lags(mine_first, rows):
        for d in range(hb):
            at = 8 * (d * atoms + mine_first)
            total_d = gt[pl.ds(at, atoms // 2, stride=8), :]
            for i in range(1, 8):
                total_d = total_d + gt[pl.ds(at + i, atoms // 2, stride=8), :]
            part[1, rows, d * W : (d + 1) * W] = total_d

    def correlate_from(start, count):
        lax.fori_loop(0, count, lambda n, carry: correlate(start + n, carry), 0, unroll=count)

    correlate_from((1 - core) * (groups // 2), groups // 2)
    lags((1 - core) * (atoms // 2), other)
    swap_tm = swap(1, tm_lanes)
    for turn in range(1, chips - 3):
        listen(turn)
        tell(turn + 1)
    if chips > 2:
        listen(chips - 3)
    spread_sp = spread(0, sp_lanes, swap_sp)
    correlate_from(core * (groups // 2), groups // 2)
    lags(core * (atoms // 2), low)
    spread_tm = spread(1, tm_lanes, swap_tm)
    last_sp = finish(0, sp_lanes, spread_sp)
    last_tm = finish(1, tm_lanes, spread_tm)
    last_sp.wait_recv()
    out_sp_ref[...] = total[0, :, :channels]
    last_tm.wait_recv()
    out_tm_ref[...] = total[1, :, :length]

    @pl.when(me_t < n_tm - 1)
    def _():
        halo_copy.wait_send()
        for copy in spill_copies:
            copy.wait_send()

    for copy in s_copies + passed + [copy for line in c_copies for copy in line]:
        copy.wait_send()
    for copy in [swap_sp, swap_tm, last_sp, last_tm] + spread_sp + spread_tm:
        copy.wait_send()


def local(n_atom, n_tm, signal, spatial, temporal, values, mask):
    atoms, channels = spatial.shape
    length = temporal.shape[1]
    samples = signal.shape[1]
    chunks = samples // length
    nb, hb = samples // W, length // W
    wide = -(-channels // W) * W
    rows_p = -(-channels // 32) * 32
    per_block = W // B
    deep = per_block * GROUP
    slots = W // deep
    place = lax.rem(lax.broadcasted_iota(jnp.int32, (8, W), 0), slots) == (
        lax.broadcasted_iota(jnp.int32, (8, W), 1) // deep
    )
    every = n_atom * atoms
    depth = (length + B - 1) // W + 1
    span = (GROUP + depth - 1) * atoms
    width = max(wide, length)
    chips = n_tm // 2
    factor = 1.0 / math.sqrt(samples * n_tm)
    dma = pltpu.SemaphoreType.DMA
    vmem = pl.BlockSpec(memory_space=pltpu.VMEM)
    return pl.pallas_call(
        functools.partial(kernel, n_atom, n_tm, factor),
        out_shape=(
            pltpu.VMEM((atoms, channels), F32),
            pltpu.VMEM((atoms, length), F32),
        ),
        in_specs=[vmem] * 5,
        out_specs=(vmem, vmem),
        scratch_shapes=[
            pltpu.VMEM((atoms, length), BF16),
            pltpu.VMEM((atoms, length), BF16),
            pltpu.VMEM((atoms, length), F32),
            pltpu.VMEM((atoms, length), F32),
            pltpu.VMEM(((GROUP + hb) * atoms, W), F32),
            pltpu.VMEM((GROUP * W, W), F32),
            pltpu.VMEM((hb * atoms, W), F32),
            pltpu.VMEM((GROUP * atoms, W), F32),
            pltpu.VMEM((chunks, every, length), BF16),
            pltpu.VMEM((every, channels), BF16),
            pltpu.VMEM((every, wide), F32),
            pltpu.VMEM((rows_p, every), BF16),
            pltpu.VMEM((atoms, rows_p), BF16),
            pltpu.VMEM((chunks, rows_p, length), BF16),
            pltpu.VMEM((per_block, span, W), F32),
            pltpu.VMEM((B * atoms, W), F32),
            pltpu.VMEM((8 * hb * atoms, W), F32),
            pltpu.VMEM((2, atoms, width), F32),
            pltpu.VMEM((2, atoms // 2, width), F32),
            pltpu.VMEM((2, chips, atoms // 2, width), jnp.int16),
            pltpu.VMEM((2, chips, 1, width), F32),
            pltpu.VMEM((2, atoms, width), F32),
            pltpu.SemaphoreType.REGULAR((max(chips - 2, 1), 2)),
            dma((6,)),
            dma((n_atom - 1,)),
            dma((n_atom - 1,)),
            dma((n_atom - 1,)),
            dma((n_atom - 1,)),
            dma((n_atom - 1, chunks, 2)),
            dma((n_atom - 1, chunks, 2)),
            dma((2,)),
            dma((2,)),
            dma((2, 2, chips - 1)),
            dma((2, 2, chips - 1)),
            dma((2,)),
            dma((2,)),
        ],
        compiler_params=pltpu.CompilerParams(collective_id=0, has_side_effects=True),
    )(signal, spatial, temporal, values, mask.T)


def settle(a_ref, b_ref, c_ref, d_ref, sems):
    one = pltpu.make_async_copy(a_ref, c_ref, sems.at[0])
    two = pltpu.make_async_copy(b_ref, d_ref, sems.at[1])
    one.start()
    two.start()
    one.wait()
    two.wait()


def placed(n_atom, n_tm, *args):
    first, second = local(n_atom, n_tm, *args)
    return pl.pallas_call(
        settle,
        out_shape=(
            jax.ShapeDtypeStruct(first.shape, F32),
            jax.ShapeDtypeStruct(second.shape, F32),
        ),
        in_specs=[pl.BlockSpec(memory_space=pltpu.VMEM)] * 2,
        out_specs=[pl.BlockSpec(memory_space=pltpu.HBM)] * 2,
        scratch_shapes=[pltpu.SemaphoreType.DMA((2,))],
        compiler_params=pltpu.CompilerParams(vmem_limit_bytes=1 << 20),
    )(first, second)


def solution(mesh):
    in_specs = (P(None, "tm"), P("atom", None), P("atom", None), P("atom", "tm"), P("atom", "tm"))
    out_specs = (P("atom", None), P("atom", None))
    body = functools.partial(placed, mesh.shape["atom"], mesh.shape["tm"])
    return jax.shard_map(body, mesh=mesh, in_specs=in_specs, out_specs=out_specs, check_vma=False)
```

```python
import functools
import math

import jax
import jax.numpy as jnp
from jax import lax
from jax.experimental import pallas as pl
from jax.experimental.pallas import tpu as pltpu
from jax.sharding import PartitionSpec as P

W = 128
B = 32
GROUP = 16
SPLIT = 2
MESH = pl.DeviceIdType.MESH
F32 = jnp.float32
BF16 = jnp.bfloat16
STEPS = 32767.0
TINY = 2.0**-112


def kernel(
    n_atom, n_tm, factor,
    signal_ref, spatial_ref, temporal_ref, values_ref, mask_ref,
    out_sp_ref, out_tm_ref,
    tail, halo, spill, spilled, cx, xt, wt, cf, cbuf, sbuf, sp32, st, own_w, resb, pj, lt, gt,
    part, recv1, half, scale, total,
    heard, halo_sems, s_send, s_recv, h_send, h_recv, c_send, c_recv,
    p_send, p_recv, z_send, z_recv, f_send, f_recv,
):
    atoms, channels = spatial_ref.shape
    length = temporal_ref.shape[1]
    samples = signal_ref.shape[1]
    blocks = mask_ref.shape[0]
    block = samples // blocks
    nb = samples // W
    hb = length // W
    chunk = length
    chunks = samples // chunk
    per = chunk // W
    rows_p = st.shape[0]
    wide = sp32.shape[1]
    span = pj.shape[1] // atoms
    chips = n_tm // 2
    me_a = lax.axis_index("atom")
    me_t = lax.axis_index("tm")
    me_z = me_t // 2
    core = lax.rem(me_t, 2)
    partner = me_z * 2 + 1 - core

    def across(at, count):
        def flip(d):
            out = at
            for bit in range(d.bit_length()):
                if d >> bit & 1:
                    step = 1 << bit
                    out = out + step - 2 * step * lax.rem(at // step, 2)
            return out

        if count & (count - 1) == 0:
            return [flip(d) for d in range(count - 1, 0, -1)]
        return [lax.rem(at + d, count) for d in range(1, count)]

    def sources(at, count):
        if count & (count - 1) == 0:
            return across(at, count)
        return [lax.rem(at + count - d, count) for d in range(1, count)]

    a_peers = across(me_a, n_atom)
    z_peers = across(me_z, chips)
    mine = pl.ds(pl.multiple_of(me_a * atoms, atoms), atoms)

    barrier = pltpu.get_barrier_semaphore()
    for peer in a_peers:
        pl.semaphore_signal(barrier, inc=1, device_id={"atom": peer}, device_id_type=MESH)
    line = me_t - 1 + 2 * core
    beside = [
        (me_z > 0, me_t - 2),
        (me_z < chips - 1, me_t + 2),
        (jnp.logical_and(line >= 0, line < n_tm), line),
    ]

    def greet(peer):
        pl.semaphore_signal(barrier, inc=1, device_id={"tm": peer}, device_id_type=MESH)

    greet(partner)
    for there, peer in beside:
        pl.when(there)(functools.partial(greet, peer))

    def tell(turn):
        for n, (there, peer) in enumerate(beside[:2]):

            @pl.when(there)
            def _():
                pl.semaphore_signal(
                    heard.at[turn, 1 - n], inc=1, device_id={"tm": peer}, device_id_type=MESH
                )

    def listen(turn):
        for n, (there, peer) in enumerate(beside[:2]):

            @pl.when(there)
            def _():
                pl.semaphore_wait(heard.at[turn, n], 1)


    groups = atoms // 8

    def put(ref, count, b, value):
        for g in range(groups):
            ref[(g * count + b) * 8 : (g * count + b + 1) * 8, :] = value[8 * g : 8 * g + 8]

    def filtered(b, lo, hi):
        return jnp.concatenate(
            [
                cf[pl.ds((g * (GROUP // 8) + b // 8) * 64 + b % 8, 8, stride=8), :]
                for g in range(lo, hi)
            ],
            axis=0,
        )

    def natural(ref, count, b):
        return jnp.concatenate(
            [ref[(g * count + b) * 8 : (g * count + b + 1) * 8, :] for g in range(groups)], axis=0
        )

    def series(ref, count, g, i, first, size):
        return ref[pl.ds((g * count + first) * 8 + i, size, stride=8), :]

    mask = mask_ref[...].astype(F32).T
    codes = [
        values_ref[:, j * block : (j + 1) * block].astype(F32) * mask[:, j : j + 1]
        for j in range(blocks)
    ]
    codes = jnp.concatenate(codes, axis=1)
    tail[...] = codes[:, samples - length :].astype(BF16)
    gap = jnp.zeros((atoms, W), F32)
    for b in list(range(hb)) + list(range(hb + nb, GROUP + hb)):
        put(cx, GROUP + hb, b, gap)
    for b in range(nb):
        put(cx, GROUP + hb, hb + b, codes[:, b * W : (b + 1) * W])
    for d in range(hb):
        wt[d * atoms : (d + 1) * atoms, :] = temporal_ref[:, d * W : (d + 1) * W].astype(F32)

    row = lax.broadcasted_iota(jnp.int32, (W, W), 0)
    col = lax.broadcasted_iota(jnp.int32, (W, W), 1)
    ahead = col >= row

    def toeplitz(rows, i):
        circ = []
        for d in range(hb):
            base = jnp.broadcast_to(rows[d][i : i + 1], (GROUP, W))
            base = pltpu.roll(base, 0, 1, stride=1, stride_axis=0).astype(BF16)
            tiles = [base] + [pltpu.roll(base, GROUP * n, 1) for n in range(1, W // GROUP)]
            circ.append(jnp.concatenate(tiles, axis=0))
        zero = jnp.zeros((W, W), BF16)
        parts = []
        for d in range(hb, -1, -1):
            near = circ[d] if d < hb else zero
            far = circ[d - 1] if d > 0 else zero
            parts.append(jnp.where(ahead, near, far))
        return jnp.concatenate(parts, axis=0)

    def windows(g, i):
        return jnp.concatenate(
            [series(cx, GROUP + hb, g, i, j, GROUP) for j in range(hb + 1)], axis=1
        )

    def first(g, carry):
        rows = [
            wt[pl.ds(pl.multiple_of(d * atoms + 8 * g, 8), 8), :] for d in range(hb)
        ]
        for i in range(0, 8, 2):
            taps = jnp.concatenate([toeplitz(rows, i), toeplitz(rows, i + 1)], axis=1)
            lhs = jnp.concatenate([windows(g, i), windows(g, i + 1)], axis=0).astype(BF16)
            out = jnp.dot(lhs, taps, preferred_element_type=F32)
            for n in range(2):
                for h in range(GROUP // 8):
                    at = pl.multiple_of(((g * (GROUP // 8) + h) * 8 + i + n) * 8, 8)
                    row = n * GROUP + 8 * h
                    cf[pl.ds(at, 8), :] = out[row : row + 8, n * W : (n + 1) * W]
        return carry

    lax.fori_loop(0, SPLIT * groups // 4 // 2 * 2, first, 0, unroll=4)

    present = n_atom
    for there, _ in beside:
        present = present + jnp.where(there, 1, 0)
    pl.semaphore_wait(barrier, present)
    if chips > 2:
        tell(0)

    right = lax.rem(me_t + 1, n_tm)
    halo_copy = pltpu.make_async_remote_copy(
        src_ref=tail, dst_ref=halo, send_sem=halo_sems.at[0], recv_sem=halo_sems.at[1],
        device_id={"tm": right}, device_id_type=MESH,
    )

    spill_copies = []

    def send_spill(n, lo, hi):
        rows = slice(8 * lo, 8 * hi)
        for b in range(hb):
            spill[rows, b * W : (b + 1) * W] = filtered(nb + b, lo, hi)
        copy = pltpu.make_async_remote_copy(
            src_ref=spill.at[rows], dst_ref=spilled.at[rows],
            send_sem=halo_sems.at[2 + n], recv_sem=halo_sems.at[4 + n],
            device_id={"tm": right}, device_id_type=MESH,
        )
        spill_copies.append(copy)

        @pl.when(me_t < n_tm - 1)
        def _():
            copy.start()

    c_copies = [[] for _ in range(chunks)]
    c_waits = [[] for _ in range(chunks)]
    firsts = {}
    relays = {}
    if n_atom == 4:
        relays = {c: (2, 1) if c % 2 else (1, 2) for c in range(1, chunks)}
    order = [chunks - 1] + list(range(1, chunks - 1))

    def send(c, lo, hi):
        rows = pl.ds(pl.multiple_of(me_a * atoms + 8 * lo, 8 * (hi - lo)), 8 * (hi - lo))
        for b in range(per):
            value = filtered(c * per + b, lo, hi)
            if c == 0:
                value = value + spilled[8 * lo : 8 * hi, b * W : (b + 1) * W]
            cbuf[c, rows, b * W : (b + 1) * W] = value.astype(BF16)
        for d, peer in enumerate(a_peers):
            if c in relays and lo == 0 and d == 0:
                continue
            copy = pltpu.make_async_remote_copy(
                src_ref=cbuf.at[c, rows], dst_ref=cbuf.at[c, rows],
                send_sem=c_send.at[d, c, min(lo, 1)], recv_sem=c_recv.at[d, c, min(lo, 1)],
                device_id={"atom": peer}, device_id_type=MESH,
            )
            copy.start()
            c_copies[c].append(copy)
            c_waits[c].append(copy)
            firsts[c, d, min(lo, 1)] = copy

    def relay(c):
        source, target = relays[c]
        copy = firsts[c, source, 0]
        copy.wait_recv()
        c_waits[c] = [other_copy for other_copy in c_waits[c] if other_copy is not copy]
        rows = pl.ds(pl.multiple_of(a_peers[source] * atoms, atoms), 8 * early)
        copy = pltpu.make_async_remote_copy(
            src_ref=cbuf.at[c, rows], dst_ref=cbuf.at[c, rows],
            send_sem=c_send.at[0, c, 0], recv_sem=c_recv.at[0, c, 0],
            device_id={"atom": a_peers[target]}, device_id_type=MESH,
        )
        copy.start()
        c_copies[c].append(copy)
        c_waits[c].append(copy)

    early = SPLIT * groups // 4 // 2 * 2
    send_spill(0, 0, early)

    @pl.when(me_t < n_tm - 1)
    def _():
        halo_copy.start()

    for c in relays:
        send(c, 0, early)

    s_copies = []
    own_half = pl.ds(pl.multiple_of(core * (atoms // 2), atoms // 2), atoms // 2)

    def half_of(peer):
        at = peer * atoms + core * (atoms // 2)
        return pl.ds(pl.multiple_of(at, atoms // 2), atoms // 2)

    for d, peer in enumerate(a_peers):
        copy = pltpu.make_async_remote_copy(
            src_ref=spatial_ref.at[own_half], dst_ref=sbuf.at[half_of(me_a)],
            send_sem=s_send.at[d], recv_sem=s_recv.at[d],
            device_id={"atom": peer}, device_id_type=MESH,
        )
        copy.start()
        s_copies.append(copy)
    for c in range(1, chunks):
        if c not in relays:
            send(c, 0, early)
    lax.fori_loop(early, groups, first, 0, unroll=4)
    send_spill(1, early, groups)
    for c in order:
        send(c, early, groups)

    def lay_time(b, value):
        turned = value.T
        for u in range(W // 8):
            at = (u * GROUP + b) * 8
            xt[at : at + 8, :atoms] = turned[8 * u : 8 * u + 8]

    for b in range(nb):
        lay_time(hb + b, codes[:, b * W : (b + 1) * W])
    for u in range(W // 8):
        xt[(u * GROUP + hb + nb) * 8 : (u + 1) * GROUP * 8, :] = jnp.zeros(
            ((GROUP - hb - nb) * 8, W), F32
        )
    pj[...] = jnp.zeros(pj.shape, F32)
    resb[:, channels // 16 * 16 :, :] = jnp.zeros(
        (chunks, rows_p - channels // 16 * 16, chunk), BF16
    )
    sp32[...] = jnp.zeros(sp32.shape, F32)

    for c in relays:
        relay(c)

    @pl.when(me_t == 0)
    def _():
        halo[...] = jnp.zeros(halo.shape, halo.dtype)
        spilled[...] = jnp.zeros(spilled.shape, F32)

    @pl.when(me_t > 0)
    def _():
        for copy in spill_copies:
            copy.wait_recv()

    send(0, 0, groups)
    if chips > 3:
        listen(0)
        tell(1)

    sbuf[mine, :] = spatial_ref[...]
    passed = []
    for d, source in enumerate(sources(me_a, n_atom)):
        s_copies[d].wait_recv()
        rows = half_of(source)
        out = pltpu.make_async_remote_copy(
            src_ref=sbuf.at[rows], dst_ref=sbuf.at[rows],
            send_sem=h_send.at[d], recv_sem=h_recv.at[d],
            device_id={"tm": partner}, device_id_type=MESH,
        )
        out.start()
        passed.append(out)

    @pl.when(me_t > 0)
    def _():
        halo_copy.wait_recv()

    before = halo[...].astype(F32)
    for b in range(hb):
        lay_time(b, before[:, b * W : (b + 1) * W])

    per_block = W // B
    deep = per_block * GROUP
    slots = W // deep
    place = lax.rem(lax.broadcasted_iota(jnp.int32, (8, W), 0), slots) == (
        lax.broadcasted_iota(jnp.int32, (8, W), 1) // deep
    )

    def lay(n, carry):
        for i in range(8):
            picked = [
                xt[pl.ds((B // 8 * r + B // 8 - 1 - n) * GROUP * 8 + 7 - i, GROUP, stride=8), :]
                for r in range(per_block)
            ]
            picked = jnp.concatenate(picked * (W // deep), axis=0).T
            for g in range(groups):
                at = pl.multiple_of((g * B + 8 * n + i) * 8, 8)
                lt[pl.ds(at, 8), :] = jnp.where(place, picked[8 * g : 8 * g + 8], 0.0)
        return carry

    lax.fori_loop(0, B // 8, lay, 0)

    for copy in passed:
        copy.wait_recv()
    sp32[:, :channels] = sbuf[...].astype(F32)
    st[...] = sp32[...].T[:rows_p].astype(BF16)
    own_w[...] = sp32[mine, :rows_p].astype(BF16)

    def process(c, gsp):
        for copy in c_waits[c]:
            copy.wait_recv()
        model = jnp.dot(st[...], cbuf[c], preferred_element_type=F32)
        resb[c, :channels, :] = (
            model[:channels] - signal_ref[:, c * chunk : (c + 1) * chunk].astype(F32)
        ).astype(BF16)
        residual = resb[c]
        grad = lax.dot_general(
            cbuf[c, mine, :], residual, (((1,), (1,)), ((), ())), preferred_element_type=F32
        )
        return grad if gsp is None else gsp + grad

    def project(c):
        projected = jnp.dot(own_w[...], resb[c], preferred_element_type=F32)
        projected = projected.astype(BF16).astype(F32)
        for b in range(per):
            at = hb + c * per + b
            put(pj.at[0], span, at, projected[:, b * W : (b + 1) * W])

    gsp = None
    for c in order + [0]:
        gsp = process(c, gsp)

    low = pl.ds(pl.multiple_of(core * (atoms // 2), atoms // 2), atoms // 2)
    other = pl.ds(pl.multiple_of((1 - core) * (atoms // 2), atoms // 2), atoms // 2)

    def swap(i, lanes):
        copy = pltpu.make_async_remote_copy(
            src_ref=part.at[i, other, lanes], dst_ref=recv1.at[i, :, lanes],
            send_sem=p_send.at[i], recv_sem=p_recv.at[i],
            device_id={"tm": partner}, device_id_type=MESH,
        )
        copy.start()
        return copy

    def spread(i, lanes, copy):
        copy.wait_recv()
        value = part[i, low, lanes] + recv1[i, :, lanes]
        top = jnp.max(jnp.abs(value), axis=0, keepdims=True)
        up = jnp.where(top > TINY, STEPS / jnp.maximum(top, TINY), 0.0)
        shift = jnp.where(value < 0, -0.5, 0.5)
        half[i, me_z, :, lanes] = (value * up + shift).astype(jnp.int32).astype(jnp.int16)
        scale[i, me_z, :, lanes] = top * (1.0 / STEPS)
        copies = []
        for d, peer in enumerate(z_peers):
            for n, ref in enumerate((half, scale)):
                out = pltpu.make_async_remote_copy(
                    src_ref=ref.at[i, me_z, :, lanes], dst_ref=ref.at[i, me_z, :, lanes],
                    send_sem=z_send.at[i, n, d], recv_sem=z_recv.at[i, n, d],
                    device_id={"tm": peer * 2 + core}, device_id_type=MESH,
                )
                out.start()
                copies.append(out)
        return copies

    def finish(i, lanes, copies):
        for copy in copies:
            copy.wait_recv()
        acc = None
        for z in range(chips):
            value = half[i, z, :, lanes].astype(jnp.int32).astype(F32) * scale[i, z, :, lanes]
            acc = value if acc is None else acc + value
        total[i, low, lanes] = acc * factor
        copy = pltpu.make_async_remote_copy(
            src_ref=total.at[i, low, lanes], dst_ref=total.at[i, low, lanes],
            send_sem=f_send.at[i], recv_sem=f_recv.at[i],
            device_id={"tm": partner}, device_id_type=MESH,
        )
        copy.start()
        return copy

    sp_lanes = slice(0, wide)
    tm_lanes = slice(0, length)
    part[0, :, :rows_p] = gsp
    if rows_p < wide:
        part[0, :, rows_p:] = jnp.zeros((atoms, wide - rows_p), F32)
    swap_sp = swap(0, sp_lanes)
    for c in range(chunks):
        project(c)

    lane = lax.broadcasted_iota(jnp.int32, (atoms, W), 1)
    for r in range(1, per_block):
        turned = [
            pltpu.roll(natural(pj.at[0], span, i), W - B * r, 1)
            for i in range(hb, hb + nb)
        ]
        turned = [jnp.zeros((atoms, W), F32)] + turned + [jnp.zeros((atoms, W), F32)]
        for n in range(nb + 1):
            put(
                pj.at[r], span, hb - 1 + n,
                jnp.where(lane < W - B * r, turned[n], turned[n + 1]),
            )

    depth = (length + B - 1) // W + 1

    def correlate(g, carry):
        for first_atom in range(0, 8, 2 * slots):
            some = range(first_atom, first_atom + 2 * slots)
            lhs = []
            rhs = []
            for i in some:
                left = series(lt, B, g, i, 0, B).astype(BF16)
                none = jnp.zeros((B, W), BF16)
                pair = [left, none] if i - first_atom < slots else [none, left]
                lhs.append(jnp.concatenate(pair, axis=1))
                for r in range(per_block):
                    rhs.append(
                        jnp.concatenate(
                            [series(pj.at[r], span, g, i, j, GROUP) for j in range(depth)], axis=1
                        )
                    )
            prods = jnp.dot(
                jnp.concatenate(lhs, axis=0),
                jnp.concatenate(rhs, axis=0).astype(BF16),
                preferred_element_type=F32,
            )
            for n, i in enumerate(some):
                prod = prods[n * B : (n + 1) * B]
                prod = pltpu.roll(prod, depth * W - (B - 1), 1, stride=1, stride_axis=0)
                acc = prod[:8, :length]
                for q in range(1, B // 8):
                    acc = acc + prod[8 * q : 8 * q + 8, :length]
                for d in range(hb):
                    at = pl.multiple_of((d * groups + g) * 64 + 8 * i, 8)
                    gt[pl.ds(at, 8), :] = acc[:, d * W : (d + 1) * W]
        return carry

    def lags(mine_first, rows):
        for d in range(hb):
            at = 8 * (d * atoms + mine_first)
            total_d = gt[pl.ds(at, atoms // 2, stride=8), :]
            for i in range(1, 8):
                total_d = total_d + gt[pl.ds(at + i, atoms // 2, stride=8), :]
            part[1, rows, d * W : (d + 1) * W] = total_d

    def correlate_from(start, count):
        lax.fori_loop(0, count, lambda n, carry: correlate(start + n, carry), 0, unroll=count)

    for turn in range(1, chips - 3):
        listen(turn)
        tell(turn + 1)
    if chips > 2:
        listen(chips - 3)
    spread_sp = spread(0, sp_lanes, swap_sp)
    correlate_from((1 - core) * (groups // 2), groups // 2)
    lags((1 - core) * (atoms // 2), other)
    swap_tm = swap(1, tm_lanes)
    correlate_from(core * (groups // 2), groups // 2)
    lags(core * (atoms // 2), low)
    spread_tm = spread(1, tm_lanes, swap_tm)
    last_sp = finish(0, sp_lanes, spread_sp)
    last_tm = finish(1, tm_lanes, spread_tm)
    last_sp.wait_recv()
    out_sp_ref[...] = total[0, :, :channels]
    last_tm.wait_recv()
    out_tm_ref[...] = total[1, :, :length]

    @pl.when(me_t < n_tm - 1)
    def _():
        halo_copy.wait_send()
        for copy in spill_copies:
            copy.wait_send()

    for copy in s_copies + passed + [copy for line in c_copies for copy in line]:
        copy.wait_send()
    for copy in [swap_sp, swap_tm, last_sp, last_tm] + spread_sp + spread_tm:
        copy.wait_send()


def local(n_atom, n_tm, signal, spatial, temporal, values, mask):
    atoms, channels = spatial.shape
    length = temporal.shape[1]
    samples = signal.shape[1]
    chunks = samples // length
    nb, hb = samples // W, length // W
    wide = -(-channels // W) * W
    rows_p = -(-channels // 32) * 32
    per_block = W // B
    deep = per_block * GROUP
    slots = W // deep
    place = lax.rem(lax.broadcasted_iota(jnp.int32, (8, W), 0), slots) == (
        lax.broadcasted_iota(jnp.int32, (8, W), 1) // deep
    )
    every = n_atom * atoms
    depth = (length + B - 1) // W + 1
    span = (GROUP + depth - 1) * atoms
    width = max(wide, length)
    chips = n_tm // 2
    factor = 1.0 / math.sqrt(samples * n_tm)
    dma = pltpu.SemaphoreType.DMA
    vmem = pl.BlockSpec(memory_space=pltpu.VMEM)
    return pl.pallas_call(
        functools.partial(kernel, n_atom, n_tm, factor),
        out_shape=(
            pltpu.VMEM((atoms, channels), F32),
            pltpu.VMEM((atoms, length), F32),
        ),
        in_specs=[vmem] * 5,
        out_specs=(vmem, vmem),
        scratch_shapes=[
            pltpu.VMEM((atoms, length), BF16),
            pltpu.VMEM((atoms, length), BF16),
            pltpu.VMEM((atoms, length), F32),
            pltpu.VMEM((atoms, length), F32),
            pltpu.VMEM(((GROUP + hb) * atoms, W), F32),
            pltpu.VMEM((GROUP * W, W), F32),
            pltpu.VMEM((hb * atoms, W), F32),
            pltpu.VMEM((GROUP * atoms, W), F32),
            pltpu.VMEM((chunks, every, length), BF16),
            pltpu.VMEM((every, channels), BF16),
            pltpu.VMEM((every, wide), F32),
            pltpu.VMEM((rows_p, every), BF16),
            pltpu.VMEM((atoms, rows_p), BF16),
            pltpu.VMEM((chunks, rows_p, length), BF16),
            pltpu.VMEM((per_block, span, W), F32),
            pltpu.VMEM((B * atoms, W), F32),
            pltpu.VMEM((8 * hb * atoms, W), F32),
            pltpu.VMEM((2, atoms, width), F32),
            pltpu.VMEM((2, atoms // 2, width), F32),
            pltpu.VMEM((2, chips, atoms // 2, width), jnp.int16),
            pltpu.VMEM((2, chips, 1, width), F32),
            pltpu.VMEM((2, atoms, width), F32),
            pltpu.SemaphoreType.REGULAR((max(chips - 2, 1), 2)),
            dma((6,)),
            dma((n_atom - 1,)),
            dma((n_atom - 1,)),
            dma((n_atom - 1,)),
            dma((n_atom - 1,)),
            dma((n_atom - 1, chunks, 2)),
            dma((n_atom - 1, chunks, 2)),
            dma((2,)),
            dma((2,)),
            dma((2, 2, chips - 1)),
            dma((2, 2, chips - 1)),
            dma((2,)),
            dma((2,)),
        ],
        compiler_params=pltpu.CompilerParams(collective_id=0, has_side_effects=True),
    )(signal, spatial, temporal, values, mask.T)


def settle(a_ref, b_ref, c_ref, d_ref, sems):
    one = pltpu.make_async_copy(a_ref, c_ref, sems.at[0])
    two = pltpu.make_async_copy(b_ref, d_ref, sems.at[1])
    one.start()
    two.start()
    one.wait()
    two.wait()


def placed(n_atom, n_tm, *args):
    first, second = local(n_atom, n_tm, *args)
    return pl.pallas_call(
        settle,
        out_shape=(
            jax.ShapeDtypeStruct(first.shape, F32),
            jax.ShapeDtypeStruct(second.shape, F32),
        ),
        in_specs=[pl.BlockSpec(memory_space=pltpu.VMEM)] * 2,
        out_specs=[pl.BlockSpec(memory_space=pltpu.HBM)] * 2,
        scratch_shapes=[pltpu.SemaphoreType.DMA((2,))],
        compiler_params=pltpu.CompilerParams(vmem_limit_bytes=1 << 20),
    )(first, second)


def solution(mesh):
    in_specs = (P(None, "tm"), P("atom", None), P("atom", None), P("atom", "tm"), P("atom", "tm"))
    out_specs = (P("atom", None), P("atom", None))
    body = functools.partial(placed, mesh.shape["atom"], mesh.shape["tm"])
    return jax.shard_map(body, mesh=mesh, in_specs=in_specs, out_specs=out_specs, check_vma=False)
```

```python
import functools
import math

import jax
import jax.numpy as jnp
from jax import lax
from jax.experimental import pallas as pl
from jax.experimental.pallas import tpu as pltpu
from jax.sharding import PartitionSpec as P

W = 128
B = 32
GROUP = 16
SPLIT = 2
MESH = pl.DeviceIdType.MESH
F32 = jnp.float32
BF16 = jnp.bfloat16
STEPS = 32767.0
TINY = 2.0**-112


def kernel(
    n_atom, n_tm, factor,
    signal_ref, spatial_ref, temporal_ref, values_ref, mask_ref,
    out_sp_ref, out_tm_ref,
    tail, halo, spill, spilled, cx, xt, wt, cf, cbuf, sbuf, sp32, st, own_w, resb, pj, lt, gt,
    part, recv1, half, folded, scale, total,
    heard, halo_sems, s_send, s_recv, h_send, h_recv, c_send, c_recv,
    p_send, p_recv, z_send, z_recv, f_send, f_recv,
):
    atoms, channels = spatial_ref.shape
    length = temporal_ref.shape[1]
    samples = signal_ref.shape[1]
    blocks = mask_ref.shape[0]
    block = samples // blocks
    nb = samples // W
    hb = length // W
    chunk = length
    chunks = samples // chunk
    per = chunk // W
    rows_p = st.shape[0]
    wide = sp32.shape[1]
    span = pj.shape[1] // atoms
    chips = n_tm // 2
    me_a = lax.axis_index("atom")
    me_t = lax.axis_index("tm")
    me_z = me_t // 2
    core = lax.rem(me_t, 2)
    partner = me_z * 2 + 1 - core

    def across(at, count):
        def flip(d):
            out = at
            for bit in range(d.bit_length()):
                if d >> bit & 1:
                    step = 1 << bit
                    out = out + step - 2 * step * lax.rem(at // step, 2)
            return out

        if count & (count - 1) == 0:
            return [flip(d) for d in range(count - 1, 0, -1)]
        return [lax.rem(at + d, count) for d in range(1, count)]

    def sources(at, count):
        if count & (count - 1) == 0:
            return across(at, count)
        return [lax.rem(at + count - d, count) for d in range(1, count)]

    a_peers = across(me_a, n_atom)
    z_peers = across(me_z, chips)
    mine = pl.ds(pl.multiple_of(me_a * atoms, atoms), atoms)

    barrier = pltpu.get_barrier_semaphore()
    for peer in a_peers:
        pl.semaphore_signal(barrier, inc=1, device_id={"atom": peer}, device_id_type=MESH)
    line = me_t - 1 + 2 * core
    beside = [
        (me_z > 0, me_t - 2),
        (me_z < chips - 1, me_t + 2),
        (jnp.logical_and(line >= 0, line < n_tm), line),
    ]

    def greet(peer):
        pl.semaphore_signal(barrier, inc=1, device_id={"tm": peer}, device_id_type=MESH)

    greet(partner)
    for there, peer in beside:
        pl.when(there)(functools.partial(greet, peer))

    def tell(turn):
        for n, (there, peer) in enumerate(beside[:2]):

            @pl.when(there)
            def _():
                pl.semaphore_signal(
                    heard.at[turn, 1 - n], inc=1, device_id={"tm": peer}, device_id_type=MESH
                )

    def listen(turn):
        for n, (there, peer) in enumerate(beside[:2]):

            @pl.when(there)
            def _():
                pl.semaphore_wait(heard.at[turn, n], 1)


    groups = atoms // 8

    def put(ref, count, b, value):
        for g in range(groups):
            ref[(g * count + b) * 8 : (g * count + b + 1) * 8, :] = value[8 * g : 8 * g + 8]

    def filtered(b, lo, hi):
        return jnp.concatenate(
            [
                cf[pl.ds((g * (GROUP // 8) + b // 8) * 64 + b % 8, 8, stride=8), :]
                for g in range(lo, hi)
            ],
            axis=0,
        )

    def natural(ref, count, b):
        return jnp.concatenate(
            [ref[(g * count + b) * 8 : (g * count + b + 1) * 8, :] for g in range(groups)], axis=0
        )

    def series(ref, count, g, i, first, size):
        return ref[pl.ds((g * count + first) * 8 + i, size, stride=8), :]

    mask = mask_ref[...].astype(F32).T
    codes = [
        values_ref[:, j * block : (j + 1) * block].astype(F32) * mask[:, j : j + 1]
        for j in range(blocks)
    ]
    codes = jnp.concatenate(codes, axis=1)
    tail[...] = codes[:, samples - length :].astype(BF16)
    gap = jnp.zeros((atoms, W), F32)
    for b in list(range(hb)) + list(range(hb + nb, GROUP + hb)):
        put(cx, GROUP + hb, b, gap)
    for b in range(nb):
        put(cx, GROUP + hb, hb + b, codes[:, b * W : (b + 1) * W])
    for d in range(hb):
        wt[d * atoms : (d + 1) * atoms, :] = temporal_ref[:, d * W : (d + 1) * W].astype(F32)

    row = lax.broadcasted_iota(jnp.int32, (W, W), 0)
    col = lax.broadcasted_iota(jnp.int32, (W, W), 1)
    ahead = col >= row

    def toeplitz(rows, i):
        circ = []
        for d in range(hb):
            base = jnp.broadcast_to(rows[d][i : i + 1], (GROUP, W))
            base = pltpu.roll(base, 0, 1, stride=1, stride_axis=0).astype(BF16)
            tiles = [base] + [pltpu.roll(base, GROUP * n, 1) for n in range(1, W // GROUP)]
            circ.append(jnp.concatenate(tiles, axis=0))
        zero = jnp.zeros((W, W), BF16)
        parts = []
        for d in range(hb, -1, -1):
            near = circ[d] if d < hb else zero
            far = circ[d - 1] if d > 0 else zero
            parts.append(jnp.where(ahead, near, far))
        return jnp.concatenate(parts, axis=0)

    def windows(g, i):
        return jnp.concatenate(
            [series(cx, GROUP + hb, g, i, j, GROUP) for j in range(hb + 1)], axis=1
        )

    def first(g, carry):
        rows = [
            wt[pl.ds(pl.multiple_of(d * atoms + 8 * g, 8), 8), :] for d in range(hb)
        ]
        for i in range(0, 8, 2):
            taps = jnp.concatenate([toeplitz(rows, i), toeplitz(rows, i + 1)], axis=1)
            lhs = jnp.concatenate([windows(g, i), windows(g, i + 1)], axis=0).astype(BF16)
            out = jnp.dot(lhs, taps, preferred_element_type=F32)
            for n in range(2):
                for h in range(GROUP // 8):
                    at = pl.multiple_of(((g * (GROUP // 8) + h) * 8 + i + n) * 8, 8)
                    row = n * GROUP + 8 * h
                    cf[pl.ds(at, 8), :] = out[row : row + 8, n * W : (n + 1) * W]
        return carry

    lax.fori_loop(0, SPLIT * groups // 4 // 2 * 2, first, 0, unroll=4)

    present = n_atom
    for there, _ in beside:
        present = present + jnp.where(there, 1, 0)
    pl.semaphore_wait(barrier, present)
    if chips > 2:
        tell(0)

    right = lax.rem(me_t + 1, n_tm)
    halo_copy = pltpu.make_async_remote_copy(
        src_ref=tail, dst_ref=halo, send_sem=halo_sems.at[0], recv_sem=halo_sems.at[1],
        device_id={"tm": right}, device_id_type=MESH,
    )

    spill_copies = []

    def send_spill(n, lo, hi):
        rows = slice(8 * lo, 8 * hi)
        for b in range(hb):
            spill[rows, b * W : (b + 1) * W] = filtered(nb + b, lo, hi)
        copy = pltpu.make_async_remote_copy(
            src_ref=spill.at[rows], dst_ref=spilled.at[rows],
            send_sem=halo_sems.at[2 + n], recv_sem=halo_sems.at[4 + n],
            device_id={"tm": right}, device_id_type=MESH,
        )
        spill_copies.append(copy)

        @pl.when(me_t < n_tm - 1)
        def _():
            copy.start()

    c_copies = [[] for _ in range(chunks)]
    c_waits = [[] for _ in range(chunks)]
    firsts = {}
    relays = {}
    if n_atom == 4:
        relays = {c: (2, 1) if c % 2 else (1, 2) for c in range(1, chunks)}
    order = [chunks - 1] + list(range(1, chunks - 1))

    def send(c, lo, hi):
        rows = pl.ds(pl.multiple_of(me_a * atoms + 8 * lo, 8 * (hi - lo)), 8 * (hi - lo))
        for b in range(per):
            value = filtered(c * per + b, lo, hi)
            if c == 0:
                value = value + spilled[8 * lo : 8 * hi, b * W : (b + 1) * W]
            cbuf[c, rows, b * W : (b + 1) * W] = value.astype(BF16)
        for d, peer in enumerate(a_peers):
            if c in relays and lo == 0 and d == 0:
                continue
            copy = pltpu.make_async_remote_copy(
                src_ref=cbuf.at[c, rows], dst_ref=cbuf.at[c, rows],
                send_sem=c_send.at[d, c, min(lo, 1)], recv_sem=c_recv.at[d, c, min(lo, 1)],
                device_id={"atom": peer}, device_id_type=MESH,
            )
            copy.start()
            c_copies[c].append(copy)
            c_waits[c].append(copy)
            firsts[c, d, min(lo, 1)] = copy

    def relay(c):
        source, target = relays[c]
        copy = firsts[c, source, 0]
        copy.wait_recv()
        c_waits[c] = [other_copy for other_copy in c_waits[c] if other_copy is not copy]
        rows = pl.ds(pl.multiple_of(a_peers[source] * atoms, atoms), 8 * early)
        copy = pltpu.make_async_remote_copy(
            src_ref=cbuf.at[c, rows], dst_ref=cbuf.at[c, rows],
            send_sem=c_send.at[0, c, 0], recv_sem=c_recv.at[0, c, 0],
            device_id={"atom": a_peers[target]}, device_id_type=MESH,
        )
        copy.start()
        c_copies[c].append(copy)
        c_waits[c].append(copy)

    early = SPLIT * groups // 4 // 2 * 2
    send_spill(0, 0, early)

    @pl.when(me_t < n_tm - 1)
    def _():
        halo_copy.start()

    for c in relays:
        send(c, 0, early)

    s_copies = []
    own_half = pl.ds(pl.multiple_of(core * (atoms // 2), atoms // 2), atoms // 2)

    def half_of(peer):
        at = peer * atoms + core * (atoms // 2)
        return pl.ds(pl.multiple_of(at, atoms // 2), atoms // 2)

    for d, peer in enumerate(a_peers):
        copy = pltpu.make_async_remote_copy(
            src_ref=spatial_ref.at[own_half], dst_ref=sbuf.at[half_of(me_a)],
            send_sem=s_send.at[d], recv_sem=s_recv.at[d],
            device_id={"atom": peer}, device_id_type=MESH,
        )
        copy.start()
        s_copies.append(copy)
    for c in range(1, chunks):
        if c not in relays:
            send(c, 0, early)
    lax.fori_loop(early, groups, first, 0, unroll=4)
    send_spill(1, early, groups)
    for c in order:
        send(c, early, groups)

    def lay_time(b, value):
        turned = value.T
        for u in range(W // 8):
            at = (u * GROUP + b) * 8
            xt[at : at + 8, :atoms] = turned[8 * u : 8 * u + 8]

    for b in range(nb):
        lay_time(hb + b, codes[:, b * W : (b + 1) * W])
    for u in range(W // 8):
        xt[(u * GROUP + hb + nb) * 8 : (u + 1) * GROUP * 8, :] = jnp.zeros(
            ((GROUP - hb - nb) * 8, W), F32
        )
    pj[...] = jnp.zeros(pj.shape, F32)
    resb[:, channels // 16 * 16 :, :] = jnp.zeros(
        (chunks, rows_p - channels // 16 * 16, chunk), BF16
    )
    sp32[...] = jnp.zeros(sp32.shape, F32)

    for c in relays:
        relay(c)

    @pl.when(me_t == 0)
    def _():
        halo[...] = jnp.zeros(halo.shape, halo.dtype)
        spilled[...] = jnp.zeros(spilled.shape, F32)

    @pl.when(me_t > 0)
    def _():
        for copy in spill_copies:
            copy.wait_recv()

    send(0, 0, groups)
    if chips > 3:
        listen(0)
        tell(1)

    sbuf[mine, :] = spatial_ref[...]
    passed = []
    for d, source in enumerate(sources(me_a, n_atom)):
        s_copies[d].wait_recv()
        rows = half_of(source)
        out = pltpu.make_async_remote_copy(
            src_ref=sbuf.at[rows], dst_ref=sbuf.at[rows],
            send_sem=h_send.at[d], recv_sem=h_recv.at[d],
            device_id={"tm": partner}, device_id_type=MESH,
        )
        out.start()
        passed.append(out)

    @pl.when(me_t > 0)
    def _():
        halo_copy.wait_recv()

    before = halo[...].astype(F32)
    for b in range(hb):
        lay_time(b, before[:, b * W : (b + 1) * W])

    per_block = W // B
    deep = per_block * GROUP
    slots = W // deep
    place = lax.rem(lax.broadcasted_iota(jnp.int32, (8, W), 0), slots) == (
        lax.broadcasted_iota(jnp.int32, (8, W), 1) // deep
    )

    def lay(n, carry):
        for i in range(8):
            picked = [
                xt[pl.ds((B // 8 * r + B // 8 - 1 - n) * GROUP * 8 + 7 - i, GROUP, stride=8), :]
                for r in range(per_block)
            ]
            picked = jnp.concatenate(picked * (W // deep), axis=0).T
            for g in range(groups):
                at = pl.multiple_of((g * B + 8 * n + i) * 8, 8)
                lt[pl.ds(at, 8), :] = jnp.where(place, picked[8 * g : 8 * g + 8], 0.0)
        return carry

    lax.fori_loop(0, B // 8, lay, 0)

    for copy in passed:
        copy.wait_recv()
    sp32[:, :channels] = sbuf[...].astype(F32)
    st[...] = sp32[...].T[:rows_p].astype(BF16)
    own_w[...] = sp32[mine, :rows_p].astype(BF16)

    def process(c, gsp):
        for copy in c_waits[c]:
            copy.wait_recv()
        model = jnp.dot(st[...], cbuf[c], preferred_element_type=F32)
        resb[c, :channels, :] = (
            model[:channels] - signal_ref[:, c * chunk : (c + 1) * chunk].astype(F32)
        ).astype(BF16)
        residual = resb[c]
        grad = lax.dot_general(
            cbuf[c, mine, :], residual, (((1,), (1,)), ((), ())), preferred_element_type=F32
        )
        return grad if gsp is None else gsp + grad

    def project(c):
        projected = jnp.dot(own_w[...], resb[c], preferred_element_type=F32)
        projected = projected.astype(BF16).astype(F32)
        for b in range(per):
            at = hb + c * per + b
            put(pj.at[0], span, at, projected[:, b * W : (b + 1) * W])

    gsp = None
    for c in order + [0]:
        gsp = process(c, gsp)

    low = pl.ds(pl.multiple_of(core * (atoms // 2), atoms // 2), atoms // 2)
    other = pl.ds(pl.multiple_of((1 - core) * (atoms // 2), atoms // 2), atoms // 2)

    def swap(i, lanes):
        copy = pltpu.make_async_remote_copy(
            src_ref=part.at[i, other, lanes], dst_ref=recv1.at[i, :, lanes],
            send_sem=p_send.at[i], recv_sem=p_recv.at[i],
            device_id={"tm": partner}, device_id_type=MESH,
        )
        copy.start()
        return copy

    def encode(value):
        top = jnp.max(jnp.abs(value), axis=0, keepdims=True)
        up = jnp.where(top > TINY, STEPS / jnp.maximum(top, TINY), 0.0)
        shift = jnp.where(value < 0, -0.5, 0.5)
        return value * up + shift, top * (1.0 / STEPS)

    def spread(i, lanes, copy):
        copy.wait_recv()
        value, step = encode(part[i, low, lanes] + recv1[i, :, lanes])
        scale[i, me_z, :, lanes] = step
        refs = [half.at[i, me_z, :, lanes], scale.at[i, me_z, :, lanes]]
        if i == 0 and fold:
            rest = value[:, wide - W :]
            rest = jnp.where(
                low_lane, rest[: atoms // 4], pltpu.roll(rest[atoms // 4 :], W // 2, 1)
            )
            folded[me_z] = rest.astype(jnp.int32).astype(jnp.int16)
            lanes = slice(0, wide - W)
            refs[0] = half.at[i, me_z, :, lanes]
            refs.append(folded.at[me_z])
            value = value[:, : wide - W]
        half[i, me_z, :, lanes] = value.astype(jnp.int32).astype(jnp.int16)
        copies = []
        for d, peer in enumerate(z_peers):
            for n, ref in enumerate(refs):
                out = pltpu.make_async_remote_copy(
                    src_ref=ref, dst_ref=ref,
                    send_sem=z_send.at[i, n, d], recv_sem=z_recv.at[i, n, d],
                    device_id={"tm": peer * 2 + core}, device_id_type=MESH,
                )
                out.start()
                copies.append(out)
        return copies

    def finish(i, lanes, copies):
        for copy in copies:
            copy.wait_recv()
        acc = None
        for z in range(chips):
            if i == 0 and fold:
                rest = folded[z].astype(jnp.int32).astype(F32)
                rest = jnp.concatenate([rest, pltpu.roll(rest, W // 2, 1)], axis=0)
                value = half[i, z, :, : wide - W].astype(jnp.int32).astype(F32)
                value = jnp.concatenate([value, rest], axis=1)
            else:
                value = half[i, z, :, lanes].astype(jnp.int32).astype(F32)
            value = value * scale[i, z, :, lanes]
            acc = value if acc is None else acc + value
        total[i, low, lanes] = acc * factor
        copy = pltpu.make_async_remote_copy(
            src_ref=total.at[i, low, lanes], dst_ref=total.at[i, low, lanes],
            send_sem=f_send.at[i], recv_sem=f_recv.at[i],
            device_id={"tm": partner}, device_id_type=MESH,
        )
        copy.start()
        return copy

    fold = wide > W and channels - (wide - W) <= W // 2 and atoms % 64 == 0
    low_lane = lax.broadcasted_iota(jnp.int32, (atoms // 4, W), 1) < W // 2
    sp_lanes = slice(0, wide)
    tm_lanes = slice(0, length)
    part[0, :, :rows_p] = gsp
    if rows_p < wide:
        part[0, :, rows_p:] = jnp.zeros((atoms, wide - rows_p), F32)
    swap_sp = swap(0, sp_lanes)
    for c in range(chunks):
        project(c)

    lane = lax.broadcasted_iota(jnp.int32, (atoms, W), 1)
    for r in range(1, per_block):
        turned = [
            pltpu.roll(natural(pj.at[0], span, i), W - B * r, 1)
            for i in range(hb, hb + nb)
        ]
        turned = [jnp.zeros((atoms, W), F32)] + turned + [jnp.zeros((atoms, W), F32)]
        for n in range(nb + 1):
            put(
                pj.at[r], span, hb - 1 + n,
                jnp.where(lane < W - B * r, turned[n], turned[n + 1]),
            )

    depth = (length + B - 1) // W + 1

    def correlate(g, carry):
        for first_atom in range(0, 8, 2 * slots):
            some = range(first_atom, first_atom + 2 * slots)
            lhs = []
            rhs = []
            for i in some:
                left = series(lt, B, g, i, 0, B).astype(BF16)
                none = jnp.zeros((B, W), BF16)
                pair = [left, none] if i - first_atom < slots else [none, left]
                lhs.append(jnp.concatenate(pair, axis=1))
                for r in range(per_block):
                    rhs.append(
                        jnp.concatenate(
                            [series(pj.at[r], span, g, i, j, GROUP) for j in range(depth)], axis=1
                        )
                    )
            prods = jnp.dot(
                jnp.concatenate(lhs, axis=0),
                jnp.concatenate(rhs, axis=0).astype(BF16),
                preferred_element_type=F32,
            )
            for n, i in enumerate(some):
                prod = prods[n * B : (n + 1) * B]
                prod = pltpu.roll(prod, depth * W - (B - 1), 1, stride=1, stride_axis=0)
                acc = prod[:8, :length]
                for q in range(1, B // 8):
                    acc = acc + prod[8 * q : 8 * q + 8, :length]
                for d in range(hb):
                    at = pl.multiple_of((d * groups + g) * 64 + 8 * i, 8)
                    gt[pl.ds(at, 8), :] = acc[:, d * W : (d + 1) * W]
        return carry

    def lags(mine_first, rows):
        for d in range(hb):
            at = 8 * (d * atoms + mine_first)
            total_d = gt[pl.ds(at, atoms // 2, stride=8), :]
            for i in range(1, 8):
                total_d = total_d + gt[pl.ds(at + i, atoms // 2, stride=8), :]
            part[1, rows, d * W : (d + 1) * W] = total_d

    def correlate_from(start, count):
        lax.fori_loop(0, count, lambda n, carry: correlate(start + n, carry), 0, unroll=count)

    for turn in range(1, chips - 3):
        listen(turn)
        tell(turn + 1)
    if chips > 2:
        listen(chips - 3)
    spread_sp = spread(0, sp_lanes, swap_sp)
    correlate_from((1 - core) * (groups // 2), groups // 2)
    lags((1 - core) * (atoms // 2), other)
    swap_tm = swap(1, tm_lanes)
    correlate_from(core * (groups // 2), groups // 2)
    lags(core * (atoms // 2), low)
    spread_tm = spread(1, tm_lanes, swap_tm)
    last_sp = finish(0, sp_lanes, spread_sp)
    last_tm = finish(1, tm_lanes, spread_tm)
    last_sp.wait_recv()
    out_sp_ref[...] = total[0, :, :channels]
    last_tm.wait_recv()
    out_tm_ref[...] = total[1, :, :length]

    @pl.when(me_t < n_tm - 1)
    def _():
        halo_copy.wait_send()
        for copy in spill_copies:
            copy.wait_send()

    for copy in s_copies + passed + [copy for line in c_copies for copy in line]:
        copy.wait_send()
    for copy in [swap_sp, swap_tm, last_sp, last_tm] + spread_sp + spread_tm:
        copy.wait_send()


def local(n_atom, n_tm, signal, spatial, temporal, values, mask):
    atoms, channels = spatial.shape
    length = temporal.shape[1]
    samples = signal.shape[1]
    chunks = samples // length
    nb, hb = samples // W, length // W
    wide = -(-channels // W) * W
    rows_p = -(-channels // 32) * 32
    per_block = W // B
    deep = per_block * GROUP
    slots = W // deep
    place = lax.rem(lax.broadcasted_iota(jnp.int32, (8, W), 0), slots) == (
        lax.broadcasted_iota(jnp.int32, (8, W), 1) // deep
    )
    every = n_atom * atoms
    depth = (length + B - 1) // W + 1
    span = (GROUP + depth - 1) * atoms
    width = max(wide, length)
    chips = n_tm // 2
    factor = 1.0 / math.sqrt(samples * n_tm)
    dma = pltpu.SemaphoreType.DMA
    vmem = pl.BlockSpec(memory_space=pltpu.VMEM)
    return pl.pallas_call(
        functools.partial(kernel, n_atom, n_tm, factor),
        out_shape=(
            pltpu.VMEM((atoms, channels), F32),
            pltpu.VMEM((atoms, length), F32),
        ),
        in_specs=[vmem] * 5,
        out_specs=(vmem, vmem),
        scratch_shapes=[
            pltpu.VMEM((atoms, length), BF16),
            pltpu.VMEM((atoms, length), BF16),
            pltpu.VMEM((atoms, length), F32),
            pltpu.VMEM((atoms, length), F32),
            pltpu.VMEM(((GROUP + hb) * atoms, W), F32),
            pltpu.VMEM((GROUP * W, W), F32),
            pltpu.VMEM((hb * atoms, W), F32),
            pltpu.VMEM((GROUP * atoms, W), F32),
            pltpu.VMEM((chunks, every, length), BF16),
            pltpu.VMEM((every, channels), BF16),
            pltpu.VMEM((every, wide), F32),
            pltpu.VMEM((rows_p, every), BF16),
            pltpu.VMEM((atoms, rows_p), BF16),
            pltpu.VMEM((chunks, rows_p, length), BF16),
            pltpu.VMEM((per_block, span, W), F32),
            pltpu.VMEM((B * atoms, W), F32),
            pltpu.VMEM((8 * hb * atoms, W), F32),
            pltpu.VMEM((2, atoms, width), F32),
            pltpu.VMEM((2, atoms // 2, width), F32),
            pltpu.VMEM((2, chips, atoms // 2, width), jnp.int16),
            pltpu.VMEM((chips, max(atoms // 4, GROUP), W), jnp.int16),
            pltpu.VMEM((2, chips, 1, width), F32),
            pltpu.VMEM((2, atoms, width), F32),
            pltpu.SemaphoreType.REGULAR((max(chips - 2, 1), 2)),
            dma((6,)),
            dma((n_atom - 1,)),
            dma((n_atom - 1,)),
            dma((n_atom - 1,)),
            dma((n_atom - 1,)),
            dma((n_atom - 1, chunks, 2)),
            dma((n_atom - 1, chunks, 2)),
            dma((2,)),
            dma((2,)),
            dma((2, 3, chips - 1)),
            dma((2, 3, chips - 1)),
            dma((2,)),
            dma((2,)),
        ],
        compiler_params=pltpu.CompilerParams(collective_id=0, has_side_effects=True),
    )(signal, spatial, temporal, values, mask.T)


def settle(a_ref, b_ref, c_ref, d_ref, sems):
    one = pltpu.make_async_copy(a_ref, c_ref, sems.at[0])
    two = pltpu.make_async_copy(b_ref, d_ref, sems.at[1])
    one.start()
    two.start()
    one.wait()
    two.wait()


def placed(n_atom, n_tm, *args):
    first, second = local(n_atom, n_tm, *args)
    return pl.pallas_call(
        settle,
        out_shape=(
            jax.ShapeDtypeStruct(first.shape, F32),
            jax.ShapeDtypeStruct(second.shape, F32),
        ),
        in_specs=[pl.BlockSpec(memory_space=pltpu.VMEM)] * 2,
        out_specs=[pl.BlockSpec(memory_space=pltpu.HBM)] * 2,
        scratch_shapes=[pltpu.SemaphoreType.DMA((2,))],
        compiler_params=pltpu.CompilerParams(vmem_limit_bytes=1 << 20),
    )(first, second)


def solution(mesh):
    in_specs = (P(None, "tm"), P("atom", None), P("atom", None), P("atom", "tm"), P("atom", "tm"))
    out_specs = (P("atom", None), P("atom", None))
    body = functools.partial(placed, mesh.shape["atom"], mesh.shape["tm"])
    return jax.shard_map(body, mesh=mesh, in_specs=in_specs, out_specs=out_specs, check_vma=False)
```

```python
import functools
import math

import jax
import jax.numpy as jnp
from jax import lax
from jax.experimental import pallas as pl
from jax.experimental.pallas import tpu as pltpu
from jax.sharding import PartitionSpec as P

W = 128
B = 32
GROUP = 16
SPLIT = 2
MESH = pl.DeviceIdType.MESH
F32 = jnp.float32
BF16 = jnp.bfloat16
STEPS = 32767.0
TINY = 2.0**-112


def kernel(
    n_atom, n_tm, factor,
    signal_ref, spatial_ref, temporal_ref, values_ref, mask_ref,
    out_sp_ref, out_tm_ref,
    tail, halo, spill, spilled, cx, xt, wt, cf, cbuf, sbuf, sp32, st, own_w, resb, pj, lt, gt,
    part, recv1, half, folded, scale, total,
    heard, halo_sems, s_send, s_recv, h_send, h_recv, c_send, c_recv,
    p_send, p_recv, z_send, z_recv, f_send, f_recv,
):
    atoms, channels = spatial_ref.shape
    length = temporal_ref.shape[1]
    samples = signal_ref.shape[1]
    blocks = mask_ref.shape[0]
    block = samples // blocks
    nb = samples // W
    hb = length // W
    chunk = length
    chunks = samples // chunk
    per = chunk // W
    rows_p = st.shape[0]
    wide = sp32.shape[1]
    span = pj.shape[1] // atoms
    chips = n_tm // 2
    me_a = lax.axis_index("atom")
    me_t = lax.axis_index("tm")
    me_z = me_t // 2
    core = lax.rem(me_t, 2)
    partner = me_z * 2 + 1 - core

    def across(at, count):
        def flip(d):
            out = at
            for bit in range(d.bit_length()):
                if d >> bit & 1:
                    step = 1 << bit
                    out = out + step - 2 * step * lax.rem(at // step, 2)
            return out

        if count & (count - 1) == 0:
            return [flip(d) for d in range(count - 1, 0, -1)]
        return [lax.rem(at + d, count) for d in range(1, count)]

    def sources(at, count):
        if count & (count - 1) == 0:
            return across(at, count)
        return [lax.rem(at + count - d, count) for d in range(1, count)]

    a_peers = across(me_a, n_atom)
    z_peers = across(me_z, chips)
    mine = pl.ds(pl.multiple_of(me_a * atoms, atoms), atoms)

    barrier = pltpu.get_barrier_semaphore()
    for peer in a_peers:
        pl.semaphore_signal(barrier, inc=1, device_id={"atom": peer}, device_id_type=MESH)
    line = me_t - 1 + 2 * core
    beside = [
        (me_z > 0, me_t - 2),
        (me_z < chips - 1, me_t + 2),
        (jnp.logical_and(line >= 0, line < n_tm), line),
    ]

    def greet(peer):
        pl.semaphore_signal(barrier, inc=1, device_id={"tm": peer}, device_id_type=MESH)

    greet(partner)
    for there, peer in beside:
        pl.when(there)(functools.partial(greet, peer))

    def tell(turn):
        for n, (there, peer) in enumerate(beside[:2]):

            @pl.when(there)
            def _():
                pl.semaphore_signal(
                    heard.at[turn, 1 - n], inc=1, device_id={"tm": peer}, device_id_type=MESH
                )

    def listen(turn):
        for n, (there, peer) in enumerate(beside[:2]):

            @pl.when(there)
            def _():
                pl.semaphore_wait(heard.at[turn, n], 1)


    groups = atoms // 8

    def put(ref, count, b, value):
        for g in range(groups):
            ref[(g * count + b) * 8 : (g * count + b + 1) * 8, :] = value[8 * g : 8 * g + 8]

    def filtered(b, lo, hi):
        return jnp.concatenate(
            [
                cf[pl.ds((g * (GROUP // 8) + b // 8) * 64 + b % 8, 8, stride=8), :]
                for g in range(lo, hi)
            ],
            axis=0,
        )

    def natural(ref, count, b):
        return jnp.concatenate(
            [ref[(g * count + b) * 8 : (g * count + b + 1) * 8, :] for g in range(groups)], axis=0
        )

    def series(ref, count, g, i, first, size):
        return ref[pl.ds((g * count + first) * 8 + i, size, stride=8), :]

    mask = mask_ref[...].astype(F32).T
    codes = [
        values_ref[:, j * block : (j + 1) * block].astype(F32) * mask[:, j : j + 1]
        for j in range(blocks)
    ]
    codes = jnp.concatenate(codes, axis=1)
    tail[...] = codes[:, samples - length :].astype(BF16)
    gap = jnp.zeros((atoms, W), F32)
    for b in list(range(hb)) + list(range(hb + nb, GROUP + hb)):
        put(cx, GROUP + hb, b, gap)
    for b in range(nb):
        put(cx, GROUP + hb, hb + b, codes[:, b * W : (b + 1) * W])
    for d in range(hb):
        wt[d * atoms : (d + 1) * atoms, :] = temporal_ref[:, d * W : (d + 1) * W].astype(F32)

    row = lax.broadcasted_iota(jnp.int32, (W, W), 0)
    col = lax.broadcasted_iota(jnp.int32, (W, W), 1)
    ahead = col >= row

    def toeplitz(rows, i):
        circ = []
        for d in range(hb):
            base = jnp.broadcast_to(rows[d][i : i + 1], (GROUP, W))
            base = pltpu.roll(base, 0, 1, stride=1, stride_axis=0).astype(BF16)
            tiles = [base] + [pltpu.roll(base, GROUP * n, 1) for n in range(1, W // GROUP)]
            circ.append(jnp.concatenate(tiles, axis=0))
        zero = jnp.zeros((W, W), BF16)
        parts = []
        for d in range(hb, -1, -1):
            near = circ[d] if d < hb else zero
            far = circ[d - 1] if d > 0 else zero
            parts.append(jnp.where(ahead, near, far))
        return jnp.concatenate(parts, axis=0)

    def windows(g, i):
        return jnp.concatenate(
            [series(cx, GROUP + hb, g, i, j, GROUP) for j in range(hb + 1)], axis=1
        )

    def first(g, carry):
        rows = [
            wt[pl.ds(pl.multiple_of(d * atoms + 8 * g, 8), 8), :] for d in range(hb)
        ]
        for i in range(0, 8, 2):
            taps = jnp.concatenate([toeplitz(rows, i), toeplitz(rows, i + 1)], axis=1)
            lhs = jnp.concatenate([windows(g, i), windows(g, i + 1)], axis=0).astype(BF16)
            out = jnp.dot(lhs, taps, preferred_element_type=F32)
            for n in range(2):
                for h in range(GROUP // 8):
                    at = pl.multiple_of(((g * (GROUP // 8) + h) * 8 + i + n) * 8, 8)
                    row = n * GROUP + 8 * h
                    cf[pl.ds(at, 8), :] = out[row : row + 8, n * W : (n + 1) * W]
        return carry

    lax.fori_loop(0, SPLIT * groups // 4 // 2 * 2, first, 0, unroll=4)

    present = n_atom
    for there, _ in beside:
        present = present + jnp.where(there, 1, 0)
    pl.semaphore_wait(barrier, present)
    if chips > 2:
        tell(0)

    right = lax.rem(me_t + 1, n_tm)
    halo_copy = pltpu.make_async_remote_copy(
        src_ref=tail, dst_ref=halo, send_sem=halo_sems.at[0], recv_sem=halo_sems.at[1],
        device_id={"tm": right}, device_id_type=MESH,
    )

    spill_copies = []

    def send_spill(n, lo, hi):
        rows = slice(8 * lo, 8 * hi)
        for b in range(hb):
            spill[rows, b * W : (b + 1) * W] = filtered(nb + b, lo, hi)
        copy = pltpu.make_async_remote_copy(
            src_ref=spill.at[rows], dst_ref=spilled.at[rows],
            send_sem=halo_sems.at[2 + n], recv_sem=halo_sems.at[4 + n],
            device_id={"tm": right}, device_id_type=MESH,
        )
        spill_copies.append(copy)

        @pl.when(me_t < n_tm - 1)
        def _():
            copy.start()

    c_copies = [[] for _ in range(chunks)]
    c_waits = [[] for _ in range(chunks)]
    firsts = {}
    relays = {}
    if n_atom == 4:
        relays = {c: (2, 1) if c % 2 else (1, 2) for c in range(1, chunks)}
    order = [chunks - 1] + list(range(1, chunks - 1))

    def send(c, lo, hi):
        rows = pl.ds(pl.multiple_of(me_a * atoms + 8 * lo, 8 * (hi - lo)), 8 * (hi - lo))
        for b in range(per):
            value = filtered(c * per + b, lo, hi)
            if c == 0:
                value = value + spilled[8 * lo : 8 * hi, b * W : (b + 1) * W]
            cbuf[c, rows, b * W : (b + 1) * W] = value.astype(BF16)
        for d, peer in enumerate(a_peers):
            if c in relays and lo == 0 and d == 0:
                continue
            copy = pltpu.make_async_remote_copy(
                src_ref=cbuf.at[c, rows], dst_ref=cbuf.at[c, rows],
                send_sem=c_send.at[d, c, min(lo, 1)], recv_sem=c_recv.at[d, c, min(lo, 1)],
                device_id={"atom": peer}, device_id_type=MESH,
            )
            copy.start()
            c_copies[c].append(copy)
            c_waits[c].append(copy)
            firsts[c, d, min(lo, 1)] = copy

    def relay(c):
        source, target = relays[c]
        copy = firsts[c, source, 0]
        copy.wait_recv()
        c_waits[c] = [other_copy for other_copy in c_waits[c] if other_copy is not copy]
        rows = pl.ds(pl.multiple_of(a_peers[source] * atoms, atoms), 8 * early)
        copy = pltpu.make_async_remote_copy(
            src_ref=cbuf.at[c, rows], dst_ref=cbuf.at[c, rows],
            send_sem=c_send.at[0, c, 0], recv_sem=c_recv.at[0, c, 0],
            device_id={"atom": a_peers[target]}, device_id_type=MESH,
        )
        copy.start()
        c_copies[c].append(copy)
        c_waits[c].append(copy)

    early = SPLIT * groups // 4 // 2 * 2
    send_spill(0, 0, early)

    @pl.when(me_t < n_tm - 1)
    def _():
        halo_copy.start()

    for c in relays:
        send(c, 0, early)

    s_copies = []
    own_half = pl.ds(pl.multiple_of(core * (atoms // 2), atoms // 2), atoms // 2)

    def half_of(peer):
        at = peer * atoms + core * (atoms // 2)
        return pl.ds(pl.multiple_of(at, atoms // 2), atoms // 2)

    for d, peer in enumerate(a_peers):
        copy = pltpu.make_async_remote_copy(
            src_ref=spatial_ref.at[own_half], dst_ref=sbuf.at[half_of(me_a)],
            send_sem=s_send.at[d], recv_sem=s_recv.at[d],
            device_id={"atom": peer}, device_id_type=MESH,
        )
        copy.start()
        s_copies.append(copy)
    for c in range(1, chunks):
        if c not in relays:
            send(c, 0, early)
    lax.fori_loop(early, groups, first, 0, unroll=4)
    send_spill(1, early, groups)
    for c in order:
        send(c, early, groups)

    def lay_time(b, value):
        turned = value.T
        for u in range(W // 8):
            at = (u * GROUP + b) * 8
            xt[at : at + 8, :atoms] = turned[8 * u : 8 * u + 8]

    for b in range(nb):
        lay_time(hb + b, codes[:, b * W : (b + 1) * W])
    for u in range(W // 8):
        xt[(u * GROUP + hb + nb) * 8 : (u + 1) * GROUP * 8, :] = jnp.zeros(
            ((GROUP - hb - nb) * 8, W), F32
        )
    pj[...] = jnp.zeros(pj.shape, F32)
    resb[:, channels // 16 * 16 :, :] = jnp.zeros(
        (chunks, rows_p - channels // 16 * 16, chunk), BF16
    )
    sp32[...] = jnp.zeros(sp32.shape, F32)

    for c in relays:
        relay(c)

    @pl.when(me_t == 0)
    def _():
        halo[...] = jnp.zeros(halo.shape, halo.dtype)
        spilled[...] = jnp.zeros(spilled.shape, F32)

    @pl.when(me_t > 0)
    def _():
        for copy in spill_copies:
            copy.wait_recv()

    send(0, 0, groups)
    if chips > 3:
        listen(0)
        tell(1)

    sbuf[mine, :] = spatial_ref[...]
    passed = []
    for d, source in enumerate(sources(me_a, n_atom)):
        s_copies[d].wait_recv()
        rows = half_of(source)
        out = pltpu.make_async_remote_copy(
            src_ref=sbuf.at[rows], dst_ref=sbuf.at[rows],
            send_sem=h_send.at[d], recv_sem=h_recv.at[d],
            device_id={"tm": partner}, device_id_type=MESH,
        )
        out.start()
        passed.append(out)

    @pl.when(me_t > 0)
    def _():
        halo_copy.wait_recv()

    before = halo[...].astype(F32)
    for b in range(hb):
        lay_time(b, before[:, b * W : (b + 1) * W])

    per_block = W // B
    deep = per_block * GROUP
    slots = W // deep
    place = lax.rem(lax.broadcasted_iota(jnp.int32, (8, W), 0), slots) == (
        lax.broadcasted_iota(jnp.int32, (8, W), 1) // deep
    )

    def lay(n, carry):
        for i in range(8):
            picked = [
                xt[pl.ds((B // 8 * r + B // 8 - 1 - n) * GROUP * 8 + 7 - i, GROUP, stride=8), :]
                for r in range(per_block)
            ]
            picked = jnp.concatenate(picked * (W // deep), axis=0).T
            for g in range(groups):
                at = pl.multiple_of((g * B + 8 * n + i) * 8, 8)
                lt[pl.ds(at, 8), :] = jnp.where(place, picked[8 * g : 8 * g + 8], 0.0)
        return carry

    lax.fori_loop(0, B // 8, lay, 0)

    for copy in passed:
        copy.wait_recv()
    sp32[:, :channels] = sbuf[...].astype(F32)
    st[...] = sp32[...].T[:rows_p].astype(BF16)
    own_w[...] = sp32[mine, :rows_p].astype(BF16)

    def process(c, gsp):
        for copy in c_waits[c]:
            copy.wait_recv()
        model = jnp.dot(st[...], cbuf[c], preferred_element_type=F32)
        resb[c, :channels, :] = (
            model[:channels] - signal_ref[:, c * chunk : (c + 1) * chunk].astype(F32)
        ).astype(BF16)
        residual = resb[c]
        grad = lax.dot_general(
            cbuf[c, mine, :], residual, (((1,), (1,)), ((), ())), preferred_element_type=F32
        )
        return grad if gsp is None else gsp + grad

    def project(c):
        projected = jnp.dot(own_w[...], resb[c], preferred_element_type=F32)
        projected = projected.astype(BF16).astype(F32)
        for b in range(per):
            at = hb + c * per + b
            put(pj.at[0], span, at, projected[:, b * W : (b + 1) * W])

    gsp = None
    for c in order + [0]:
        gsp = process(c, gsp)

    low = pl.ds(pl.multiple_of(core * (atoms // 2), atoms // 2), atoms // 2)
    other = pl.ds(pl.multiple_of((1 - core) * (atoms // 2), atoms // 2), atoms // 2)

    def swap(i, lanes):
        copy = pltpu.make_async_remote_copy(
            src_ref=part.at[i, other, lanes], dst_ref=recv1.at[i, :, lanes],
            send_sem=p_send.at[i], recv_sem=p_recv.at[i],
            device_id={"tm": partner}, device_id_type=MESH,
        )
        return copy

    def encode(value):
        top = jnp.max(jnp.abs(value), axis=0, keepdims=True)
        up = jnp.where(top > TINY, STEPS / jnp.maximum(top, TINY), 0.0)
        shift = jnp.where(value < 0, -0.5, 0.5)
        return value * up + shift, top * (1.0 / STEPS)

    def spread(i, lanes, copy):
        copy.wait_recv()
        value, step = encode(part[i, low, lanes] + recv1[i, :, lanes])
        scale[i, me_z, :, lanes] = step
        refs = [half.at[i, me_z, :, lanes], scale.at[i, me_z, :, lanes]]
        if i == 0 and fold:
            rest = value[:, wide - W :]
            rest = jnp.where(
                low_lane, rest[: atoms // 4], pltpu.roll(rest[atoms // 4 :], W // 2, 1)
            )
            folded[me_z] = rest.astype(jnp.int32).astype(jnp.int16)
            lanes = slice(0, wide - W)
            refs[0] = half.at[i, me_z, :, lanes]
            refs.append(folded.at[me_z])
            value = value[:, : wide - W]
        half[i, me_z, :, lanes] = value.astype(jnp.int32).astype(jnp.int16)
        copies = []
        for d, peer in enumerate(z_peers):
            for n, ref in enumerate(refs):
                out = pltpu.make_async_remote_copy(
                    src_ref=ref, dst_ref=ref,
                    send_sem=z_send.at[i, n, d], recv_sem=z_recv.at[i, n, d],
                    device_id={"tm": peer * 2 + core}, device_id_type=MESH,
                )
                out.start()
                copies.append(out)
        return copies

    def finish(i, lanes, copies):
        for copy in copies:
            copy.wait_recv()
        acc = None
        for z in range(chips):
            if i == 0 and fold:
                rest = folded[z].astype(jnp.int32).astype(F32)
                rest = jnp.concatenate([rest, pltpu.roll(rest, W // 2, 1)], axis=0)
                value = half[i, z, :, : wide - W].astype(jnp.int32).astype(F32)
                value = jnp.concatenate([value, rest], axis=1)
            else:
                value = half[i, z, :, lanes].astype(jnp.int32).astype(F32)
            value = value * scale[i, z, :, lanes]
            acc = value if acc is None else acc + value
        total[i, low, lanes] = acc * factor
        copy = pltpu.make_async_remote_copy(
            src_ref=total.at[i, low, lanes], dst_ref=total.at[i, low, lanes],
            send_sem=f_send.at[i], recv_sem=f_recv.at[i],
            device_id={"tm": partner}, device_id_type=MESH,
        )
        copy.start()
        return copy

    fold = wide > W and channels - (wide - W) <= W // 2 and atoms % 64 == 0
    low_lane = lax.broadcasted_iota(jnp.int32, (atoms // 4, W), 1) < W // 2
    sp_lanes = slice(0, wide)
    tm_lanes = slice(0, length)
    part[0, :, :rows_p] = gsp
    if rows_p < wide:
        part[0, :, rows_p:] = jnp.zeros((atoms, wide - rows_p), F32)
    swap_sp = swap(0, sp_lanes)
    swap_sp.start()
    for c in range(chunks):
        project(c)

    lane = lax.broadcasted_iota(jnp.int32, (atoms, W), 1)
    for r in range(1, per_block):
        turned = [
            pltpu.roll(natural(pj.at[0], span, i), W - B * r, 1)
            for i in range(hb, hb + nb)
        ]
        turned = [jnp.zeros((atoms, W), F32)] + turned + [jnp.zeros((atoms, W), F32)]
        for n in range(nb + 1):
            put(
                pj.at[r], span, hb - 1 + n,
                jnp.where(lane < W - B * r, turned[n], turned[n + 1]),
            )

    depth = (length + B - 1) // W + 1

    def correlate(g, carry):
        for first_atom in range(0, 8, 2 * slots):
            some = range(first_atom, first_atom + 2 * slots)
            lhs = []
            rhs = []
            for i in some:
                left = series(lt, B, g, i, 0, B).astype(BF16)
                none = jnp.zeros((B, W), BF16)
                pair = [left, none] if i - first_atom < slots else [none, left]
                lhs.append(jnp.concatenate(pair, axis=1))
                for r in range(per_block):
                    rhs.append(
                        jnp.concatenate(
                            [series(pj.at[r], span, g, i, j, GROUP) for j in range(depth)], axis=1
                        )
                    )
            prods = jnp.dot(
                jnp.concatenate(lhs, axis=0),
                jnp.concatenate(rhs, axis=0).astype(BF16),
                preferred_element_type=F32,
            )
            for n, i in enumerate(some):
                prod = prods[n * B : (n + 1) * B]
                prod = pltpu.roll(prod, depth * W - (B - 1), 1, stride=1, stride_axis=0)
                acc = prod[:8, :length]
                for q in range(1, B // 8):
                    acc = acc + prod[8 * q : 8 * q + 8, :length]
                for d in range(hb):
                    at = pl.multiple_of((d * groups + g) * 64 + 8 * i, 8)
                    gt[pl.ds(at, 8), :] = acc[:, d * W : (d + 1) * W]
        return carry

    def lags(mine_first, rows):
        for d in range(hb):
            at = 8 * (d * atoms + mine_first)
            total_d = gt[pl.ds(at, atoms // 2, stride=8), :]
            for i in range(1, 8):
                total_d = total_d + gt[pl.ds(at + i, atoms // 2, stride=8), :]
            part[1, rows, d * W : (d + 1) * W] = total_d

    def correlate_from(start, count):
        lax.fori_loop(0, count, lambda n, carry: correlate(start + n, carry), 0, unroll=count)

    swap_tm = swap(1, tm_lanes)

    def theirs():
        correlate_from((1 - core) * (groups // 2), groups // 2)
        lags((1 - core) * (atoms // 2), other)
        swap_tm.start()

    pl.when(core == 1)(theirs)
    for turn in range(1, chips - 3):
        listen(turn)
        tell(turn + 1)
    if chips > 2:
        listen(chips - 3)
    spread_sp = spread(0, sp_lanes, swap_sp)
    pl.when(core == 0)(theirs)
    correlate_from(core * (groups // 2), groups // 2)
    lags(core * (atoms // 2), low)
    spread_tm = spread(1, tm_lanes, swap_tm)
    last_sp = finish(0, sp_lanes, spread_sp)
    last_tm = finish(1, tm_lanes, spread_tm)
    last_sp.wait_recv()
    out_sp_ref[...] = total[0, :, :channels]
    last_tm.wait_recv()
    out_tm_ref[...] = total[1, :, :length]

    @pl.when(me_t < n_tm - 1)
    def _():
        halo_copy.wait_send()
        for copy in spill_copies:
            copy.wait_send()

    for copy in s_copies + passed + [copy for line in c_copies for copy in line]:
        copy.wait_send()
    for copy in [swap_sp, swap_tm, last_sp, last_tm] + spread_sp + spread_tm:
        copy.wait_send()


def local(n_atom, n_tm, signal, spatial, temporal, values, mask):
    atoms, channels = spatial.shape
    length = temporal.shape[1]
    samples = signal.shape[1]
    chunks = samples // length
    nb, hb = samples // W, length // W
    wide = -(-channels // W) * W
    rows_p = -(-channels // 32) * 32
    per_block = W // B
    deep = per_block * GROUP
    slots = W // deep
    place = lax.rem(lax.broadcasted_iota(jnp.int32, (8, W), 0), slots) == (
        lax.broadcasted_iota(jnp.int32, (8, W), 1) // deep
    )
    every = n_atom * atoms
    depth = (length + B - 1) // W + 1
    span = (GROUP + depth - 1) * atoms
    width = max(wide, length)
    chips = n_tm // 2
    factor = 1.0 / math.sqrt(samples * n_tm)
    dma = pltpu.SemaphoreType.DMA
    vmem = pl.BlockSpec(memory_space=pltpu.VMEM)
    return pl.pallas_call(
        functools.partial(kernel, n_atom, n_tm, factor),
        out_shape=(
            pltpu.VMEM((atoms, channels), F32),
            pltpu.VMEM((atoms, length), F32),
        ),
        in_specs=[vmem] * 5,
        out_specs=(vmem, vmem),
        scratch_shapes=[
            pltpu.VMEM((atoms, length), BF16),
            pltpu.VMEM((atoms, length), BF16),
            pltpu.VMEM((atoms, length), F32),
            pltpu.VMEM((atoms, length), F32),
            pltpu.VMEM(((GROUP + hb) * atoms, W), F32),
            pltpu.VMEM((GROUP * W, W), F32),
            pltpu.VMEM((hb * atoms, W), F32),
            pltpu.VMEM((GROUP * atoms, W), F32),
            pltpu.VMEM((chunks, every, length), BF16),
            pltpu.VMEM((every, channels), BF16),
            pltpu.VMEM((every, wide), F32),
            pltpu.VMEM((rows_p, every), BF16),
            pltpu.VMEM((atoms, rows_p), BF16),
            pltpu.VMEM((chunks, rows_p, length), BF16),
            pltpu.VMEM((per_block, span, W), F32),
            pltpu.VMEM((B * atoms, W), F32),
            pltpu.VMEM((8 * hb * atoms, W), F32),
            pltpu.VMEM((2, atoms, width), F32),
            pltpu.VMEM((2, atoms // 2, width), F32),
            pltpu.VMEM((2, chips, atoms // 2, width), jnp.int16),
            pltpu.VMEM((chips, max(atoms // 4, GROUP), W), jnp.int16),
            pltpu.VMEM((2, chips, 1, width), F32),
            pltpu.VMEM((2, atoms, width), F32),
            pltpu.SemaphoreType.REGULAR((max(chips - 2, 1), 2)),
            dma((6,)),
            dma((n_atom - 1,)),
            dma((n_atom - 1,)),
            dma((n_atom - 1,)),
            dma((n_atom - 1,)),
            dma((n_atom - 1, chunks, 2)),
            dma((n_atom - 1, chunks, 2)),
            dma((2,)),
            dma((2,)),
            dma((2, 3, chips - 1)),
            dma((2, 3, chips - 1)),
            dma((2,)),
            dma((2,)),
        ],
        compiler_params=pltpu.CompilerParams(collective_id=0, has_side_effects=True),
    )(signal, spatial, temporal, values, mask.T)


def settle(a_ref, b_ref, c_ref, d_ref, sems):
    one = pltpu.make_async_copy(a_ref, c_ref, sems.at[0])
    two = pltpu.make_async_copy(b_ref, d_ref, sems.at[1])
    one.start()
    two.start()
    one.wait()
    two.wait()


def placed(n_atom, n_tm, *args):
    first, second = local(n_atom, n_tm, *args)
    return pl.pallas_call(
        settle,
        out_shape=(
            jax.ShapeDtypeStruct(first.shape, F32),
            jax.ShapeDtypeStruct(second.shape, F32),
        ),
        in_specs=[pl.BlockSpec(memory_space=pltpu.VMEM)] * 2,
        out_specs=[pl.BlockSpec(memory_space=pltpu.HBM)] * 2,
        scratch_shapes=[pltpu.SemaphoreType.DMA((2,))],
        compiler_params=pltpu.CompilerParams(vmem_limit_bytes=1 << 20),
    )(first, second)


def solution(mesh):
    in_specs = (P(None, "tm"), P("atom", None), P("atom", None), P("atom", "tm"), P("atom", "tm"))
    out_specs = (P("atom", None), P("atom", None))
    body = functools.partial(placed, mesh.shape["atom"], mesh.shape["tm"])
    return jax.shard_map(body, mesh=mesh, in_specs=in_specs, out_specs=out_specs, check_vma=False)
```

```python
import functools
import math

import jax
import jax.numpy as jnp
from jax import lax
from jax.experimental import pallas as pl
from jax.experimental.pallas import tpu as pltpu
from jax.sharding import PartitionSpec as P

W = 128
B = 32
GROUP = 16
SPLIT = 2
MESH = pl.DeviceIdType.MESH
F32 = jnp.float32
BF16 = jnp.bfloat16
STEPS = 32767.0
TINY = 2.0**-112


def kernel(
    n_atom, n_tm, factor,
    signal_ref, spatial_ref, temporal_ref, values_ref, mask_ref,
    out_sp_ref, out_tm_ref,
    tail, halo, spill, spilled, cx, xt, wt, cf, cbuf, sbuf, sp32, st, own_w, resb, pj, lt, gt,
    part, recv1, half, folded, scale, total,
    heard, halo_sems, s_send, s_recv, h_send, h_recv, c_send, c_recv,
    p_send, p_recv, z_send, z_recv, f_send, f_recv,
):
    atoms, channels = spatial_ref.shape
    length = temporal_ref.shape[1]
    samples = signal_ref.shape[1]
    blocks = mask_ref.shape[0]
    block = samples // blocks
    nb = samples // W
    hb = length // W
    chunk = length
    chunks = samples // chunk
    per = chunk // W
    rows_p = st.shape[0]
    wide = sp32.shape[1]
    span = pj.shape[1] // atoms
    chips = n_tm // 2
    me_a = lax.axis_index("atom")
    me_t = lax.axis_index("tm")
    me_z = me_t // 2
    core = lax.rem(me_t, 2)
    partner = me_z * 2 + 1 - core

    def across(at, count):
        def flip(d):
            out = at
            for bit in range(d.bit_length()):
                if d >> bit & 1:
                    step = 1 << bit
                    out = out + step - 2 * step * lax.rem(at // step, 2)
            return out

        if count & (count - 1) == 0:
            return [flip(d) for d in range(count - 1, 0, -1)]
        return [lax.rem(at + d, count) for d in range(1, count)]

    def sources(at, count):
        if count & (count - 1) == 0:
            return across(at, count)
        return [lax.rem(at + count - d, count) for d in range(1, count)]

    a_peers = across(me_a, n_atom)
    z_peers = across(me_z, chips)
    mine = pl.ds(pl.multiple_of(me_a * atoms, atoms), atoms)

    barrier = pltpu.get_barrier_semaphore()
    for peer in a_peers:
        pl.semaphore_signal(barrier, inc=1, device_id={"atom": peer}, device_id_type=MESH)
    line = me_t - 1 + 2 * core
    beside = [
        (me_z > 0, me_t - 2),
        (me_z < chips - 1, me_t + 2),
        (jnp.logical_and(line >= 0, line < n_tm), line),
    ]

    def greet(peer):
        pl.semaphore_signal(barrier, inc=1, device_id={"tm": peer}, device_id_type=MESH)

    greet(partner)
    for there, peer in beside:
        pl.when(there)(functools.partial(greet, peer))

    def tell(turn):
        for n, (there, peer) in enumerate(beside[:2]):

            @pl.when(there)
            def _():
                pl.semaphore_signal(
                    heard.at[turn, 1 - n], inc=1, device_id={"tm": peer}, device_id_type=MESH
                )

    def listen(turn):
        for n, (there, peer) in enumerate(beside[:2]):

            @pl.when(there)
            def _():
                pl.semaphore_wait(heard.at[turn, n], 1)


    groups = atoms // 8

    def put(ref, count, b, value):
        for g in range(groups):
            ref[(g * count + b) * 8 : (g * count + b + 1) * 8, :] = value[8 * g : 8 * g + 8]

    def filtered(b, lo, hi):
        return jnp.concatenate(
            [
                cf[pl.ds((g * (GROUP // 8) + b // 8) * 64 + b % 8, 8, stride=8), :]
                for g in range(lo, hi)
            ],
            axis=0,
        )

    def natural(ref, count, b):
        return jnp.concatenate(
            [ref[(g * count + b) * 8 : (g * count + b + 1) * 8, :] for g in range(groups)], axis=0
        )

    def series(ref, count, g, i, first, size):
        return ref[pl.ds((g * count + first) * 8 + i, size, stride=8), :]

    mask = mask_ref[...].astype(F32).T
    codes = [
        values_ref[:, j * block : (j + 1) * block].astype(F32) * mask[:, j : j + 1]
        for j in range(blocks)
    ]
    codes = jnp.concatenate(codes, axis=1)
    tail[...] = codes[:, samples - length :].astype(BF16)
    gap = jnp.zeros((atoms, W), F32)
    for b in list(range(hb)) + list(range(hb + nb, GROUP + hb)):
        put(cx, GROUP + hb, b, gap)
    for b in range(nb):
        put(cx, GROUP + hb, hb + b, codes[:, b * W : (b + 1) * W])
    for d in range(hb):
        wt[d * atoms : (d + 1) * atoms, :] = temporal_ref[:, d * W : (d + 1) * W].astype(F32)

    row = lax.broadcasted_iota(jnp.int32, (W, W), 0)
    col = lax.broadcasted_iota(jnp.int32, (W, W), 1)
    ahead = col >= row

    def toeplitz(rows, i):
        circ = []
        for d in range(hb):
            base = jnp.broadcast_to(rows[d][i : i + 1], (GROUP, W))
            base = pltpu.roll(base, 0, 1, stride=1, stride_axis=0).astype(BF16)
            tiles = [base] + [pltpu.roll(base, GROUP * n, 1) for n in range(1, W // GROUP)]
            circ.append(jnp.concatenate(tiles, axis=0))
        zero = jnp.zeros((W, W), BF16)
        parts = []
        for d in range(hb, -1, -1):
            near = circ[d] if d < hb else zero
            far = circ[d - 1] if d > 0 else zero
            parts.append(jnp.where(ahead, near, far))
        return jnp.concatenate(parts, axis=0)

    def windows(g, i):
        return jnp.concatenate(
            [series(cx, GROUP + hb, g, i, j, GROUP) for j in range(hb + 1)], axis=1
        )

    def first(g, carry):
        rows = [
            wt[pl.ds(pl.multiple_of(d * atoms + 8 * g, 8), 8), :] for d in range(hb)
        ]
        for i in range(0, 8, 2):
            taps = jnp.concatenate([toeplitz(rows, i), toeplitz(rows, i + 1)], axis=1)
            lhs = jnp.concatenate([windows(g, i), windows(g, i + 1)], axis=0).astype(BF16)
            out = jnp.dot(lhs, taps, preferred_element_type=F32)
            for n in range(2):
                for h in range(GROUP // 8):
                    at = pl.multiple_of(((g * (GROUP // 8) + h) * 8 + i + n) * 8, 8)
                    row = n * GROUP + 8 * h
                    cf[pl.ds(at, 8), :] = out[row : row + 8, n * W : (n + 1) * W]
        return carry

    lax.fori_loop(0, SPLIT * groups // 4 // 2 * 2, first, 0, unroll=4)

    @pl.when(me_a == 0)
    def _():
        lax.fori_loop(SPLIT * groups // 4 // 2 * 2, groups, first, 0, unroll=4)


    present = n_atom
    for there, _ in beside:
        present = present + jnp.where(there, 1, 0)
    pl.semaphore_wait(barrier, present)
    if chips > 2:
        tell(0)

    right = lax.rem(me_t + 1, n_tm)
    halo_copy = pltpu.make_async_remote_copy(
        src_ref=tail, dst_ref=halo, send_sem=halo_sems.at[0], recv_sem=halo_sems.at[1],
        device_id={"tm": right}, device_id_type=MESH,
    )

    spill_copies = []

    def send_spill(n, lo, hi):
        rows = slice(8 * lo, 8 * hi)
        for b in range(hb):
            spill[rows, b * W : (b + 1) * W] = filtered(nb + b, lo, hi)
        copy = pltpu.make_async_remote_copy(
            src_ref=spill.at[rows], dst_ref=spilled.at[rows],
            send_sem=halo_sems.at[2 + n], recv_sem=halo_sems.at[4 + n],
            device_id={"tm": right}, device_id_type=MESH,
        )
        spill_copies.append(copy)

        @pl.when(me_t < n_tm - 1)
        def _():
            copy.start()

    c_copies = [[] for _ in range(chunks)]
    c_waits = [[] for _ in range(chunks)]
    firsts = {}
    relays = {}
    if n_atom == 4:
        relays = {c: (2, 1) if c % 2 else (1, 2) for c in range(1, chunks)}
    order = list(range(1, chunks))

    def send(c, lo, hi):
        rows = pl.ds(pl.multiple_of(me_a * atoms + 8 * lo, 8 * (hi - lo)), 8 * (hi - lo))
        for b in range(per):
            value = filtered(c * per + b, lo, hi)
            if c == 0:
                value = value + spilled[8 * lo : 8 * hi, b * W : (b + 1) * W]
            cbuf[c, rows, b * W : (b + 1) * W] = value.astype(BF16)
        for d, peer in enumerate(a_peers):
            if c in relays and lo == 0 and d == 0:
                continue
            copy = pltpu.make_async_remote_copy(
                src_ref=cbuf.at[c, rows], dst_ref=cbuf.at[c, rows],
                send_sem=c_send.at[d, c, min(lo, 1)], recv_sem=c_recv.at[d, c, min(lo, 1)],
                device_id={"atom": peer}, device_id_type=MESH,
            )
            copy.start()
            c_copies[c].append(copy)
            c_waits[c].append(copy)
            firsts[c, d, min(lo, 1)] = copy

    def relay(c):
        source, target = relays[c]
        copy = firsts[c, source, 0]
        copy.wait_recv()
        c_waits[c] = [other_copy for other_copy in c_waits[c] if other_copy is not copy]
        rows = pl.ds(pl.multiple_of(a_peers[source] * atoms, atoms), 8 * early)
        copy = pltpu.make_async_remote_copy(
            src_ref=cbuf.at[c, rows], dst_ref=cbuf.at[c, rows],
            send_sem=c_send.at[0, c, 0], recv_sem=c_recv.at[0, c, 0],
            device_id={"atom": a_peers[target]}, device_id_type=MESH,
        )
        copy.start()
        c_copies[c].append(copy)
        c_waits[c].append(copy)

    early = SPLIT * groups // 4 // 2 * 2
    send_spill(0, 0, early)

    @pl.when(me_t < n_tm - 1)
    def _():
        halo_copy.start()

    for c in relays:
        send(c, 0, early)

    s_copies = []
    own_half = pl.ds(pl.multiple_of(core * (atoms // 2), atoms // 2), atoms // 2)

    def half_of(peer):
        at = peer * atoms + core * (atoms // 2)
        return pl.ds(pl.multiple_of(at, atoms // 2), atoms // 2)

    for d, peer in enumerate(a_peers):
        copy = pltpu.make_async_remote_copy(
            src_ref=spatial_ref.at[own_half], dst_ref=sbuf.at[half_of(me_a)],
            send_sem=s_send.at[d], recv_sem=s_recv.at[d],
            device_id={"atom": peer}, device_id_type=MESH,
        )
        copy.start()
        s_copies.append(copy)
    for c in range(1, chunks):
        if c not in relays:
            send(c, 0, early)
    @pl.when(me_a > 0)
    def _():
        lax.fori_loop(early, groups, first, 0, unroll=4)

    send_spill(1, early, groups)
    for c in order:
        send(c, early, groups)

    def lay_time(b, value):
        turned = value.T
        for u in range(W // 8):
            at = (u * GROUP + b) * 8
            xt[at : at + 8, :atoms] = turned[8 * u : 8 * u + 8]

    for b in range(nb):
        lay_time(hb + b, codes[:, b * W : (b + 1) * W])
    for u in range(W // 8):
        xt[(u * GROUP + hb + nb) * 8 : (u + 1) * GROUP * 8, :] = jnp.zeros(
            ((GROUP - hb - nb) * 8, W), F32
        )
    pj[...] = jnp.zeros(pj.shape, F32)
    resb[:, channels // 16 * 16 :, :] = jnp.zeros(
        (chunks, rows_p - channels // 16 * 16, chunk), BF16
    )
    sp32[...] = jnp.zeros(sp32.shape, F32)

    for c in relays:
        relay(c)

    @pl.when(me_t == 0)
    def _():
        halo[...] = jnp.zeros(halo.shape, halo.dtype)
        spilled[...] = jnp.zeros(spilled.shape, F32)

    @pl.when(me_t > 0)
    def _():
        for copy in spill_copies:
            copy.wait_recv()

    send(0, 0, groups)
    if chips > 3:
        listen(0)
        tell(1)

    sbuf[mine, :] = spatial_ref[...]
    passed = []
    for d, source in enumerate(sources(me_a, n_atom)):
        s_copies[d].wait_recv()
        rows = half_of(source)
        out = pltpu.make_async_remote_copy(
            src_ref=sbuf.at[rows], dst_ref=sbuf.at[rows],
            send_sem=h_send.at[d], recv_sem=h_recv.at[d],
            device_id={"tm": partner}, device_id_type=MESH,
        )
        out.start()
        passed.append(out)

    @pl.when(me_t > 0)
    def _():
        halo_copy.wait_recv()

    before = halo[...].astype(F32)
    for b in range(hb):
        lay_time(b, before[:, b * W : (b + 1) * W])

    per_block = W // B
    deep = per_block * GROUP
    slots = W // deep
    place = lax.rem(lax.broadcasted_iota(jnp.int32, (8, W), 0), slots) == (
        lax.broadcasted_iota(jnp.int32, (8, W), 1) // deep
    )

    def lay(n, carry):
        for i in range(8):
            picked = [
                xt[pl.ds((B // 8 * r + B // 8 - 1 - n) * GROUP * 8 + 7 - i, GROUP, stride=8), :]
                for r in range(per_block)
            ]
            picked = jnp.concatenate(picked * (W // deep), axis=0).T
            for g in range(groups):
                at = pl.multiple_of((g * B + 8 * n + i) * 8, 8)
                lt[pl.ds(at, 8), :] = jnp.where(place, picked[8 * g : 8 * g + 8], 0.0)
        return carry

    lax.fori_loop(0, B // 8, lay, 0)

    for copy in passed:
        copy.wait_recv()
    sp32[:, :channels] = sbuf[...].astype(F32)
    st[...] = sp32[...].T[:rows_p].astype(BF16)
    own_w[...] = sp32[mine, :rows_p].astype(BF16)

    def process(c, gsp):
        for copy in c_waits[c]:
            copy.wait_recv()
        model = jnp.dot(st[...], cbuf[c], preferred_element_type=F32)
        resb[c, :channels, :] = (
            model[:channels] - signal_ref[:, c * chunk : (c + 1) * chunk].astype(F32)
        ).astype(BF16)
        residual = resb[c]
        grad = lax.dot_general(
            cbuf[c, mine, :], residual, (((1,), (1,)), ((), ())), preferred_element_type=F32
        )
        return grad if gsp is None else gsp + grad

    def project(c):
        projected = jnp.dot(own_w[...], resb[c], preferred_element_type=F32)
        projected = projected.astype(BF16).astype(F32)
        for b in range(per):
            at = hb + c * per + b
            put(pj.at[0], span, at, projected[:, b * W : (b + 1) * W])

    gsp = None
    for c in order + [0]:
        gsp = process(c, gsp)

    low = pl.ds(pl.multiple_of(core * (atoms // 2), atoms // 2), atoms // 2)
    other = pl.ds(pl.multiple_of((1 - core) * (atoms // 2), atoms // 2), atoms // 2)

    def swap(i, lanes):
        copy = pltpu.make_async_remote_copy(
            src_ref=part.at[i, other, lanes], dst_ref=recv1.at[i, :, lanes],
            send_sem=p_send.at[i], recv_sem=p_recv.at[i],
            device_id={"tm": partner}, device_id_type=MESH,
        )
        return copy

    def encode(value):
        top = jnp.max(jnp.abs(value), axis=0, keepdims=True)
        up = jnp.where(top > TINY, STEPS / jnp.maximum(top, TINY), 0.0)
        shift = jnp.where(value < 0, -0.5, 0.5)
        return value * up + shift, top * (1.0 / STEPS)

    def spread(i, lanes, copy):
        copy.wait_recv()
        value, step = encode(part[i, low, lanes] + recv1[i, :, lanes])
        scale[i, me_z, :, lanes] = step
        refs = [half.at[i, me_z, :, lanes], scale.at[i, me_z, :, lanes]]
        if i == 0 and fold:
            rest = value[:, wide - W :]
            rest = jnp.where(
                low_lane, rest[: atoms // 4], pltpu.roll(rest[atoms // 4 :], W // 2, 1)
            )
            folded[me_z] = rest.astype(jnp.int32).astype(jnp.int16)
            lanes = slice(0, wide - W)
            refs[0] = half.at[i, me_z, :, lanes]
            refs.append(folded.at[me_z])
            value = value[:, : wide - W]
        half[i, me_z, :, lanes] = value.astype(jnp.int32).astype(jnp.int16)
        copies = []
        for d, peer in enumerate(z_peers):
            for n, ref in enumerate(refs):
                out = pltpu.make_async_remote_copy(
                    src_ref=ref, dst_ref=ref,
                    send_sem=z_send.at[i, n, d], recv_sem=z_recv.at[i, n, d],
                    device_id={"tm": peer * 2 + core}, device_id_type=MESH,
                )
                out.start()
                copies.append(out)
        return copies

    def finish(i, lanes, copies):
        for copy in copies:
            copy.wait_recv()
        acc = None
        for z in range(chips):
            if i == 0 and fold:
                rest = folded[z].astype(jnp.int32).astype(F32)
                rest = jnp.concatenate([rest, pltpu.roll(rest, W // 2, 1)], axis=0)
                value = half[i, z, :, : wide - W].astype(jnp.int32).astype(F32)
                value = jnp.concatenate([value, rest], axis=1)
            else:
                value = half[i, z, :, lanes].astype(jnp.int32).astype(F32)
            value = value * scale[i, z, :, lanes]
            acc = value if acc is None else acc + value
        total[i, low, lanes] = acc * factor
        copy = pltpu.make_async_remote_copy(
            src_ref=total.at[i, low, lanes], dst_ref=total.at[i, low, lanes],
            send_sem=f_send.at[i], recv_sem=f_recv.at[i],
            device_id={"tm": partner}, device_id_type=MESH,
        )
        copy.start()
        return copy

    fold = wide > W and channels - (wide - W) <= W // 2 and atoms % 64 == 0
    low_lane = lax.broadcasted_iota(jnp.int32, (atoms // 4, W), 1) < W // 2
    sp_lanes = slice(0, wide)
    tm_lanes = slice(0, length)
    part[0, :, :rows_p] = gsp
    if rows_p < wide:
        part[0, :, rows_p:] = jnp.zeros((atoms, wide - rows_p), F32)
    swap_sp = swap(0, sp_lanes)
    swap_sp.start()
    for c in range(chunks):
        project(c)

    lane = lax.broadcasted_iota(jnp.int32, (atoms, W), 1)
    for r in range(1, per_block):
        turned = [
            pltpu.roll(natural(pj.at[0], span, i), W - B * r, 1)
            for i in range(hb, hb + nb)
        ]
        turned = [jnp.zeros((atoms, W), F32)] + turned + [jnp.zeros((atoms, W), F32)]
        for n in range(nb + 1):
            put(
                pj.at[r], span, hb - 1 + n,
                jnp.where(lane < W - B * r, turned[n], turned[n + 1]),
            )

    depth = (length + B - 1) // W + 1

    def correlate(g, carry):
        for first_atom in range(0, 8, 2 * slots):
            some = range(first_atom, first_atom + 2 * slots)
            lhs = []
            rhs = []
            for i in some:
                left = series(lt, B, g, i, 0, B).astype(BF16)
                none = jnp.zeros((B, W), BF16)
                pair = [left, none] if i - first_atom < slots else [none, left]
                lhs.append(jnp.concatenate(pair, axis=1))
                for r in range(per_block):
                    rhs.append(
                        jnp.concatenate(
                            [series(pj.at[r], span, g, i, j, GROUP) for j in range(depth)], axis=1
                        )
                    )
            prods = jnp.dot(
                jnp.concatenate(lhs, axis=0),
                jnp.concatenate(rhs, axis=0).astype(BF16),
                preferred_element_type=F32,
            )
            for n, i in enumerate(some):
                prod = prods[n * B : (n + 1) * B]
                prod = pltpu.roll(prod, depth * W - (B - 1), 1, stride=1, stride_axis=0)
                acc = prod[:8, :length]
                for q in range(1, B // 8):
                    acc = acc + prod[8 * q : 8 * q + 8, :length]
                for d in range(hb):
                    at = pl.multiple_of((d * groups + g) * 64 + 8 * i, 8)
                    gt[pl.ds(at, 8), :] = acc[:, d * W : (d + 1) * W]
        return carry

    def lags(mine_first, rows):
        for d in range(hb):
            at = 8 * (d * atoms + mine_first)
            total_d = gt[pl.ds(at, atoms // 2, stride=8), :]
            for i in range(1, 8):
                total_d = total_d + gt[pl.ds(at + i, atoms // 2, stride=8), :]
            part[1, rows, d * W : (d + 1) * W] = total_d

    def correlate_from(start, count):
        lax.fori_loop(0, count, lambda n, carry: correlate(start + n, carry), 0, unroll=count)

    swap_tm = swap(1, tm_lanes)

    def theirs():
        correlate_from((1 - core) * (groups // 2), groups // 2)
        lags((1 - core) * (atoms // 2), other)
        swap_tm.start()

    pl.when(core == 1)(theirs)
    for turn in range(1, chips - 3):
        listen(turn)
        tell(turn + 1)
    if chips > 2:
        listen(chips - 3)
    spread_sp = spread(0, sp_lanes, swap_sp)
    pl.when(core == 0)(theirs)
    correlate_from(core * (groups // 2), groups // 2)
    lags(core * (atoms // 2), low)
    spread_tm = spread(1, tm_lanes, swap_tm)
    last_sp = finish(0, sp_lanes, spread_sp)
    last_tm = finish(1, tm_lanes, spread_tm)
    last_sp.wait_recv()
    out_sp_ref[...] = total[0, :, :channels]
    last_tm.wait_recv()
    out_tm_ref[...] = total[1, :, :length]

    @pl.when(me_t < n_tm - 1)
    def _():
        halo_copy.wait_send()
        for copy in spill_copies:
            copy.wait_send()

    for copy in s_copies + passed + [copy for line in c_copies for copy in line]:
        copy.wait_send()
    for copy in [swap_sp, swap_tm, last_sp, last_tm] + spread_sp + spread_tm:
        copy.wait_send()


def local(n_atom, n_tm, signal, spatial, temporal, values, mask):
    atoms, channels = spatial.shape
    length = temporal.shape[1]
    samples = signal.shape[1]
    chunks = samples // length
    nb, hb = samples // W, length // W
    wide = -(-channels // W) * W
    rows_p = -(-channels // 32) * 32
    per_block = W // B
    deep = per_block * GROUP
    slots = W // deep
    place = lax.rem(lax.broadcasted_iota(jnp.int32, (8, W), 0), slots) == (
        lax.broadcasted_iota(jnp.int32, (8, W), 1) // deep
    )
    every = n_atom * atoms
    depth = (length + B - 1) // W + 1
    span = (GROUP + depth - 1) * atoms
    width = max(wide, length)
    chips = n_tm // 2
    factor = 1.0 / math.sqrt(samples * n_tm)
    dma = pltpu.SemaphoreType.DMA
    vmem = pl.BlockSpec(memory_space=pltpu.VMEM)
    return pl.pallas_call(
        functools.partial(kernel, n_atom, n_tm, factor),
        out_shape=(
            pltpu.VMEM((atoms, channels), F32),
            pltpu.VMEM((atoms, length), F32),
        ),
        in_specs=[vmem] * 5,
        out_specs=(vmem, vmem),
        scratch_shapes=[
            pltpu.VMEM((atoms, length), BF16),
            pltpu.VMEM((atoms, length), BF16),
            pltpu.VMEM((atoms, length), F32),
            pltpu.VMEM((atoms, length), F32),
            pltpu.VMEM(((GROUP + hb) * atoms, W), F32),
            pltpu.VMEM((GROUP * W, W), F32),
            pltpu.VMEM((hb * atoms, W), F32),
            pltpu.VMEM((GROUP * atoms, W), F32),
            pltpu.VMEM((chunks, every, length), BF16),
            pltpu.VMEM((every, channels), BF16),
            pltpu.VMEM((every, wide), F32),
            pltpu.VMEM((rows_p, every), BF16),
            pltpu.VMEM((atoms, rows_p), BF16),
            pltpu.VMEM((chunks, rows_p, length), BF16),
            pltpu.VMEM((per_block, span, W), F32),
            pltpu.VMEM((B * atoms, W), F32),
            pltpu.VMEM((8 * hb * atoms, W), F32),
            pltpu.VMEM((2, atoms, width), F32),
            pltpu.VMEM((2, atoms // 2, width), F32),
            pltpu.VMEM((2, chips, atoms // 2, width), jnp.int16),
            pltpu.VMEM((chips, max(atoms // 4, GROUP), W), jnp.int16),
            pltpu.VMEM((2, chips, 1, width), F32),
            pltpu.VMEM((2, atoms, width), F32),
            pltpu.SemaphoreType.REGULAR((max(chips - 2, 1), 2)),
            dma((6,)),
            dma((n_atom - 1,)),
            dma((n_atom - 1,)),
            dma((n_atom - 1,)),
            dma((n_atom - 1,)),
            dma((n_atom - 1, chunks, 2)),
            dma((n_atom - 1, chunks, 2)),
            dma((2,)),
            dma((2,)),
            dma((2, 3, chips - 1)),
            dma((2, 3, chips - 1)),
            dma((2,)),
            dma((2,)),
        ],
        compiler_params=pltpu.CompilerParams(collective_id=0, has_side_effects=True),
    )(signal, spatial, temporal, values, mask.T)


def settle(a_ref, b_ref, c_ref, d_ref, sems):
    one = pltpu.make_async_copy(a_ref, c_ref, sems.at[0])
    two = pltpu.make_async_copy(b_ref, d_ref, sems.at[1])
    one.start()
    two.start()
    one.wait()
    two.wait()


def placed(n_atom, n_tm, *args):
    first, second = local(n_atom, n_tm, *args)
    return pl.pallas_call(
        settle,
        out_shape=(
            jax.ShapeDtypeStruct(first.shape, F32),
            jax.ShapeDtypeStruct(second.shape, F32),
        ),
        in_specs=[pl.BlockSpec(memory_space=pltpu.VMEM)] * 2,
        out_specs=[pl.BlockSpec(memory_space=pltpu.HBM)] * 2,
        scratch_shapes=[pltpu.SemaphoreType.DMA((2,))],
        compiler_params=pltpu.CompilerParams(vmem_limit_bytes=1 << 20),
    )(first, second)


def solution(mesh):
    in_specs = (P(None, "tm"), P("atom", None), P("atom", None), P("atom", "tm"), P("atom", "tm"))
    out_specs = (P("atom", None), P("atom", None))
    body = functools.partial(placed, mesh.shape["atom"], mesh.shape["tm"])
    return jax.shard_map(body, mesh=mesh, in_specs=in_specs, out_specs=out_specs, check_vma=False)
```
